16 devices in a mesh: dp: 4 (over z, y), tp: 4 (over x, core).
Axes of the slice: x: 2, y: 2, z: 2, core: 2. Of those that a mesh axis runs over, the one named last changes fastest.
Arguments:
- latents: bfloat16 [32, 24, 24, 1280], P('dp', 'tp'), parts along dimension 0
- context: bfloat16 [32, 77, 1024], P('dp'), parts along dimension 0
- io_vecs: float32 [4, 1280], replicated
- w_proj: bfloat16 [2, 1280, 1280], replicated
- block_vecs: float32 [2, 9, 1280], replicated
- w_qkv: bfloat16 [2, 1280, 3, 20, 64], P(None, None, None, 'tp')
- w_o1: bfloat16 [2, 20, 64, 1280], P(None, 'tp')
- w_q2: bfloat16 [2, 1280, 20, 64], P(None, None, 'tp')
- w_kv2: bfloat16 [2, 1024, 2, 20, 64], P(None, None, None, 'tp')
- w_o2: bfloat16 [2, 20, 64, 1280], P(None, 'tp')
- w_ff1: bfloat16 [2, 1280, 2, 5120], P(None, None, None, 'tp')
- b_ff1: float32 [2, 2, 5120], P(None, None, 'tp')
- w_ff2: bfloat16 [2, 5120, 1280], P(None, 'tp')
Outputs:
- output: bfloat16 [32, 24, 24, 1280], P('dp', 'tp'), parts along dimension 0
There are 4 independent parts. The reference program is written for one: setup_inputs(seed, part) draws one part's arguments, and reference() takes and returns one part's arrays. A program takes and returns all parts, laid end to end along the dimension named above; an argument that names none is the same for every part.
All inputs are finite; a program needn't handle non-finite values.
Results may differ from the reference program's by a relative error of at most 0.0161513.
Values are sent between devices in bfloat16 or wider.
A program may use at most 1 GiB of HBM per device.

```python
import jax
import jax.numpy as jnp
from jax import lax

BATCH = 8
SIDE = 24
CHANNELS = 1280
HEADS = 20
HEAD = 64
FF = 5120
CTX_LEN = 77
CTX_DIM = 1024
BLOCKS = 2
GROUPS = 32

TOKENS = SIDE * SIDE
INNER = HEADS * HEAD
GN_EPS = 1e-6
LN_EPS = 1e-5


def normal_weights(draw_key, out_shape, fan_in, scale_gain):
    return jax.random.normal(draw_key, out_shape, jnp.float32) * (scale_gain * fan_in ** -0.5)


def setup_inputs(seed: int = 0, part: int = 0) -> dict:
    root_keys = jax.random.split(jax.random.key(seed), 2)
    shared = jax.random.split(root_keys[0], 12)
    part_keys = jax.random.split(jax.random.fold_in(root_keys[1], part), 4)
    noise_part = jax.random.normal(part_keys[0], (BATCH, SIDE, SIDE, CHANNELS), jnp.float32)
    ramp_amp = jax.random.normal(part_keys[1], (BATCH, 1, 1, CHANNELS), jnp.float32)
    row_pos = jnp.linspace(-1.0, 1.0, SIDE).reshape(1, SIDE, 1, 1)
    sample_scale = 0.6 + 0.8 * jax.random.uniform(part_keys[2], (BATCH, 1, 1, 1), jnp.float32)
    latents = ((noise_part + 1.5 * ramp_amp * row_pos) * sample_scale).astype(jnp.bfloat16)
    context = jax.random.normal(part_keys[3], (BATCH, CTX_LEN, CTX_DIM), jnp.float32).astype(jnp.bfloat16)
    io_scale = jnp.array([0.2, 0.2, 0.3, 0.3]).reshape(4, 1)
    io_offset = jnp.array([1.0, 0.0, 0.0, 0.0]).reshape(4, 1)
    io_vecs = jax.random.normal(shared[0], (4, CHANNELS), jnp.float32) * io_scale + io_offset
    w_proj = normal_weights(shared[1], (2, CHANNELS, CHANNELS), CHANNELS, 1.0).astype(jnp.bfloat16)
    vec_scale = jnp.array([0.2, 0.2, 0.2, 0.2, 0.2, 0.2, 0.3, 0.3, 0.3]).reshape(1, 9, 1)
    vec_offset = jnp.array([1.0, 0.0, 1.0, 0.0, 1.0, 0.0, 0.0, 0.0, 0.0]).reshape(1, 9, 1)
    block_vecs = jax.random.normal(shared[2], (BLOCKS, 9, CHANNELS), jnp.float32) * vec_scale + vec_offset
    qkv_gain = jnp.array([1.5, 1.5, 1.0]).reshape(1, 1, 3, 1, 1)
    w_qkv = (normal_weights(shared[3], (BLOCKS, CHANNELS, 3, HEADS, HEAD), CHANNELS, 1.0) * qkv_gain).astype(jnp.bfloat16)
    w_o1 = normal_weights(shared[4], (BLOCKS, HEADS, HEAD, CHANNELS), INNER, 1.0).astype(jnp.bfloat16)
    w_q2 = normal_weights(shared[5], (BLOCKS, CHANNELS, HEADS, HEAD), CHANNELS, 1.5).astype(jnp.bfloat16)
    kv_gain = jnp.array([1.5, 1.0]).reshape(1, 1, 2, 1, 1)
    w_kv2 = (normal_weights(shared[6], (BLOCKS, CTX_DIM, 2, HEADS, HEAD), CTX_DIM, 1.0) * kv_gain).astype(jnp.bfloat16)
    w_o2 = normal_weights(shared[7], (BLOCKS, HEADS, HEAD, CHANNELS), INNER, 1.0).astype(jnp.bfloat16)
    w_ff1 = normal_weights(shared[8], (BLOCKS, CHANNELS, 2, FF), CHANNELS, 1.0).astype(jnp.bfloat16)
    b_ff1 = normal_weights(shared[9], (BLOCKS, 2, FF), 1, 0.4)
    w_ff2 = normal_weights(shared[10], (BLOCKS, FF, CHANNELS), FF, 1.0).astype(jnp.bfloat16)
    return {"latents": latents, "context": context, "io_vecs": io_vecs, "w_proj": w_proj, "block_vecs": block_vecs, "w_qkv": w_qkv, "w_o1": w_o1, "w_q2": w_q2, "w_kv2": w_kv2, "w_o2": w_o2, "w_ff1": w_ff1, "b_ff1": b_ff1, "w_ff2": w_ff2}


def layer_norm(hidden, ln_gain, ln_shift):
    average = jnp.mean(hidden, axis=-1, keepdims=True)
    centered = hidden - average
    variance = jnp.mean(centered * centered, axis=-1, keepdims=True)
    return centered * lax.rsqrt(variance + LN_EPS) * ln_gain + ln_shift


def attend_one(operands):
    queries, key_rows, value_rows = operands
    scale = queries.shape[-1] ** -0.5
    scores = jnp.einsum("qhd,khd->hqk", queries.astype(jnp.float32), key_rows.astype(jnp.float32)) * scale
    attn_probs = jax.nn.softmax(scores, axis=-1).astype(jnp.bfloat16)
    mixed = jnp.einsum("hqk,khd->qhd", attn_probs.astype(jnp.float32), value_rows.astype(jnp.float32))
    return mixed.astype(jnp.bfloat16)


def reference(latents, context, io_vecs, w_proj, block_vecs, w_qkv, w_o1, w_q2, w_kv2, w_o2, w_ff1, b_ff1, w_ff2):
    batch = latents.shape[0]
    x_rows = latents.reshape(batch, TOKENS, CHANNELS).astype(jnp.float32)
    grouped = x_rows.reshape(batch, TOKENS, GROUPS, CHANNELS // GROUPS)
    group_mean = jnp.mean(grouped, axis=(1, 3), keepdims=True)
    centered = grouped - group_mean
    group_var = jnp.mean(centered * centered, axis=(1, 3), keepdims=True)
    normed = (centered * lax.rsqrt(group_var + GN_EPS)).reshape(batch * TOKENS, CHANNELS)
    normed = normed * io_vecs[0] + io_vecs[1]
    hidden = jnp.dot(normed.astype(jnp.bfloat16), w_proj[0], preferred_element_type=jnp.float32) + io_vecs[2]
    ctx_rows = context.reshape(batch * CTX_LEN, CTX_DIM)

    def block_step(hidden, weights):
        layer_vecs, wqkv_l, wo1_l, wq2_l, wkv2_l, wo2_l, wff1_l, bff1_l, wff2_l = weights
        normed_a = layer_norm(hidden, layer_vecs[0], layer_vecs[1]).astype(jnp.bfloat16)
        qkv_rows = jnp.dot(normed_a, wqkv_l.reshape(CHANNELS, 3 * INNER), preferred_element_type=jnp.float32).astype(jnp.bfloat16)
        qkv_rows = qkv_rows.reshape(batch, TOKENS, 3, HEADS, HEAD)
        mixed = lax.map(attend_one, (qkv_rows[:, :, 0], qkv_rows[:, :, 1], qkv_rows[:, :, 2]))
        hidden = hidden + jnp.dot(mixed.reshape(batch * TOKENS, INNER), wo1_l.reshape(INNER, CHANNELS), preferred_element_type=jnp.float32) + layer_vecs[6]
        normed_c = layer_norm(hidden, layer_vecs[2], layer_vecs[3]).astype(jnp.bfloat16)
        cross_q = jnp.dot(normed_c, wq2_l.reshape(CHANNELS, INNER), preferred_element_type=jnp.float32).astype(jnp.bfloat16)
        cross_q = cross_q.reshape(batch, TOKENS, HEADS, HEAD)
        ctx_kv = jnp.dot(ctx_rows, wkv2_l.reshape(CTX_DIM, 2 * INNER), preferred_element_type=jnp.float32).astype(jnp.bfloat16)
        ctx_kv = ctx_kv.reshape(batch, CTX_LEN, 2, HEADS, HEAD)
        mixed_c = lax.map(attend_one, (cross_q, ctx_kv[:, :, 0], ctx_kv[:, :, 1]))
        hidden = hidden + jnp.dot(mixed_c.reshape(batch * TOKENS, INNER), wo2_l.reshape(INNER, CHANNELS), preferred_element_type=jnp.float32) + layer_vecs[7]
        normed_f = layer_norm(hidden, layer_vecs[4], layer_vecs[5]).astype(jnp.bfloat16)
        up_rows = jnp.dot(normed_f, wff1_l.reshape(CHANNELS, 2 * FF), preferred_element_type=jnp.float32).reshape(batch * TOKENS, 2, FF) + bff1_l
        gated = (up_rows[:, 0] * jax.nn.gelu(up_rows[:, 1], approximate=False)).astype(jnp.bfloat16)
        hidden = hidden + jnp.dot(gated, wff2_l, preferred_element_type=jnp.float32) + layer_vecs[8]
        return hidden, None

    hidden = lax.scan(block_step, hidden, (block_vecs, w_qkv, w_o1, w_q2, w_kv2, w_o2, w_ff1, b_ff1, w_ff2))[0]
    out_rows = jnp.dot(hidden.astype(jnp.bfloat16), w_proj[1], preferred_element_type=jnp.float32) + io_vecs[3]
    return (out_rows.reshape(batch, SIDE, SIDE, CHANNELS) + latents.astype(jnp.float32)).astype(jnp.bfloat16)
```

```python
import functools

import jax
import jax.numpy as jnp
from jax import lax
from jax.experimental import pallas as pl
from jax.experimental.pallas import tpu as pltpu
from jax.sharding import PartitionSpec as P

GROUPS = 32
GN_EPS = 1e-6
LN_EPS = 1e-5
SHARDS = 4
HEAD = 64
LOG2E = 1.4426950408889634
F32 = jnp.float32
BF16 = jnp.bfloat16
NT = (((1,), (1,)), ((), ()))
VMEM_LIMIT = 50 * 1024 * 1024


def layer_norm(hidden, ln_gain, ln_shift):
    average = jnp.mean(hidden, axis=-1, keepdims=True)
    centered = hidden - average
    variance = jnp.mean(centered * centered, axis=-1, keepdims=True)
    return (centered * lax.rsqrt(variance + LN_EPS) * ln_gain + ln_shift).astype(BF16)


def attend(q, k, v, valid=None):
    scores = lax.dot_general(q, k, NT, preferred_element_type=F32)
    if valid is not None:
        col = lax.broadcasted_iota(jnp.int32, scores.shape, 1)
        scores = jnp.where(col < valid, scores, -jnp.inf)
    top = jnp.max(scores, axis=-1, keepdims=True)
    probs = jnp.exp2((scores - top) * (HEAD ** -0.5 * LOG2E)).astype(BF16)
    values = jnp.concatenate([v, jnp.ones_like(v)], axis=1)
    mixed = jnp.dot(probs, values, preferred_element_type=F32)
    return (mixed[:, :HEAD] / mixed[:, HEAD:]).astype(BF16)


def self_kernel(a_ref, w_ref, o_ref):
    width = o_ref.shape[-1]
    qkv = lax.dot_general(a_ref[0], w_ref[0], NT, preferred_element_type=F32).astype(BF16)
    for head in range(width // HEAD):
        lo = head * HEAD
        o_ref[0, :, lo:lo + HEAD] = attend(
            qkv[:, lo:lo + HEAD], qkv[:, width + lo:width + lo + HEAD],
            qkv[:, 2 * width + lo:2 * width + lo + HEAD])


def cross_kernel(valid, a_ref, c_ref, wq_ref, wkv_ref, o_ref):
    width = o_ref.shape[-1]
    q = lax.dot_general(a_ref[0], wq_ref[0], NT, preferred_element_type=F32).astype(BF16)
    kv = lax.dot_general(c_ref[0], wkv_ref[0], NT, preferred_element_type=F32).astype(BF16)
    for head in range(width // HEAD):
        lo = head * HEAD
        o_ref[0, :, lo:lo + HEAD] = attend(
            q[:, lo:lo + HEAD], kv[:, lo:lo + HEAD], kv[:, width + lo:width + lo + HEAD], valid)


def out_kernel(h_ref, o0, o1, o2, o3, w0, w1, w2, w3, vec_ref, h_out, a_out, o_all, w_all):
    width = o0.shape[-1]
    for i, (o_ref, w_ref) in enumerate(((o0, w0), (o1, w1), (o2, w2), (o3, w3))):
        o_all[:, i * width:(i + 1) * width] = o_ref[0]
        w_all[i * width:(i + 1) * width, :] = w_ref[0]
    h = h_ref[0] + jnp.dot(o_all[...], w_all[...], preferred_element_type=F32) + vec_ref[0:1]
    h_out[0] = h
    a_out[0] = layer_norm(h, vec_ref[1:2], vec_ref[2:3])


def ff_body(a_ref, w1_ref, b1_ref, w2_ref, m_scr):
    cols = 256
    a = a_ref[0]
    for j in range(m_scr.shape[-1] // cols):
        sl = slice(j * cols, (j + 1) * cols)
        u0 = jnp.dot(a, w1_ref[0, 0, :, sl], preferred_element_type=F32) + b1_ref[0, 0:1, sl]
        u1 = jnp.dot(a, w1_ref[0, 1, :, sl], preferred_element_type=F32) + b1_ref[0, 1:2, sl]
        gate = 0.5 * u1 * (1.0 + lax.erf(u1 * (0.5 ** 0.5)))
        m_scr[:, sl] = (u0 * gate).astype(BF16)
    return jnp.dot(m_scr[...], w2_ref[0], preferred_element_type=F32)


def ff_kernel(h_ref, a_ref, w1_ref, b1_ref, w2_ref, h_out, m_scr):
    h_out[0] = h_ref[0] + ff_body(a_ref, w1_ref, b1_ref, w2_ref, m_scr)


def ff_last_kernel(h_ref, a_ref, w1_ref, b1_ref, w2_ref, vec_ref, h_out, a_out, m_scr):
    h = h_ref[0] + ff_body(a_ref, w1_ref, b1_ref, w2_ref, m_scr) + vec_ref[0:1]
    h_out[0] = h
    a_out[0] = layer_norm(h, vec_ref[1:2], vec_ref[2:3])


def rows_spec(shape):
    return pl.BlockSpec((1,) + shape, lambda i: (i, 0, 0))


def fixed_spec(shape, layer):
    return pl.BlockSpec((1,) + shape, lambda i: (layer,) + (0,) * len(shape))


def vec_spec(rows, cols):
    return pl.BlockSpec((rows, cols), lambda i: (0, 0))


def call(kernel, name, grid, in_specs, out_specs, out_shape, flops, scratch=(), aliases=None):
    return pl.pallas_call(
        kernel, grid=grid, in_specs=in_specs, out_specs=out_specs, out_shape=out_shape,
        scratch_shapes=scratch, name=name, input_output_aliases=aliases or {},
        cost_estimate=pl.CostEstimate(flops=flops, bytes_accessed=16 << 20, transcendentals=0),
        compiler_params=pltpu.CompilerParams(vmem_limit_bytes=VMEM_LIMIT))


def solution(mesh):
    tp_size = mesh.shape["tp"]
    dp_size = mesh.shape["dp"]

    def swap(value, mask):
        return lax.ppermute(value, "tp", [(i, i ^ mask) for i in range(tp_size)])

    def shard_body(latents, context, io_vecs, w_proj, block_vecs, w_qkv, w_o1, w_q2, w_kv2, w_o2, w_ff1, b_ff1, w_ff2):
        batch, rows_loc, side, channels = latents.shape
        tok = rows_loc * side
        layers = w_qkv.shape[0]
        heads = w_o1.shape[1]
        width = heads * HEAD
        ff = w_ff2.shape[1]
        ctx_len, ctx_dim = context.shape[1:]
        mine = batch // tp_size
        me = lax.axis_index("tp")
        dp_me = lax.axis_index("dp")
        x_rows = latents.reshape(tp_size, mine, tok, channels)

        def group_of(array, index):
            return lax.dynamic_index_in_dim(array, index, 0, keepdims=False)

        x_parts = [group_of(x_rows, me)]
        x_parts += [swap(group_of(x_rows, me ^ m), m) for m in (1, 2, 3)]

        qkv_t = w_qkv.transpose(0, 2, 3, 4, 1).reshape(layers, 3 * width, channels)
        q2_t = w_q2.transpose(0, 2, 3, 1).reshape(layers, width, channels)
        kv2_t = w_kv2.transpose(0, 2, 3, 4, 1).reshape(layers, 2 * width, ctx_dim)
        o1_t = w_o1.reshape(layers, width, channels)
        o2_t = w_o2.reshape(layers, width, channels)
        ff1_t = w_ff1.transpose(0, 2, 1, 3)
        own = {"qkv": qkv_t, "o1": o1_t, "q2": q2_t, "kv2": kv2_t, "o2": o2_t, "ff1": ff1_t, "ff2": w_ff2}
        sib = {name: swap(value, 1) for name, value in own.items()}
        bias = [b_ff1] + [swap(b_ff1, m) for m in (1, 2, 3)]

        def remote(name, layer):
            value = own[name][layer]
            flat = value.reshape(-1, value.shape[-1])
            rows = flat.shape[0] // dp_size
            piece = lax.dynamic_slice_in_dim(flat, dp_me * rows, rows, 0)
            full = lax.all_gather(swap(piece, 2), "dp", axis=0, tiled=True)
            full = full.reshape((1,) + value.shape)
            return full, swap(full, 1)

        far = [{name: remote(name, layer) for name in own} for layer in range(layers)]

        def shards(name, layer):
            rem, rem_sib = far[layer][name]
            return ((own[name], layer), (sib[name], layer), (rem, 0), (rem_sib, 0))

        def samples(array):
            return array.reshape((mine, tp_size * tok) + array.shape[2:])

        x_all = jnp.concatenate(x_parts, axis=1)
        grouped = x_all.astype(F32).reshape(mine, tp_size * tok, GROUPS, channels // GROUPS)
        count = tp_size * tok * (channels // GROUPS)
        mean = jnp.sum(grouped, axis=(1, 3), keepdims=True) / count
        centered = grouped - mean
        var = jnp.sum(centered * centered, axis=(1, 3), keepdims=True) / count
        normed = (centered * lax.rsqrt(var + GN_EPS)).reshape(mine, tp_size * tok, channels)
        normed = (normed * io_vecs[0] + io_vecs[1]).astype(BF16)
        hidden = jnp.dot(normed, w_proj[0], preferred_element_type=F32) + io_vecs[2]
        act = layer_norm(hidden, block_vecs[0, 0], block_vecs[0, 1])

        ctx_pad = 128
        ctx_mine = lax.dynamic_slice_in_dim(context, me * mine, mine, 0)
        ctx_mine = jnp.pad(ctx_mine, ((0, 0), (0, ctx_pad - ctx_len), (0, 0)))

        n_tok = tp_size * tok
        grid = (mine,)
        a_shape = jax.ShapeDtypeStruct((mine, n_tok, channels), BF16)
        h_shape = jax.ShapeDtypeStruct((mine, n_tok, channels), F32)
        o_shape = jax.ShapeDtypeStruct((mine, n_tok, width), BF16)
        a_spec, o_spec = rows_spec((n_tok, channels)), rows_spec((n_tok, width))
        total = mine * n_tok

        def out_proj(hidden, mixed, weights, vecs, name):
            return call(
                out_kernel, name, grid,
                [a_spec] + [o_spec] * 4 + [fixed_spec((width, channels), l) for _, l in weights] + [vec_spec(3, channels)],
                [a_spec, a_spec], [h_shape, a_shape], 2 * total * channels * channels,
                scratch=[pltpu.VMEM((n_tok, SHARDS * width), BF16), pltpu.VMEM((SHARDS * width, channels), BF16)],
                aliases={0: 0},
            )(hidden, *mixed, *[w for w, _ in weights], vecs)

        for layer in range(layers):
            vecs = block_vecs[layer]
            mixed = [
                call(self_kernel, "self_attn", grid,
                     [a_spec, fixed_spec((3 * width, channels), l)], o_spec, o_shape,
                     2 * total * channels * 3 * width + 16 * total * n_tok * width)(act, w)
                for w, l in shards("qkv", layer)]
            hidden, act = out_proj(hidden, mixed, shards("o1", layer), jnp.stack([vecs[6], vecs[2], vecs[3]]), "out1")
            mixed = [
                call(functools.partial(cross_kernel, ctx_len), "cross_attn", grid,
                     [a_spec, rows_spec((ctx_pad, ctx_dim)), fixed_spec((width, channels), l), fixed_spec((2 * width, ctx_dim), l)],
                     o_spec, o_shape, 2 * total * channels * width * 3)(act, ctx_mine, wq, wkv)
                for (wq, l), (wkv, _) in zip(shards("q2", layer), shards("kv2", layer))]
            hidden, act = out_proj(hidden, mixed, shards("o2", layer), jnp.stack([vecs[7], vecs[4], vecs[5]]), "out2")
            ff_args = list(zip(shards("ff1", layer), bias, shards("ff2", layer)))
            for i, ((w1, l1), b1, (w2, l2)) in enumerate(ff_args):
                specs = [a_spec, a_spec, pl.BlockSpec((1, 2, channels, ff), lambda i, l=l1: (l, 0, 0, 0)),
                         fixed_spec((2, ff), layer), fixed_spec((ff, channels), l2)]
                scratch = [pltpu.VMEM((n_tok, ff), BF16)]
                flops = 6 * total * channels * ff
                if i < SHARDS - 1:
                    hidden = call(ff_kernel, "ff", grid, specs, a_spec, h_shape, flops, scratch, {0: 0})(
                        hidden, act, w1, b1, w2)
                else:
                    after = block_vecs[min(layer + 1, layers - 1)]
                    hidden, act = call(
                        ff_last_kernel, "ff_last", grid, specs + [vec_spec(3, channels)],
                        [a_spec, a_spec], [h_shape, a_shape], flops, scratch, {0: 0})(
                        hidden, act, w1, b1, w2, jnp.stack([vecs[8], after[0], after[1]]))
        out_rows = jnp.dot(hidden.astype(BF16), w_proj[1], preferred_element_type=F32) + io_vecs[3]
        out_rows = (out_rows + x_all.astype(F32)).astype(BF16).reshape(mine, tp_size, tok, channels)

        y = jnp.zeros((tp_size, mine, tok, channels), BF16)
        for m in range(tp_size):
            part = out_rows[:, m]
            part = part if m == 0 else swap(part, m)
            y = lax.dynamic_update_index_in_dim(y, part, me ^ m, 0)
        return y.reshape(batch, rows_loc, side, channels)

    act_spec = P("dp", "tp", None, None)
    in_specs = (act_spec, P("dp", None, None), P(), P(), P(),
                P(None, None, None, "tp", None), P(None, "tp", None, None),
                P(None, None, "tp", None), P(None, None, None, "tp", None),
                P(None, "tp", None, None), P(None, None, None, "tp"),
                P(None, None, "tp"), P(None, "tp", None))
    return jax.shard_map(shard_body, mesh=mesh, in_specs=in_specs, out_specs=act_spec, check_vma=False)
```

```python
import functools

import jax
import jax.numpy as jnp
from jax import lax
from jax.experimental import pallas as pl
from jax.experimental.pallas import tpu as pltpu
from jax.sharding import PartitionSpec as P

GROUPS = 32
GN_EPS = 1e-6
LN_EPS = 1e-5
SHARDS = 4
HEAD = 64
LOG2E = 1.4426950408889634
F32 = jnp.float32
BF16 = jnp.bfloat16
NT = (((1,), (1,)), ((), ()))
VMEM_LIMIT = 50 * 1024 * 1024


def layer_norm(hidden, ln_gain, ln_shift):
    average = jnp.mean(hidden, axis=-1, keepdims=True)
    centered = hidden - average
    variance = jnp.mean(centered * centered, axis=-1, keepdims=True)
    return (centered * lax.rsqrt(variance + LN_EPS) * ln_gain + ln_shift).astype(BF16)


def attend(q, k, v):
    scores = lax.dot_general(q, k, NT, preferred_element_type=F32)
    top = jnp.max(scores, axis=-1, keepdims=True)
    probs = jnp.exp2((scores - top) * (HEAD ** -0.5 * LOG2E)).astype(BF16)
    values = jnp.concatenate([v, jnp.ones_like(v)], axis=1)
    mixed = jnp.dot(probs, values, preferred_element_type=F32)
    return (mixed[:, :HEAD] / mixed[:, HEAD:]).astype(BF16)


def in_kernel(x0, x1, x2, x3, w_ref, io_ref, ln_ref, h_out, a_out):
    tok, channels = x0.shape[1:]
    parts = [ref[0].astype(F32) for ref in (x0, x1, x2, x3)]
    size = channels // GROUPS
    count = len(parts) * tok * size
    lanes = 128
    row = lax.broadcasted_iota(jnp.int32, (channels, lanes), 0)
    first = lax.broadcasted_iota(jnp.int32, (channels, lanes), 1) * size
    member = ((row >= first) & (row < first + size)).astype(F32)

    def group_average(columns):
        per_group = jnp.dot(jnp.broadcast_to(columns, (8, channels)), member,
                            precision=lax.Precision.HIGHEST, preferred_element_type=F32) / count
        return lax.dot_general(per_group, member, NT, precision=lax.Precision.HIGHEST,
                               preferred_element_type=F32)[0:1]

    mean = group_average(sum(jnp.sum(p, axis=0, keepdims=True) for p in parts))
    var = group_average(sum(jnp.sum((p - mean) * (p - mean), axis=0, keepdims=True) for p in parts))
    inverse = lax.rsqrt(var + GN_EPS)
    for i, p in enumerate(parts):
        normed = ((p - mean) * inverse * io_ref[0:1] + io_ref[1:2]).astype(BF16)
        h = jnp.dot(normed, w_ref[0], preferred_element_type=F32) + io_ref[2:3]
        h_out[0, i * tok:(i + 1) * tok, :] = h
        a_out[0, i * tok:(i + 1) * tok, :] = layer_norm(h, ln_ref[0:1], ln_ref[1:2])


def end_kernel(h_ref, w_ref, io_ref, x0, x1, x2, x3, y_ref):
    tok = x0.shape[1]
    y = jnp.dot(h_ref[0].astype(BF16), w_ref[0], preferred_element_type=F32) + io_ref[3:4]
    for i, ref in enumerate((x0, x1, x2, x3)):
        y_ref[i, 0] = (y[i * tok:(i + 1) * tok] + ref[0].astype(F32)).astype(BF16)


def flat(ref):
    value = ref[...]
    return value.reshape(-1, value.shape[-1])


def self_kernel(a_ref, w_ref, o_ref):
    width = o_ref.shape[-1]
    qkv = lax.dot_general(a_ref[0], flat(w_ref), NT, preferred_element_type=F32).astype(BF16)
    for head in range(width // HEAD):
        lo = head * HEAD
        o_ref[0, :, lo:lo + HEAD] = attend(
            qkv[:, lo:lo + HEAD], qkv[:, width + lo:width + lo + HEAD],
            qkv[:, 2 * width + lo:2 * width + lo + HEAD])


def cross_kernel(valid, a_ref, kv_ref, wq_ref, o_ref, k_scr, v_scr, p_scr):
    width = o_ref.shape[-1]
    keys = kv_ref.shape[2]
    lanes = 128
    v_half = v_scr.shape[1] // 2
    q = lax.dot_general(a_ref[0], flat(wq_ref), NT, preferred_element_type=F32).astype(BF16)
    k_scr[...] = jnp.zeros_like(k_scr)
    v_scr[...] = jnp.zeros_like(v_scr)
    k, v = kv_ref[0, 0, :, :width], kv_ref[0, 0, :, width:]
    row = lax.broadcasted_iota(jnp.int32, (keys, width), 0)
    col = lax.broadcasted_iota(jnp.int32, (keys, width), 1)
    heads = width // HEAD
    for head in range(heads):
        lo = head * lanes
        inside = (col >= head * HEAD) & (col < (head + 1) * HEAD) & (row < valid)
        k_scr[lo:lo + keys, :] = jnp.where(inside, k, jnp.zeros_like(k))
        v_scr[lo:lo + keys, :width] = jnp.where(inside, v, jnp.zeros_like(v))
        v_scr[lo:lo + keys, v_half:v_half + width] = inside.astype(BF16)
    scores = lax.dot_general(q, k_scr[...], NT, preferred_element_type=F32)
    live = lax.broadcasted_iota(jnp.int32, (q.shape[0], lanes), 1) < valid
    for head in range(heads):
        sl = slice(head * lanes, (head + 1) * lanes)
        s = jnp.where(live, scores[:, sl], -jnp.inf)
        top = jnp.max(s, axis=-1, keepdims=True)
        p_scr[:, sl] = jnp.exp2((s - top) * (HEAD ** -0.5 * LOG2E)).astype(BF16)
    mixed = jnp.dot(p_scr[...], v_scr[...], preferred_element_type=F32)
    o_ref[0] = (mixed[:, :width] / mixed[:, v_half:v_half + width]).astype(BF16)


def out_kernel(h_ref, o0, o1, o2, o3, w0, w1, w2, w3, vec_ref, h_out, a_out, o_all, w_all):
    width = o0.shape[-1]
    for i, (o_ref, w_ref) in enumerate(((o0, w0), (o1, w1), (o2, w2), (o3, w3))):
        o_all[:, i * width:(i + 1) * width] = o_ref[0]
        w_all[i * width:(i + 1) * width, :] = flat(w_ref)
    h = h_ref[0] + jnp.dot(o_all[...], w_all[...], preferred_element_type=F32) + vec_ref[0:1]
    h_out[0] = h
    a_out[0] = layer_norm(h, vec_ref[1:2], vec_ref[2:3])


def ff_body(packed, a_ref, w_ref, b1_ref, m_scr):
    cols = 256
    channels = w_ref.shape[-1]
    a = a_ref[0]

    def weight(i, sl):
        if packed:
            return w_ref[:, i, :, sl].reshape(channels, -1)
        return w_ref[0, i, :, sl]

    for j in range(m_scr.shape[-1] // cols):
        sl = slice(j * cols, (j + 1) * cols)
        u0 = jnp.dot(a, weight(0, sl), preferred_element_type=F32) + b1_ref[0, 0:1, sl]
        u1 = jnp.dot(a, weight(1, sl), preferred_element_type=F32) + b1_ref[0, 1:2, sl]
        gate = 0.5 * u1 * (1.0 + lax.erf(u1 * (0.5 ** 0.5)))
        m_scr[:, sl] = (u0 * gate).astype(BF16)
    return jnp.dot(m_scr[...], weight(2, slice(None)), preferred_element_type=F32)


def ff_kernel(packed, h_ref, a_ref, w_ref, b1_ref, h_out, m_scr):
    h_out[0] = h_ref[0] + ff_body(packed, a_ref, w_ref, b1_ref, m_scr)


def ff_last_kernel(packed, h_ref, a_ref, w_ref, b1_ref, vec_ref, h_out, a_out, m_scr):
    h = h_ref[0] + ff_body(packed, a_ref, w_ref, b1_ref, m_scr) + vec_ref[0:1]
    h_out[0] = h
    a_out[0] = layer_norm(h, vec_ref[1:2], vec_ref[2:3])


def rows_spec(shape):
    return pl.BlockSpec((1,) + shape, lambda i: (i, 0, 0))


def fixed_spec(shape, layer):
    return pl.BlockSpec((1,) + shape, lambda i: (layer,) + (0,) * len(shape))


def vec_spec(rows, cols):
    return pl.BlockSpec((rows, cols), lambda i: (0, 0))


def call(kernel, name, grid, in_specs, out_specs, out_shape, flops, scratch=(), aliases=None):
    return pl.pallas_call(
        kernel, grid=grid, in_specs=in_specs, out_specs=out_specs, out_shape=out_shape,
        scratch_shapes=scratch, name=name, input_output_aliases=aliases or {},
        cost_estimate=pl.CostEstimate(flops=flops, bytes_accessed=16 << 20, transcendentals=0),
        compiler_params=pltpu.CompilerParams(vmem_limit_bytes=VMEM_LIMIT))


def tie(*values):
    return lax.optimization_barrier(values)


def solution(mesh):
    tp_size = mesh.shape["tp"]
    dp_size = mesh.shape["dp"]

    def swap(value, mask):
        return lax.ppermute(value, "tp", [(i, i ^ mask) for i in range(tp_size)])

    def shard_body(latents, context, io_vecs, w_proj, block_vecs, w_qkv, w_o1, w_q2, w_kv2, w_o2, w_ff1, b_ff1, w_ff2):
        batch, rows_loc, side, channels = latents.shape
        tok = rows_loc * side
        layers = w_qkv.shape[0]
        width = w_o1.shape[1] * HEAD
        ff = w_ff2.shape[1]
        ctx_len = context.shape[1]
        ctx_pad = -(-ctx_len // 16) * 16
        mine = batch // tp_size
        n_tok = tp_size * tok
        me = lax.axis_index("tp")
        dp_me = lax.axis_index("dp")

        def dp_rows(value, axis):
            rows = value.shape[axis] // dp_size
            return lax.dynamic_slice_in_dim(value, dp_me * rows, rows, axis)

        def gather(piece):
            return lax.all_gather(piece, "dp", axis=0, tiled=True)

        qkv_t = w_qkv.transpose(0, 2, 3, 4, 1).reshape(layers, 3 * width, channels)
        q2_t = w_q2.transpose(0, 2, 3, 1).reshape(layers, width, channels)
        o1_t = w_o1.reshape(layers, width, channels)
        o2_t = w_o2.reshape(layers, width, channels)

        x_rows = latents.reshape(tp_size, mine, tok, channels)

        def group_of(array, index):
            return lax.dynamic_index_in_dim(array, index, 0, keepdims=False)

        x_parts = [group_of(x_rows, me)] + [swap(group_of(x_rows, me ^ m), m) for m in (1, 2, 3)]
        far_qkv = [swap(dp_rows(qkv_t[l], 0), 2) for l in range(1)]
        far_rest = [swap(jnp.concatenate([dp_rows(w[l], 0) for w in (o1_t, q2_t, o2_t)]), 2) for l in range(1)]
        sib_qkv, sib_o1, sib_q2, sib_o2 = (swap(w, 1) for w in (qkv_t, o1_t, q2_t, o2_t))
        bias = [b_ff1] + [swap(b_ff1, m) for m in (1, 2, 3)]

        kv = jnp.einsum("blc,rcjhd->rbljhd", context, w_kv2, preferred_element_type=F32).astype(BF16)
        kv = kv.reshape(layers, batch, ctx_len, 2 * width)
        kv = jnp.pad(kv, ((0, 0), (0, 0), (0, ctx_pad - ctx_len), (0, 0)))

        def kv_of(index):
            return lax.dynamic_slice_in_dim(kv, index * mine, mine, 1)

        kv_parts = [kv_of(me)] + [swap(kv_of(me ^ m), m) for m in (1, 2, 3)]
        ff_own = jnp.concatenate([w_ff1.transpose(0, 2, 1, 3), w_ff2[:, None]], axis=1)

        x0, x1, x2, x3, piece = tie(*x_parts, far_qkv[0])
        x_parts = [x0, x1, x2, x3]
        full_qkv = [gather(piece)]
        full_rest, full_ff = [], []
        x0, ff_src = tie(x0, ff_own)
        far_ff = [swap(dp_rows(ff_src[0], 1), 2)]
        sib_ff = swap(ff_own, 1)

        grid = (mine,)
        total = mine * n_tok
        a_shape = jax.ShapeDtypeStruct((mine, n_tok, channels), BF16)
        h_shape = jax.ShapeDtypeStruct((mine, n_tok, channels), F32)
        o_shape = jax.ShapeDtypeStruct((mine, n_tok, width), BF16)
        a_spec, o_spec = rows_spec((n_tok, channels)), rows_spec((n_tok, width))
        x_spec = rows_spec((tok, channels))

        hidden, act = call(
            in_kernel, "proj_in", grid,
            [x_spec] * 4 + [fixed_spec((channels, channels), 0), vec_spec(4, channels), vec_spec(2, channels)],
            [a_spec, a_spec], [h_shape, a_shape], 2 * total * channels * channels,
        )(*x_parts, w_proj, io_vecs, block_vecs[0, 0:2])

        def self_attn(act, weight, spec):
            return call(self_kernel, "self_attn", grid, [a_spec, spec], o_spec, o_shape,
                        2 * total * channels * 3 * width + 16 * total * n_tok * width)(act, weight)

        def cross_attn(act, kv, weight, spec, layer):
            kv_spec = pl.BlockSpec((1, 1, ctx_pad, 2 * width), lambda i: (layer, i, 0, 0))
            return call(functools.partial(cross_kernel, ctx_len), "cross_attn", grid, [a_spec, kv_spec, spec],
                        o_spec, o_shape, 2 * total * channels * width + 16 * total * 128 * width,
                        scratch=[pltpu.VMEM((width * 2, width), BF16),
                                 pltpu.VMEM((width * 2, 2 * (-(-width // 128) * 128)), BF16),
                                 pltpu.VMEM((n_tok, width * 2), BF16)])(act, kv, weight)

        def out_proj(hidden, mixed, weights, specs, vecs, name):
            return call(
                out_kernel, name, grid, [a_spec] + [o_spec] * 4 + specs + [vec_spec(3, channels)],
                [a_spec, a_spec], [h_shape, a_shape], 2 * total * channels * channels,
                scratch=[pltpu.VMEM((n_tok, SHARDS * width), BF16), pltpu.VMEM((SHARDS * width, channels), BF16)],
                aliases={0: 0},
            )(hidden, *mixed, *weights, vecs)

        def feed_forward(hidden, act, weight, layer, shard, vecs):
            packed = shard >= 2
            if packed:
                w_spec = pl.BlockSpec((dp_size, 3, ff // dp_size, channels), lambda i: (0, 0, 0, 0))
            else:
                w_spec = pl.BlockSpec((1, 3, ff, channels), lambda i: (layer, 0, 0, 0))
            specs = [a_spec, a_spec, w_spec, fixed_spec((2, ff), layer)]
            scratch = [pltpu.VMEM((n_tok, ff), BF16)]
            flops = 6 * total * channels * ff
            if vecs is None:
                return call(functools.partial(ff_kernel, packed), "ff", grid, specs, a_spec, h_shape,
                            flops, scratch, {0: 0})(hidden, act, weight, bias[shard])
            return call(functools.partial(ff_last_kernel, packed), "ff_last", grid, specs + [vec_spec(3, channels)],
                        [a_spec, a_spec], [h_shape, a_shape], flops, scratch, {0: 0})(
                        hidden, act, weight, bias[shard], vecs)

        def far_spec(slot):
            return pl.BlockSpec((dp_size, width // dp_size, channels), lambda i: (0, slot, 0))

        def four_specs(layer, slot):
            return [fixed_spec((width, channels), layer)] * 2 + [far_spec(slot)] * 2

        act, piece = tie(act, far_rest[0])
        full_rest.append(gather(piece))
        for layer in range(layers):
            vecs = block_vecs[layer]
            last = layer == layers - 1
            specs = [fixed_spec((3 * width, channels), layer)] * 2 + [fixed_spec((3 * width, channels), 0)] * 2
            m0 = self_attn(act, qkv_t, specs[0])
            if layer == 0:
                act, m0, piece = tie(act, m0, far_ff[0])
                full_ff.append(gather(piece))
                act, full = tie(act, full_qkv[0])
            else:
                act, m0, full = tie(act, m0, full_qkv[layer])
            rem = full[None]
            rem_sib = swap(rem, 1)
            m1 = self_attn(act, sib_qkv, specs[1])
            act, m1, rest = tie(act, m1, full_rest[layer])
            rest = rest.reshape(dp_size, -1, channels)
            rest_sib = swap(rest, 1)
            if not last:
                act, src_a, src_b, src_c, src_d = tie(act, qkv_t, o1_t, q2_t, o2_t)
                far_qkv.append(swap(dp_rows(src_a[layer + 1], 0), 2))
                far_rest.append(swap(jnp.concatenate([dp_rows(w[layer + 1], 0) for w in (src_b, src_c, src_d)]), 2))
            m2 = self_attn(act, rem, specs[2])
            m3 = self_attn(act, rem_sib, specs[3])
            hidden, act = out_proj(hidden, [m0, m1, m2, m3], [o1_t, sib_o1, rest, rest_sib],
                                   four_specs(layer, 0), jnp.stack([vecs[6], vecs[2], vecs[3]]), "out1")
            if not last:
                act, piece_a, piece_b, ff_src = tie(act, far_qkv[layer + 1], far_rest[layer + 1], ff_own)
                full_qkv.append(gather(piece_a))
                full_rest.append(gather(piece_b))
                far_ff.append(swap(dp_rows(ff_src[layer + 1], 1), 2))
            mixed = [cross_attn(act, part, weight, spec, layer) for part, weight, spec in
                     zip(kv_parts, [q2_t, sib_q2, rest, rest_sib], four_specs(layer, 1))]
            hidden, act = out_proj(hidden, mixed, [o2_t, sib_o2, rest, rest_sib],
                                   four_specs(layer, 2), jnp.stack([vecs[7], vecs[4], vecs[5]]), "out2")
            if not last:
                act, piece = tie(act, far_ff[layer + 1])
                full_ff.append(gather(piece))
            hidden = feed_forward(hidden, act, ff_own, layer, 0, None)
            hidden, act, full = tie(hidden, act, full_ff[layer])
            rem = full.reshape(dp_size, 3, ff // dp_size, channels)
            rem_sib = swap(rem, 1)
            hidden = feed_forward(hidden, act, sib_ff, layer, 1, None)
            hidden = feed_forward(hidden, act, rem, layer, 2, None)
            after = block_vecs[min(layer + 1, layers - 1)]
            hidden, act = feed_forward(hidden, act, rem_sib, layer, 3, jnp.stack([vecs[8], after[0], after[1]]))

        parts = call(
            end_kernel, "proj_out", grid,
            [a_spec, fixed_spec((channels, channels), 1), vec_spec(4, channels)] + [x_spec] * 4,
            pl.BlockSpec((tp_size, 1, tok, channels), lambda i: (0, i, 0, 0)),
            jax.ShapeDtypeStruct((tp_size, mine, tok, channels), BF16), 2 * total * channels * channels,
        )(hidden, w_proj, io_vecs, *x_parts)

        y = jnp.zeros((tp_size, mine, tok, channels), BF16)
        for m in range(tp_size):
            part = parts[m]
            part = part if m == 0 else swap(part, m)
            y = lax.dynamic_update_index_in_dim(y, part, me ^ m, 0)
        return y.reshape(batch, rows_loc, side, channels)

    act_spec = P("dp", "tp", None, None)
    in_specs = (act_spec, P("dp", None, None), P(), P(), P(),
                P(None, None, None, "tp", None), P(None, "tp", None, None),
                P(None, None, "tp", None), P(None, None, None, "tp", None),
                P(None, "tp", None, None), P(None, None, None, "tp"),
                P(None, None, "tp"), P(None, "tp", None))
    return jax.shard_map(shard_body, mesh=mesh, in_specs=in_specs, out_specs=act_spec, check_vma=False)
```

```python
import functools

import jax
import jax.numpy as jnp
from jax import lax
from jax.experimental import pallas as pl
from jax.experimental.pallas import tpu as pltpu
from jax.sharding import PartitionSpec as P


GROUPS = 32
GN_EPS = 1e-6
LN_EPS = 1e-5
SHARDS = 4
HEAD = 64
LOG2E = 1.4426950408889634
F32 = jnp.float32
BF16 = jnp.bfloat16
NT = (((1,), (1,)), ((), ()))
VMEM_LIMIT = 50 * 1024 * 1024


def layer_norm(hidden, ln_gain, ln_shift):
    average = jnp.mean(hidden, axis=-1, keepdims=True)
    centered = hidden - average
    variance = jnp.mean(centered * centered, axis=-1, keepdims=True)
    return (centered * lax.rsqrt(variance + LN_EPS) * ln_gain + ln_shift).astype(BF16)


def attend(q, k, v):
    scores = lax.dot_general(q, k, NT, preferred_element_type=F32)
    top = jnp.max(scores, axis=-1, keepdims=True)
    probs = jnp.exp2((scores - top) * (HEAD ** -0.5 * LOG2E)).astype(BF16)
    values = jnp.concatenate([v, jnp.ones_like(v)], axis=1)
    mixed = jnp.dot(probs, values, preferred_element_type=F32)
    return (mixed[:, :HEAD] / mixed[:, HEAD:]).astype(BF16)


def in_kernel(x0, x1, x2, x3, w_ref, io_ref, ln_ref, h_out, a_out):
    tok, channels = x0.shape[1:]
    parts = [ref[0].astype(F32) for ref in (x0, x1, x2, x3)]
    size = channels // GROUPS
    count = len(parts) * tok * size
    lanes = 128
    row = lax.broadcasted_iota(jnp.int32, (channels, lanes), 0)
    first = lax.broadcasted_iota(jnp.int32, (channels, lanes), 1) * size
    member = ((row >= first) & (row < first + size)).astype(F32)

    def group_average(columns):
        per_group = jnp.dot(jnp.broadcast_to(columns, (8, channels)), member,
                            precision=lax.Precision.HIGHEST, preferred_element_type=F32) / count
        return lax.dot_general(per_group, member, NT, precision=lax.Precision.HIGHEST,
                               preferred_element_type=F32)[0:1]

    mean = group_average(sum(jnp.sum(p, axis=0, keepdims=True) for p in parts))
    var = group_average(sum(jnp.sum((p - mean) * (p - mean), axis=0, keepdims=True) for p in parts))
    inverse = lax.rsqrt(var + GN_EPS)
    for i, p in enumerate(parts):
        normed = ((p - mean) * inverse * io_ref[0:1] + io_ref[1:2]).astype(BF16)
        h = jnp.dot(normed, w_ref[0], preferred_element_type=F32) + io_ref[2:3]
        h_out[0, i * tok:(i + 1) * tok, :] = h
        a_out[0, i * tok:(i + 1) * tok, :] = layer_norm(h, ln_ref[0:1], ln_ref[1:2])


def flat(ref):
    value = ref[...]
    return value.reshape(-1, value.shape[-1])


def self_kernel(a_ref, w_ref, o_ref):
    width = o_ref.shape[-1]
    qkv = lax.dot_general(a_ref[0], flat(w_ref), NT, preferred_element_type=F32).astype(BF16)
    for head in range(width // HEAD):
        lo = head * HEAD
        o_ref[0, :, lo:lo + HEAD] = attend(
            qkv[:, lo:lo + HEAD], qkv[:, width + lo:width + lo + HEAD],
            qkv[:, 2 * width + lo:2 * width + lo + HEAD])


def cross_kernel(valid, a_ref, kv_ref, wq_ref, o_ref, k_scr, v_scr, p_scr):
    width = o_ref.shape[-1]
    keys = kv_ref.shape[2]
    lanes = 128
    v_half = v_scr.shape[1] // 2
    q = lax.dot_general(a_ref[0], flat(wq_ref), NT, preferred_element_type=F32).astype(BF16)
    k_scr[...] = jnp.zeros_like(k_scr)
    v_scr[...] = jnp.zeros_like(v_scr)
    k, v = kv_ref[0, 0, :, :width], kv_ref[0, 0, :, width:]
    row = lax.broadcasted_iota(jnp.int32, (keys, width), 0)
    col = lax.broadcasted_iota(jnp.int32, (keys, width), 1)
    heads = width // HEAD
    for head in range(heads):
        lo = head * lanes
        inside = (col >= head * HEAD) & (col < (head + 1) * HEAD) & (row < valid)
        k_scr[lo:lo + keys, :] = jnp.where(inside, k, jnp.zeros_like(k))
        v_scr[lo:lo + keys, :width] = jnp.where(inside, v, jnp.zeros_like(v))
        v_scr[lo:lo + keys, v_half:v_half + width] = inside.astype(BF16)
    scores = lax.dot_general(q, k_scr[...], NT, preferred_element_type=F32)
    live = lax.broadcasted_iota(jnp.int32, (q.shape[0], lanes), 1) < valid
    for head in range(heads):
        sl = slice(head * lanes, (head + 1) * lanes)
        s = jnp.where(live, scores[:, sl], -jnp.inf)
        top = jnp.max(s, axis=-1, keepdims=True)
        p_scr[:, sl] = jnp.exp2((s - top) * (HEAD ** -0.5 * LOG2E)).astype(BF16)
    mixed = jnp.dot(p_scr[...], v_scr[...], preferred_element_type=F32)
    o_ref[0] = (mixed[:, :width] / mixed[:, v_half:v_half + width]).astype(BF16)


def out_kernel(h_ref, o0, o1, o2, o3, w0, w1, w2, w3, vec_ref, h_out, a_out, o_all, w_all):
    width = o0.shape[-1]
    for i, (o_ref, w_ref) in enumerate(((o0, w0), (o1, w1), (o2, w2), (o3, w3))):
        o_all[:, i * width:(i + 1) * width] = o_ref[0]
        w_all[i * width:(i + 1) * width, :] = flat(w_ref)
    h = h_ref[0] + jnp.dot(o_all[...], w_all[...], preferred_element_type=F32) + vec_ref[0:1]
    h_out[0] = h
    a_out[0] = layer_norm(h, vec_ref[1:2], vec_ref[2:3])


def ff_body(packed, a_ref, w_refs, b1_ref, m_scr):
    cols = 256
    channels = m_scr.shape[-1]
    a = a_ref[0]

    def weight(i, sl):
        if packed:
            return w_refs[0][:, i, :, sl].reshape(channels, -1)
        return w_refs[1][0, :, sl] if i == 2 else w_refs[0][0, i, :, sl]

    for j in range(m_scr.shape[-1] // cols):
        sl = slice(j * cols, (j + 1) * cols)
        u0 = jnp.dot(a, weight(0, sl), preferred_element_type=F32) + b1_ref[0, 0:1, sl]
        u1 = jnp.dot(a, weight(1, sl), preferred_element_type=F32) + b1_ref[0, 1:2, sl]
        gate = 0.5 * u1 * (1.0 + lax.erf(u1 * (0.5 ** 0.5)))
        m_scr[:, sl] = (u0 * gate).astype(BF16)
    return jnp.dot(m_scr[...], weight(2, slice(None)), preferred_element_type=F32)


def ff_kernel(packed, h_ref, a_ref, b1_ref, *refs):
    w_refs, (h_out, m_scr) = refs[:-2], refs[-2:]
    h_out[0] = h_ref[0] + ff_body(packed, a_ref, w_refs, b1_ref, m_scr)


def ff_last_kernel(h_ref, a_ref, b1_ref, w_ref, vec_ref, h_out, a_out, m_scr):
    h = h_ref[0] + ff_body(True, a_ref, (w_ref,), b1_ref, m_scr) + vec_ref[0:1]
    h_out[0] = h
    a_out[0] = layer_norm(h, vec_ref[1:2], vec_ref[2:3])


def ff_end_kernel(h_ref, a_ref, b1_ref, w_ref, vec_ref, wp_ref, io_ref, x0, x1, x2, x3, y_ref, m_scr):
    tok = x0.shape[1]
    h = h_ref[0] + ff_body(True, a_ref, (w_ref,), b1_ref, m_scr) + vec_ref[0:1]
    y = jnp.dot(h.astype(BF16), wp_ref[0], preferred_element_type=F32) + io_ref[3:4]
    for i, ref in enumerate((x0, x1, x2, x3)):
        y_ref[i, 0] = (y[i * tok:(i + 1) * tok] + ref[0].astype(F32)).astype(BF16)


def rows_spec(shape):
    return pl.BlockSpec((1,) + shape, lambda i: (i, 0, 0))


def fixed_spec(shape, layer):
    return pl.BlockSpec((1,) + shape, lambda i: (layer,) + (0,) * len(shape))


def vec_spec(rows, cols):
    return pl.BlockSpec((rows, cols), lambda i: (0, 0))


def call(kernel, grid, in_specs, out_specs, out_shape, flops, scratch=(), aliases=None):
    return pl.pallas_call(
        kernel, grid=grid, in_specs=in_specs, out_specs=out_specs, out_shape=out_shape,
        scratch_shapes=scratch, input_output_aliases=aliases or {},
        cost_estimate=pl.CostEstimate(flops=flops, bytes_accessed=16 << 20, transcendentals=0),
        compiler_params=pltpu.CompilerParams(vmem_limit_bytes=VMEM_LIMIT))


def tie(*values):
    return lax.optimization_barrier(values)


def solution(mesh):
    tp_size = mesh.shape["tp"]
    dp_size = mesh.shape["dp"]

    def swap(value, mask):
        return lax.ppermute(value, "tp", [(i, i ^ mask) for i in range(tp_size)])

    def body(latents, context, io_vecs, w_proj, block_vecs, w_qkv, w_o1, w_q2, w_kv2, w_o2, w_ff1, b_ff1, w_ff2):
        batch, rows_loc, side, channels = latents.shape
        tok = rows_loc * side
        layers = w_qkv.shape[0]
        width = w_o1.shape[1] * HEAD
        ff = w_ff2.shape[1]
        ctx_len = context.shape[1]
        ctx_pad = -(-ctx_len // 16) * 16
        mine = batch // tp_size
        n_tok = tp_size * tok
        me = lax.axis_index("tp")
        dp_me = lax.axis_index("dp")

        def piece_of(value, layer, axis):
            rows = value.shape[axis] // dp_size
            start = [0] * value.ndim
            start[0], start[axis] = layer, dp_me * rows
            size = list(value.shape)
            size[0], size[axis] = 1, rows
            return lax.dynamic_slice(value, start, size)

        def gather(piece):
            return lax.all_gather(piece, "dp", axis=0, tiled=True)

        qkv_t = w_qkv.transpose(0, 2, 3, 4, 1).reshape(layers, 3 * width, channels)
        q2_t = w_q2.transpose(0, 2, 3, 1).reshape(layers, width, channels)
        o1_t = w_o1.reshape(layers, width, channels)
        o2_t = w_o2.reshape(layers, width, channels)
        ff1_t = w_ff1.transpose(0, 2, 1, 3)

        def ff_piece(ff1, ff2, layer):
            return jnp.concatenate([piece_of(ff1, layer, 2)[0], piece_of(ff2, layer, 1)])

        x_rows = latents.reshape(tp_size, mine, tok, channels)

        def group_of(array, index):
            return lax.dynamic_index_in_dim(array, index, 0, keepdims=False)

        x_parts = [group_of(x_rows, me)] + [swap(group_of(x_rows, me ^ m), m) for m in (1, 2, 3)]
        far_qkv = swap(piece_of(qkv_t, 0, 1)[0], 2)
        far_rest = swap(jnp.concatenate([piece_of(w, 0, 1)[0] for w in (o1_t, q2_t, o2_t)]), 2)
        sib_qkv, sib_o1, sib_q2, sib_o2 = (
            swap(w, 1) for w in (qkv_t, o1_t, q2_t, o2_t))
        bias = [b_ff1] + [swap(b_ff1, m) for m in (1, 2, 3)]

        kv = jnp.einsum("blc,rcjhd->rbljhd", context, w_kv2, preferred_element_type=F32).astype(BF16)
        kv = kv.reshape(layers, batch, ctx_len, 2 * width)
        kv = jnp.pad(kv, ((0, 0), (0, 0), (0, ctx_pad - ctx_len), (0, 0)))
        kv_out = [lax.dynamic_slice_in_dim(kv, (me ^ m) * mine, mine, 1) for m in range(tp_size)]
        kv_parts = [kv_out[0]] + [swap(kv_out[m], m) for m in (1, 2, 3)]
        ff_src = ff_piece(ff1_t, w_ff2, 0)
        far_ff = swap(ff_src, 2)
        sib_ff1, sib_ff2 = swap(ff1_t, 1), swap(w_ff2, 1)
        x_parts = list(tie(*x_parts, ff_src, *kv_out))[:tp_size]

        grid = (mine,)
        total = mine * n_tok
        a_shape = jax.ShapeDtypeStruct((mine, n_tok, channels), BF16)
        h_shape = jax.ShapeDtypeStruct((mine, n_tok, channels), F32)
        o_shape = jax.ShapeDtypeStruct((mine, n_tok, width), BF16)
        a_spec, o_spec = rows_spec((n_tok, channels)), rows_spec((n_tok, width))
        x_spec = rows_spec((tok, channels))

        hidden, act = call(
            in_kernel, grid,
            [x_spec] * 4 + [fixed_spec((channels, channels), 0), vec_spec(4, channels), vec_spec(2, channels)],
            [a_spec, a_spec], [h_shape, a_shape], 2 * total * channels * channels,
        )(*x_parts, w_proj, io_vecs, block_vecs[0, 0:2])

        def self_attn(act, weight, spec):
            return call(self_kernel, grid, [a_spec, spec], o_spec, o_shape,
                        2 * total * channels * 3 * width + 16 * total * n_tok * width)(act, weight)

        def cross_attn(act, kv, weight, spec, layer):
            kv_spec = pl.BlockSpec((1, 1, ctx_pad, 2 * width), lambda i: (layer, i, 0, 0))
            return call(functools.partial(cross_kernel, ctx_len), grid, [a_spec, kv_spec, spec],
                        o_spec, o_shape, 2 * total * channels * width + 16 * total * 128 * width,
                        scratch=[pltpu.VMEM((width * 2, width), BF16),
                                 pltpu.VMEM((width * 2, 2 * (-(-width // 128) * 128)), BF16),
                                 pltpu.VMEM((n_tok, width * 2), BF16)])(act, kv, weight)

        def out_proj(hidden, mixed, weights, specs, vecs):
            return call(
                out_kernel, grid, [a_spec] + [o_spec] * 4 + specs + [vec_spec(3, channels)],
                [a_spec, a_spec], [h_shape, a_shape], 2 * total * channels * channels,
                scratch=[pltpu.VMEM((n_tok, SHARDS * width), BF16), pltpu.VMEM((SHARDS * width, channels), BF16)],
                aliases={0: 0},
            )(hidden, *mixed, *weights, vecs)

        far_ff_spec = pl.BlockSpec((dp_size, 3, ff // dp_size, channels), lambda i: (0, 0, 0, 0))
        ff_scratch = [pltpu.VMEM((n_tok, ff), BF16)]
        ff_flops = 6 * total * channels * ff

        def feed_forward(hidden, act, layer, shard, *weights):
            specs = [far_ff_spec]
            if len(weights) > 1:
                specs = [pl.BlockSpec((1, 2, channels, ff), lambda i: (layer, 0, 0, 0)), fixed_spec((ff, channels), layer)]
            return call(functools.partial(ff_kernel, len(weights) == 1), grid,
                        [a_spec, a_spec, fixed_spec((2, ff), layer)] + specs, a_spec, h_shape,
                        ff_flops, ff_scratch, {0: 0})(hidden, act, bias[shard], *weights)

        def far_spec(rows, slot):
            return pl.BlockSpec((dp_size, rows // dp_size, channels), lambda i: (0, slot, 0))

        def four_specs(layer, slot):
            return [fixed_spec((width, channels), layer)] * 2 + [far_spec(width, slot)] * 2

        act, piece = tie(act, far_qkv)
        full_qkv = gather(piece)
        for layer in range(layers):
            vecs = block_vecs[layer]
            specs = [fixed_spec((3 * width, channels), layer)] * 2 + [far_spec(3 * width, 0)] * 2
            m0 = self_attn(act, qkv_t, specs[0])
            if layer == 0:
                act, m0, piece = tie(act, m0, far_rest)
                full_rest = gather(piece)
                slot = 0
            else:
                act, m0, full_qkv = tie(act, m0, full_attn)
                slot = 3
            m1 = self_attn(act, sib_qkv, specs[1])
            act, m1, full = tie(act, m1, full_qkv)
            rem = full.reshape(dp_size, -1, channels)
            rem_sib = swap(rem, 1)
            if layer == 0:
                act, src_a, src_b, src_c, src_d = tie(act, qkv_t, o1_t, q2_t, o2_t)
                far_attn = swap(jnp.concatenate([piece_of(w, 1, 1)[0] for w in (src_a, src_b, src_c, src_d)]), 2)
                act, src_a, src_b = tie(act, ff1_t, w_ff2)
                far_ff1 = swap(ff_piece(src_a, src_b, 1), 2)
            m2 = self_attn(act, rem, specs[2])
            if layer == 0:
                act, m2, rest = tie(act, m2, full_rest)
                rest = rest.reshape(dp_size, -1, channels)
                rest_sib = swap(rest, 1)
            else:
                rest, rest_sib = rem, rem_sib
            m3 = self_attn(act, rem_sib, specs[3])
            hidden, act = out_proj(hidden, [m0, m1, m2, m3], [o1_t, sib_o1, rest, rest_sib],
                                   four_specs(layer, slot), jnp.stack([vecs[6], vecs[2], vecs[3]]))
            if layer == 0:
                act, piece = tie(act, far_ff)
                full_ff = gather(piece)
            mixed = [cross_attn(act, part, weight, spec, layer) for part, weight, spec in
                     zip(kv_parts, [q2_t, sib_q2, rest, rest_sib], four_specs(layer, slot + 1))]
            hidden, act = out_proj(hidden, mixed, [o2_t, sib_o2, rest, rest_sib],
                                   four_specs(layer, slot + 2), jnp.stack([vecs[7], vecs[4], vecs[5]]))
            if layer == 0:
                act, piece = tie(act, far_attn)
                full_attn = gather(piece)
            hidden = feed_forward(hidden, act, layer, 0, ff1_t, w_ff2)
            hidden = feed_forward(hidden, act, layer, 1, sib_ff1, sib_ff2)
            hidden, act, full = tie(hidden, act, full_ff)
            rem = full.reshape(dp_size, 3, ff // dp_size, channels)
            rem_sib = swap(rem, 1)
            if layer == 0:
                act, piece = tie(act, far_ff1)
                full_ff = gather(piece)
            hidden = feed_forward(hidden, act, layer, 2, rem)
            if layer < layers - 1:
                after = block_vecs[layer + 1]
                hidden, act = call(
                    ff_last_kernel, grid,
                    [a_spec, a_spec, fixed_spec((2, ff), layer), far_ff_spec, vec_spec(3, channels)],
                    [a_spec, a_spec], [h_shape, a_shape], ff_flops, ff_scratch, {0: 0},
                )(hidden, act, bias[3], rem_sib, jnp.stack([vecs[8], after[0], after[1]]))

        y = []
        for sample in range(mine):
            def one(shape, sample=sample):
                return pl.BlockSpec((1,) + shape, lambda i: (sample, 0, 0))

            parts = call(
                ff_end_kernel, (1,),
                [one((n_tok, channels))] * 2 + [fixed_spec((2, ff), layers - 1), far_ff_spec, vec_spec(1, channels),
                 fixed_spec((channels, channels), 1), vec_spec(4, channels)] + [one((tok, channels))] * 4,
                pl.BlockSpec((tp_size, 1, tok, channels), lambda i: (0, 0, 0, 0)),
                jax.ShapeDtypeStruct((tp_size, 1, tok, channels), BF16), ff_flops // mine, ff_scratch,
            )(hidden, act, bias[3], rem_sib, vecs[8:9], w_proj, io_vecs, *x_parts)
            y.append([parts[0]] + [swap(parts[m], m) for m in (1, 2, 3)])
            if sample < mine - 1:
                hidden, parts = tie(hidden, parts)
        out = jnp.zeros((tp_size, mine, tok, channels), BF16)
        for m in range(tp_size):
            for sample in range(mine):
                out = lax.dynamic_update_slice(out, y[sample][m][None], (me ^ m, sample, 0, 0))
        return out.reshape(batch, rows_loc, side, channels)

    act_spec = P("dp", "tp", None, None)
    in_specs = (act_spec, P("dp", None, None), P(), P(), P(),
                P(None, None, None, "tp", None), P(None, "tp", None, None),
                P(None, None, "tp", None), P(None, None, None, "tp", None),
                P(None, "tp", None, None), P(None, None, None, "tp"),
                P(None, None, "tp"), P(None, "tp", None))
    return jax.shard_map(body, mesh=mesh, in_specs=in_specs, out_specs=act_spec, check_vma=False)
```

```python
import functools

import jax
import jax.numpy as jnp
from jax import lax
from jax.experimental import pallas as pl
from jax.experimental.pallas import tpu as pltpu
from jax.sharding import PartitionSpec as P


GROUPS = 32
GN_EPS = 1e-6
LN_EPS = 1e-5
SHARDS = 4
HEAD = 64
LOG2E = 1.4426950408889634
F32 = jnp.float32
BF16 = jnp.bfloat16
NT = (((1,), (1,)), ((), ()))
VMEM_LIMIT = 50 * 1024 * 1024


def layer_norm(hidden, ln_gain, ln_shift):
    average = jnp.mean(hidden, axis=-1, keepdims=True)
    centered = hidden - average
    variance = jnp.mean(centered * centered, axis=-1, keepdims=True)
    return (centered * lax.rsqrt(variance + LN_EPS) * ln_gain + ln_shift).astype(BF16)


def attend(q, k, v):
    scores = lax.dot_general(q, k, NT, preferred_element_type=F32)
    top = jnp.max(scores, axis=-1, keepdims=True)
    probs = jnp.exp2((scores - top) * (HEAD ** -0.5 * LOG2E)).astype(BF16)
    values = jnp.concatenate([v, jnp.ones_like(v)], axis=1)
    mixed = jnp.dot(probs, values, preferred_element_type=F32)
    return (mixed[:, :HEAD] / mixed[:, HEAD:]).astype(BF16)


def in_kernel(x0, x1, x2, x3, w_ref, io_ref, ln_ref, h_out, a_out):
    tok, channels = x0.shape[1:]
    parts = [ref[0].astype(F32) for ref in (x0, x1, x2, x3)]
    size = channels // GROUPS
    count = len(parts) * tok * size
    lanes = 128
    row = lax.broadcasted_iota(jnp.int32, (channels, lanes), 0)
    first = lax.broadcasted_iota(jnp.int32, (channels, lanes), 1) * size
    member = ((row >= first) & (row < first + size)).astype(F32)

    def group_average(columns):
        per_group = jnp.dot(jnp.broadcast_to(columns, (8, channels)), member,
                            precision=lax.Precision.HIGHEST, preferred_element_type=F32) / count
        return lax.dot_general(per_group, member, NT, precision=lax.Precision.HIGHEST,
                               preferred_element_type=F32)[0:1]

    mean = group_average(sum(jnp.sum(p, axis=0, keepdims=True) for p in parts))
    var = group_average(sum(jnp.sum((p - mean) * (p - mean), axis=0, keepdims=True) for p in parts))
    inverse = lax.rsqrt(var + GN_EPS)
    for i, p in enumerate(parts):
        normed = ((p - mean) * inverse * io_ref[0:1] + io_ref[1:2]).astype(BF16)
        h = jnp.dot(normed, w_ref[0], preferred_element_type=F32) + io_ref[2:3]
        h_out[0, i * tok:(i + 1) * tok, :] = h
        a_out[0, i * tok:(i + 1) * tok, :] = layer_norm(h, ln_ref[0:1], ln_ref[1:2])


def flat(ref):
    value = ref[...]
    return value.reshape(-1, value.shape[-1])


def self_kernel(a_ref, w_ref, o_ref):
    width = o_ref.shape[-1]
    qkv = lax.dot_general(a_ref[0], flat(w_ref), NT, preferred_element_type=F32).astype(BF16)
    for head in range(width // HEAD):
        lo = head * HEAD
        o_ref[0, :, lo:lo + HEAD] = attend(
            qkv[:, lo:lo + HEAD], qkv[:, width + lo:width + lo + HEAD],
            qkv[:, 2 * width + lo:2 * width + lo + HEAD])


def row_copies(own, sib, rest, rest_sib, layer, slot, dst, sem):
    width = own.shape[1]
    pieces = rest.shape[0]
    rows = width // pieces
    pairs = [(ref.at[layer], dst.at[pl.ds(i * width, width)]) for i, ref in enumerate((own, sib))]
    for i, ref in ((2, rest), (3, rest_sib)):
        pairs += [(ref.at[d, pl.ds(slot * rows, rows)], dst.at[pl.ds(i * width + d * rows, rows)]) for d in range(pieces)]
    return [pltpu.make_async_copy(src, to, sem) for src, to in pairs]


def mid_kernel(valid, layer, slot, h_ref, o0, o1, o2, o3, kv0, kv1, kv2, kv3, vec_ref,
               o1_own, o1_sib, q2_own, q2_sib, o2_own, o2_sib, rest, rest_sib,
               h_out, a_out, o_all, w_out1, w_q, w_out2, k_scr, v_scr, p_scr, sems):
    step = pl.program_id(0)
    width = o0.shape[-1]
    heads = width // HEAD
    keys = kv0.shape[2]
    lanes = 128
    group = k_scr.shape[2] // HEAD
    cols = group * HEAD
    copies = [row_copies(own, sib, rest, rest_sib, layer, slot + i, dst, sems.at[i]) for i, (own, sib, dst) in enumerate(
        ((o1_own, o1_sib, w_out1), (q2_own, q2_sib, w_q), (o2_own, o2_sib, w_out2)))]

    def wait(i):
        @pl.when(step == 0)
        def _():
            for copy in copies[i]:
                copy.wait()

    @pl.when(step == 0)
    def _():
        for some in copies:
            for copy in some:
                copy.start()
        k_scr[...] = jnp.zeros_like(k_scr)
        v_scr[...] = jnp.zeros_like(v_scr)

    @pl.when(step % 2 == 0)
    def _():
        live = lax.broadcasted_iota(jnp.int32, (keys, HEAD), 0) < valid
        for shard, ref in enumerate((kv0, kv1, kv2, kv3)):
            kv = ref[0, 0]
            for head in range(heads):
                place = shard * heads + head
                g, r = place // group, place % group
                rows = slice(r * lanes, r * lanes + keys)
                at = slice(r * HEAD, (r + 1) * HEAD)
                k_scr[g, rows, at] = kv[:, head * HEAD:(head + 1) * HEAD]
                v_scr[g, rows, at] = kv[:, width + head * HEAD:width + (head + 1) * HEAD]
                v_scr[g, rows, cols + r * HEAD:cols + (r + 1) * HEAD] = live.astype(BF16)

    for i, o_ref in enumerate((o0, o1, o2, o3)):
        o_all[:, i * width:(i + 1) * width] = o_ref[0]
    wait(0)
    h = h_ref[0] + jnp.dot(o_all[...], w_out1[...], preferred_element_type=F32) + vec_ref[0:1]
    act = layer_norm(h, vec_ref[1:2], vec_ref[2:3])
    wait(1)
    q = lax.dot_general(act, w_q[...], NT, preferred_element_type=F32).astype(BF16)
    live = lax.broadcasted_iota(jnp.int32, (q.shape[0], lanes), 1) < valid
    for g in range(k_scr.shape[0]):
        at = slice(g * cols, (g + 1) * cols)
        scores = lax.dot_general(q[:, at], k_scr[g], NT, preferred_element_type=F32)
        for r in range(group):
            sl = slice(r * lanes, (r + 1) * lanes)
            s = jnp.where(live, scores[:, sl], -jnp.inf)
            top = jnp.max(s, axis=-1, keepdims=True)
            p_scr[g, :, sl] = jnp.exp2((s - top) * (HEAD ** -0.5 * LOG2E)).astype(BF16)
        mixed = jnp.dot(p_scr[g], v_scr[g], preferred_element_type=F32)
        o_all[:, at] = (mixed[:, :cols] / mixed[:, cols:]).astype(BF16)
    wait(2)
    h = h + jnp.dot(o_all[...], w_out2[...], preferred_element_type=F32) + vec_ref[3:4]
    h_out[0] = h
    a_out[0] = layer_norm(h, vec_ref[4:5], vec_ref[5:6])


FF_COLS = 256


def ff_copies(layer, refs, w1, w2, sems):
    chunks = w2.shape[0] // FF_COLS
    groups = []
    for j in range(chunks):
        at = pl.ds(j * FF_COLS, FF_COLS)
        if len(refs) == 2:
            pairs = [(refs[0].at[layer, :, :, at], w1.at[:, :, at])]
        else:
            rows = refs[0].shape[2]
            pairs = [(refs[0].at[d, pl.ds(0, 2), :, at], w1.at[:, pl.ds(d * rows, rows), at]) for d in range(refs[0].shape[0])]
        groups.append([pltpu.make_async_copy(src, to, sems.at[j]) for src, to in pairs])
    if len(refs) == 2:
        pairs = [(refs[1].at[layer], w2)]
    else:
        rows = refs[0].shape[2]
        pairs = [(refs[0].at[d, 2], w2.at[pl.ds(d * rows, rows)]) for d in range(refs[0].shape[0])]
    groups.append([pltpu.make_async_copy(src, to, sems.at[chunks]) for src, to in pairs])
    return groups


def ff_steps(layer, a_ref, b1_ref, refs, w1, w2, m_scr, sems, finish):
    step = pl.program_id(0)
    groups = ff_copies(layer, refs, w1, w2, sems)

    def run(first):
        if first:
            for some in groups:
                for copy in some:
                    copy.start()
        a = a_ref[0]
        for j, some in enumerate(groups[:-1]):
            if first:
                for copy in some:
                    copy.wait()
            sl = slice(j * FF_COLS, (j + 1) * FF_COLS)
            u0 = jnp.dot(a, w1[0, :, sl], preferred_element_type=F32) + b1_ref[0, 0:1, sl]
            u1 = jnp.dot(a, w1[1, :, sl], preferred_element_type=F32) + b1_ref[0, 1:2, sl]
            gate = 0.5 * u1 * (1.0 + lax.erf(u1 * (0.5 ** 0.5)))
            m_scr[:, sl] = (u0 * gate).astype(BF16)
        if first:
            for copy in groups[-1]:
                copy.wait()
        finish(jnp.dot(m_scr[...], w2[...], preferred_element_type=F32), first)

    pl.when(step == 0)(functools.partial(run, True))
    pl.when(step > 0)(functools.partial(run, False))


def ff_kernel(layer, h_ref, a_ref, b1_ref, *rest):
    refs, (h_out, w1, w2, m_scr, sems) = rest[:-5], rest[-5:]

    def finish(update, first):
        h_out[0] = h_ref[0] + update

    ff_steps(layer, a_ref, b1_ref, refs, w1, w2, m_scr, sems, finish)


def ff_last_kernel(layer, h_ref, a_ref, b1_ref, vec_ref, w_ref, h_out, a_out, w1, w2, m_scr, sems):
    def finish(update, first):
        h = h_ref[0] + update + vec_ref[0:1]
        h_out[0] = h
        a_out[0] = layer_norm(h, vec_ref[1:2], vec_ref[2:3])

    ff_steps(layer, a_ref, b1_ref, (w_ref,), w1, w2, m_scr, sems, finish)


def ff_end_kernel(layer, h_ref, a_ref, b1_ref, vec_ref, io_ref, x0, x1, x2, x3, wp_ref, w_ref, y_ref,
                  w1, w2, m_scr, wp, sems):
    tok = x0.shape[1]
    last = pltpu.make_async_copy(wp_ref.at[1], wp, sems.at[sems.shape[0] - 1])

    @pl.when(pl.program_id(0) == 0)
    def _():
        last.start()

    def finish(update, first):
        h = h_ref[0] + update + vec_ref[0:1]
        if first:
            last.wait()
        y = jnp.dot(h.astype(BF16), wp[...], preferred_element_type=F32) + io_ref[3:4]
        for i, ref in enumerate((x0, x1) if first else (x2, x3)):
            y_ref[i, 0] = (y[i * tok:(i + 1) * tok] + ref[0].astype(F32)).astype(BF16)

    ff_steps(layer, a_ref, b1_ref, (w_ref,), w1, w2, m_scr, sems, finish)


def rows_spec(shape):
    return pl.BlockSpec((1,) + shape, lambda i: (i, 0, 0))


def fixed_spec(shape, layer):
    return pl.BlockSpec((1,) + shape, lambda i: (layer,) + (0,) * len(shape))


def vec_spec(rows, cols):
    return pl.BlockSpec((rows, cols), lambda i: (0, 0))


def call(kernel, grid, in_specs, out_specs, out_shape, flops, scratch=(), aliases=None):
    return pl.pallas_call(
        kernel, grid=grid, in_specs=in_specs, out_specs=out_specs, out_shape=out_shape,
        scratch_shapes=scratch, input_output_aliases=aliases or {},
        cost_estimate=pl.CostEstimate(flops=flops, bytes_accessed=16 << 20, transcendentals=0),
        compiler_params=pltpu.CompilerParams(vmem_limit_bytes=VMEM_LIMIT))


def tie(*values):
    return lax.optimization_barrier(values)


def solution(mesh):
    tp_size = mesh.shape["tp"]
    dp_size = mesh.shape["dp"]

    def swap(value, mask):
        return lax.ppermute(value, "tp", [(i, i ^ mask) for i in range(tp_size)])

    def body(latents, context, io_vecs, w_proj, block_vecs, w_qkv, w_o1, w_q2, w_kv2, w_o2, w_ff1, b_ff1, w_ff2):
        batch, rows_loc, side, channels = latents.shape
        tok = rows_loc * side
        layers = w_qkv.shape[0]
        width = w_o1.shape[1] * HEAD
        ff = w_ff2.shape[1]
        ctx_len = context.shape[1]
        ctx_pad = -(-ctx_len // 16) * 16
        mine = batch // tp_size
        n_tok = tp_size * tok
        me = lax.axis_index("tp")
        dp_me = lax.axis_index("dp")

        def piece_of(value, layer, axis):
            rows = value.shape[axis] // dp_size
            start = [0] * value.ndim
            start[0], start[axis] = layer, dp_me * rows
            size = list(value.shape)
            size[0], size[axis] = 1, rows
            return lax.dynamic_slice(value, start, size)

        def gather(piece):
            return lax.all_gather(piece, "dp", axis=0, tiled=True)

        qkv_t = w_qkv.transpose(0, 2, 3, 4, 1).reshape(layers, 3 * width, channels)
        q2_t = w_q2.transpose(0, 2, 3, 1).reshape(layers, width, channels)
        o1_t = w_o1.reshape(layers, width, channels)
        o2_t = w_o2.reshape(layers, width, channels)
        ff1_t = w_ff1.transpose(0, 2, 1, 3)

        def ff_piece(ff1, ff2, layer):
            return jnp.concatenate([piece_of(ff1, layer, 2)[0], piece_of(ff2, layer, 1)])

        x_rows = latents.reshape(tp_size, mine, tok, channels)

        def group_of(array, index):
            return lax.dynamic_index_in_dim(array, index, 0, keepdims=False)

        x_parts = [group_of(x_rows, me)] + [swap(group_of(x_rows, me ^ m), m) for m in (1, 2, 3)]
        far_qkv = swap(piece_of(qkv_t, 0, 1)[0], 2)
        far_rest = swap(jnp.concatenate([piece_of(w, 0, 1)[0] for w in (o1_t, q2_t, o2_t)]), 2)
        sib_qkv, sib_o1, sib_q2, sib_o2 = (
            swap(w, 1) for w in (qkv_t, o1_t, q2_t, o2_t))
        bias = [b_ff1] + [swap(b_ff1, m) for m in (1, 2, 3)]

        kv = jnp.einsum("blc,rcjhd->rbljhd", context, w_kv2, preferred_element_type=F32).astype(BF16)
        kv = kv.reshape(layers, batch, ctx_len, 2 * width)
        kv = jnp.pad(kv, ((0, 0), (0, 0), (0, ctx_pad - ctx_len), (0, 0)))
        kv_out = [lax.dynamic_slice_in_dim(kv, (me ^ m) * mine, mine, 1) for m in range(tp_size)]
        kv_parts = [kv_out[0]] + [swap(kv_out[m], m) for m in (1, 2, 3)]
        ff_src = ff_piece(ff1_t, w_ff2, 0)
        far_ff = swap(ff_src, 2)
        sib_ff1, sib_ff2 = swap(ff1_t, 1), swap(w_ff2, 1)
        x_parts = list(tie(*x_parts, ff_src, *kv_out))[:tp_size]
        *x_parts, piece = tie(*x_parts, far_qkv)
        full_qkv = gather(piece)

        grid = (mine,)
        total = mine * n_tok
        a_shape = jax.ShapeDtypeStruct((mine, n_tok, channels), BF16)
        h_shape = jax.ShapeDtypeStruct((mine, n_tok, channels), F32)
        o_shape = jax.ShapeDtypeStruct((mine, n_tok, width), BF16)
        a_spec, o_spec = rows_spec((n_tok, channels)), rows_spec((n_tok, width))
        x_spec = rows_spec((tok, channels))

        hidden, act = call(
            in_kernel, grid,
            [x_spec] * 4 + [fixed_spec((channels, channels), 0), vec_spec(4, channels), vec_spec(2, channels)],
            [a_spec, a_spec], [h_shape, a_shape], 2 * total * channels * channels,
        )(*x_parts, w_proj, io_vecs, block_vecs[0, 0:2])

        def self_attn(act, weight, spec):
            return call(self_kernel, grid, [a_spec, spec], o_spec, o_shape,
                        2 * total * channels * 3 * width + 16 * total * n_tok * width)(act, weight)

        tile = n_tok // 2
        tiles = (2 * mine,)
        t_spec = pl.BlockSpec((1, tile, channels), lambda i: (i // 2, i % 2, 0))
        any_spec = pl.BlockSpec(memory_space=pl.ANY)
        group = 4
        cross_groups = SHARDS * width // (group * HEAD)

        def middle(hidden, mixed, vecs, layer, slot, rest, rest_sib):
            ot_spec = pl.BlockSpec((1, tile, width), lambda i: (i // 2, i % 2, 0))
            kv_spec = pl.BlockSpec((1, 1, ctx_pad, 2 * width), lambda i: (layer, i // 2, 0, 0))
            square = pltpu.VMEM((channels, channels), BF16)
            return call(
                functools.partial(mid_kernel, ctx_len, layer, slot), tiles,
                [t_spec] + [ot_spec] * 4 + [kv_spec] * 4 + [vec_spec(6, channels)] + [any_spec] * 8,
                [t_spec, t_spec], [h_shape, a_shape], 8 * total * channels * channels,
                [pltpu.VMEM((tile, channels), BF16), square, square, square,
                 pltpu.VMEM((cross_groups, group * 128, group * HEAD), BF16),
                 pltpu.VMEM((cross_groups, group * 128, 2 * group * HEAD), BF16),
                 pltpu.VMEM((cross_groups, tile, group * 128), BF16),
                 pltpu.SemaphoreType.DMA((3,))], {0: 0},
            )(hidden, *mixed, *kv_parts, vecs, o1_t, sib_o1, q2_t, sib_q2, o2_t, sib_o2, rest, rest_sib)

        chunks = ff // FF_COLS
        ff_scratch = [pltpu.VMEM((2, channels, ff), BF16), pltpu.VMEM((ff, channels), BF16), pltpu.VMEM((tile, ff), BF16)]
        ff_flops = 6 * total * channels * ff

        def feed_forward(hidden, act, layer, shard, *weights):
            return call(functools.partial(ff_kernel, layer), tiles,
                        [t_spec, t_spec, fixed_spec((2, ff), layer)] + [any_spec] * len(weights), t_spec, h_shape,
                        ff_flops, ff_scratch + [pltpu.SemaphoreType.DMA((chunks + 1,))],
                        {0: 0})(hidden, act, bias[shard], *weights)

        def far_spec(rows, slot):
            return pl.BlockSpec((dp_size, rows // dp_size, channels), lambda i: (0, slot, 0))

        for layer in range(layers):
            vecs = block_vecs[layer]
            specs = [fixed_spec((3 * width, channels), layer)] * 2 + [far_spec(3 * width, 0)] * 2
            m0 = self_attn(act, qkv_t, specs[0])
            if layer == 0:
                act, m0, piece = tie(act, m0, far_rest)
                full_rest = gather(piece)
                slot = 0
            else:
                act, m0, full_qkv = tie(act, m0, full_attn)
                slot = 3
            m1 = self_attn(act, sib_qkv, specs[1])
            act, m1, full = tie(act, m1, full_qkv)
            rem = full.reshape(dp_size, -1, channels)
            rem_sib = swap(rem, 1)
            if layer == 0:
                act, src_a, src_b, src_c, src_d = tie(act, qkv_t, o1_t, q2_t, o2_t)
                far_attn = swap(jnp.concatenate([piece_of(w, 1, 1)[0] for w in (src_a, src_b, src_c, src_d)]), 2)
                act, src_a, src_b = tie(act, ff1_t, w_ff2)
                far_ff1 = swap(ff_piece(src_a, src_b, 1), 2)
            m2 = self_attn(act, rem, specs[2])
            if layer == 0:
                act, m2, rest, piece = tie(act, m2, full_rest, far_ff)
                rest = rest.reshape(dp_size, -1, channels)
                rest_sib = swap(rest, 1)
                full_ff = gather(piece)
            else:
                rest, rest_sib = rem, rem_sib
            m3 = self_attn(act, rem_sib, specs[3])
            hidden, act = middle(hidden, [m0, m1, m2, m3], jnp.stack([vecs[i] for i in (6, 2, 3, 7, 4, 5)]),
                                 layer, slot, rest, rest_sib)
            if layer == 0:
                act, piece = tie(act, far_attn)
                full_attn = gather(piece)
            hidden = feed_forward(hidden, act, layer, 0, ff1_t, w_ff2)
            if layer == 0:
                hidden, piece = tie(hidden, far_ff1)
                next_ff = gather(piece)
            hidden = feed_forward(hidden, act, layer, 1, sib_ff1, sib_ff2)
            hidden, act, full = tie(hidden, act, full_ff)
            rem = full.reshape(dp_size, 3, ff // dp_size, channels)
            rem_sib = swap(rem, 1)
            hidden = feed_forward(hidden, act, layer, 2, rem)
            if layer < layers - 1:
                full_ff = next_ff
                after = block_vecs[layer + 1]
                hidden, act = call(
                    functools.partial(ff_last_kernel, layer), tiles,
                    [t_spec, t_spec, fixed_spec((2, ff), layer), vec_spec(3, channels), any_spec],
                    [t_spec, t_spec], [h_shape, a_shape], ff_flops,
                    ff_scratch + [pltpu.SemaphoreType.DMA((chunks + 1,))], {0: 0},
                )(hidden, act, bias[3], jnp.stack([vecs[8], after[0], after[1]]), rem_sib)

        y = []
        for sample in range(mine):
            row_spec = pl.BlockSpec((1, tile, channels), lambda i, sample=sample: (sample, i, 0))
            x_spec = pl.BlockSpec((1, tok, channels), lambda i, sample=sample: (sample, 0, 0))
            parts = call(
                functools.partial(ff_end_kernel, layers - 1), (2,),
                [row_spec, row_spec, fixed_spec((2, ff), layers - 1), vec_spec(1, channels), vec_spec(4, channels)]
                + [x_spec] * 4 + [any_spec] * 2,
                pl.BlockSpec((tp_size // 2, 1, tok, channels), lambda i: (i, 0, 0, 0)),
                jax.ShapeDtypeStruct((tp_size, 1, tok, channels), BF16), ff_flops // mine,
                ff_scratch + [pltpu.VMEM((channels, channels), BF16), pltpu.SemaphoreType.DMA((chunks + 2,))],
                None,
            )(hidden, act, bias[3], vecs[8:9], io_vecs, *x_parts, w_proj, rem_sib)
            y.append([parts[0]] + [swap(parts[m], m) for m in (1, 2, 3)])
            if sample < mine - 1:
                hidden, parts = tie(hidden, parts)
        out = jnp.zeros((tp_size, mine, tok, channels), BF16)
        for m in range(tp_size):
            for sample in range(mine):
                out = lax.dynamic_update_slice(out, y[sample][m][None], (me ^ m, sample, 0, 0))
        return out.reshape(batch, rows_loc, side, channels)

    act_spec = P("dp", "tp", None, None)
    in_specs = (act_spec, P("dp", None, None), P(), P(), P(),
                P(None, None, None, "tp", None), P(None, "tp", None, None),
                P(None, None, "tp", None), P(None, None, None, "tp", None),
                P(None, "tp", None, None), P(None, None, None, "tp"),
                P(None, None, "tp"), P(None, "tp", None))
    return jax.shard_map(body, mesh=mesh, in_specs=in_specs, out_specs=act_spec, check_vma=False)
```

```python
import functools

import jax
import jax.numpy as jnp
from jax import lax
from jax.experimental import pallas as pl
from jax.experimental.pallas import tpu as pltpu
from jax.sharding import PartitionSpec as P


GROUPS = 32
GN_EPS = 1e-6
LN_EPS = 1e-5
SHARDS = 4
HEAD = 64
LOG2E = 1.4426950408889634
F32 = jnp.float32
BF16 = jnp.bfloat16
NT = (((1,), (1,)), ((), ()))
VMEM_LIMIT = 50 * 1024 * 1024


def layer_norm(hidden, ln_gain, ln_shift):
    average = jnp.mean(hidden, axis=-1, keepdims=True)
    centered = hidden - average
    variance = jnp.mean(centered * centered, axis=-1, keepdims=True)
    return (centered * lax.rsqrt(variance + LN_EPS) * ln_gain + ln_shift).astype(BF16)


def attend(q, k, v):
    scores = lax.dot_general(q, k, NT, preferred_element_type=F32)
    top = jnp.max(scores, axis=-1, keepdims=True)
    probs = jnp.exp2((scores - top) * (HEAD ** -0.5 * LOG2E)).astype(BF16)
    values = jnp.concatenate([v, jnp.ones_like(v)], axis=1)
    mixed = jnp.dot(probs, values, preferred_element_type=F32)
    return (mixed[:, :HEAD] / mixed[:, HEAD:]).astype(BF16)


def in_kernel(x0, x1, x2, x3, w_ref, io_ref, ln_ref, h_out, a_out):
    tok, channels = x0.shape[1:]
    parts = [ref[0].astype(F32) for ref in (x0, x1, x2, x3)]
    size = channels // GROUPS
    count = len(parts) * tok * size
    lanes = 128
    row = lax.broadcasted_iota(jnp.int32, (channels, lanes), 0)
    first = lax.broadcasted_iota(jnp.int32, (channels, lanes), 1) * size
    member = ((row >= first) & (row < first + size)).astype(F32)

    def group_average(columns):
        per_group = jnp.dot(jnp.broadcast_to(columns, (8, channels)), member,
                            precision=lax.Precision.HIGHEST, preferred_element_type=F32) / count
        return lax.dot_general(per_group, member, NT, precision=lax.Precision.HIGHEST,
                               preferred_element_type=F32)[0:1]

    mean = group_average(sum(jnp.sum(p, axis=0, keepdims=True) for p in parts))
    var = group_average(sum(jnp.sum((p - mean) * (p - mean), axis=0, keepdims=True) for p in parts))
    inverse = lax.rsqrt(var + GN_EPS)
    for i, p in enumerate(parts):
        normed = ((p - mean) * inverse * io_ref[0:1] + io_ref[1:2]).astype(BF16)
        h = jnp.dot(normed, w_ref[0], preferred_element_type=F32) + io_ref[2:3]
        h_out[0, i * tok:(i + 1) * tok, :] = h
        a_out[0, i * tok:(i + 1) * tok, :] = layer_norm(h, ln_ref[0:1], ln_ref[1:2])


def flat(ref):
    value = ref[...]
    return value.reshape(-1, value.shape[-1])


def self_kernel(a_ref, w_ref, o_ref):
    width = o_ref.shape[-1]
    qkv = lax.dot_general(a_ref[0], flat(w_ref), NT, preferred_element_type=F32).astype(BF16)
    for head in range(width // HEAD):
        lo = head * HEAD
        o_ref[0, :, lo:lo + HEAD] = attend(
            qkv[:, lo:lo + HEAD], qkv[:, width + lo:width + lo + HEAD],
            qkv[:, 2 * width + lo:2 * width + lo + HEAD])


def row_copies(own, sib, rest, rest_sib, layer, slot, dst, sem):
    width = own.shape[1]
    pieces = rest.shape[0]
    rows = width // pieces
    pairs = [(ref.at[layer], dst.at[pl.ds(i * width, width)]) for i, ref in enumerate((own, sib))]
    for i, ref in ((2, rest), (3, rest_sib)):
        pairs += [(ref.at[d, pl.ds(slot * rows, rows)], dst.at[pl.ds(i * width + d * rows, rows)]) for d in range(pieces)]
    return [pltpu.make_async_copy(src, to, sem) for src, to in pairs]


def mid_kernel(valid, layer, slot, h_ref, o0, o1, o2, o3, kv0, kv1, kv2, kv3, vec_ref,
               o1_own, o1_sib, q2_own, q2_sib, o2_own, o2_sib, rest, rest_sib,
               h_out, a_out, o_all, w_out1, w_q, w_out2, k_scr, v_scr, p_scr, sems):
    step = pl.program_id(0)
    width = o0.shape[-1]
    heads = width // HEAD
    keys = kv0.shape[2]
    lanes = 128
    group = k_scr.shape[2] // HEAD
    cols = group * HEAD
    copies = [row_copies(own, sib, rest, rest_sib, layer, slot + i, dst, sems.at[i]) for i, (own, sib, dst) in enumerate(
        ((o1_own, o1_sib, w_out1), (q2_own, q2_sib, w_q), (o2_own, o2_sib, w_out2)))]

    def wait(i):
        @pl.when(step == 0)
        def _():
            for copy in copies[i]:
                copy.wait()

    @pl.when(step == 0)
    def _():
        for some in copies:
            for copy in some:
                copy.start()
        k_scr[...] = jnp.zeros_like(k_scr)
        v_scr[...] = jnp.zeros_like(v_scr)

    @pl.when(step % 2 == 0)
    def _():
        live = lax.broadcasted_iota(jnp.int32, (keys, HEAD), 0) < valid
        for shard, ref in enumerate((kv0, kv1, kv2, kv3)):
            kv = ref[0, 0]
            for head in range(heads):
                place = shard * heads + head
                g, r = place // group, place % group
                rows = slice(r * lanes, r * lanes + keys)
                at = slice(r * HEAD, (r + 1) * HEAD)
                k_scr[g, rows, at] = kv[:, head * HEAD:(head + 1) * HEAD]
                v_scr[g, rows, at] = kv[:, width + head * HEAD:width + (head + 1) * HEAD]
                v_scr[g, rows, cols + r * HEAD:cols + (r + 1) * HEAD] = live.astype(BF16)

    for i, o_ref in enumerate((o0, o1, o2, o3)):
        o_all[:, i * width:(i + 1) * width] = o_ref[0]
    wait(0)
    h = h_ref[0] + jnp.dot(o_all[...], w_out1[...], preferred_element_type=F32) + vec_ref[0:1]
    act = layer_norm(h, vec_ref[1:2], vec_ref[2:3])
    wait(1)
    q = lax.dot_general(act, w_q[...], NT, preferred_element_type=F32).astype(BF16)
    live = lax.broadcasted_iota(jnp.int32, (q.shape[0], lanes), 1) < valid
    for g in range(k_scr.shape[0]):
        at = slice(g * cols, (g + 1) * cols)
        scores = lax.dot_general(q[:, at], k_scr[g], NT, preferred_element_type=F32)
        for r in range(group):
            sl = slice(r * lanes, (r + 1) * lanes)
            s = jnp.where(live, scores[:, sl], -jnp.inf)
            top = jnp.max(s, axis=-1, keepdims=True)
            p_scr[g, :, sl] = jnp.exp2((s - top) * (HEAD ** -0.5 * LOG2E)).astype(BF16)
        mixed = jnp.dot(p_scr[g], v_scr[g], preferred_element_type=F32)
        o_all[:, at] = (mixed[:, :cols] / mixed[:, cols:]).astype(BF16)
    wait(2)
    h = h + jnp.dot(o_all[...], w_out2[...], preferred_element_type=F32) + vec_ref[3:4]
    h_out[0] = h
    a_out[0] = layer_norm(h, vec_ref[4:5], vec_ref[5:6])


FF_COLS = 256


def ff_copies(layer, shards, w1, w2, sems):
    ff = w1.shape[3]
    chunks = ff // FF_COLS
    first, second = [], []
    for n, refs in enumerate(shards):
        for j in range(chunks):
            at = pl.ds(j * FF_COLS, FF_COLS)
            if len(refs) == 2:
                first.append([(refs[0].at[layer, :, :, at], w1.at[n, :, :, at])])
            else:
                rows = refs[0].shape[2]
                first.append([(refs[0].at[d, pl.ds(0, 2), :, at], w1.at[n, :, pl.ds(d * rows, rows), at])
                              for d in range(refs[0].shape[0])])
        if len(refs) == 2:
            second.append([(refs[1].at[layer], w2.at[pl.ds(n * ff, ff)])])
        else:
            rows = refs[0].shape[2]
            second.append([(refs[0].at[d, 2], w2.at[pl.ds(n * ff + d * rows, rows)]) for d in range(refs[0].shape[0])])
    return [[pltpu.make_async_copy(src, to, sems.at[i]) for src, to in pairs] for i, pairs in enumerate(first + second)]


def ff_steps(layer, a_ref, biases, shards, w1, w2, m_scr, sems, finish):
    step = pl.program_id(0)
    groups = ff_copies(layer, shards, w1, w2, sems)
    ff = w1.shape[3]
    chunks = ff // FF_COLS
    ahead = 2

    def start(i):
        for copy in groups[i] if i < len(groups) else ():
            copy.start()

    def run(first):
        if first:
            for i in range(ahead):
                start(i)
        a = a_ref[0]
        for n, b1_ref in enumerate(biases):
            for j in range(chunks):
                if first:
                    start(n * chunks + j + ahead)
                    for copy in groups[n * chunks + j]:
                        copy.wait()
                sl = slice(j * FF_COLS, (j + 1) * FF_COLS)
                u0 = jnp.dot(a, w1[n, 0, :, sl], preferred_element_type=F32) + b1_ref[0, 0:1, sl]
                u1 = jnp.dot(a, w1[n, 1, :, sl], preferred_element_type=F32) + b1_ref[0, 1:2, sl]
                gate = 0.5 * u1 * (1.0 + lax.erf(u1 * (0.5 ** 0.5)))
                m_scr[:, n * ff + j * FF_COLS:n * ff + (j + 1) * FF_COLS] = (u0 * gate).astype(BF16)
        if first:
            for some in groups[len(biases) * chunks:]:
                for copy in some:
                    copy.wait()
        finish(jnp.dot(m_scr[...], w2[...], preferred_element_type=F32), first)

    pl.when(step == 0)(functools.partial(run, True))
    pl.when(step > 0)(functools.partial(run, False))


def ff_pair_kernel(layer, h_ref, a_ref, b0_ref, b1_ref, own1, own2, sib1, sib2, h_out, w1, w2, m_scr, sems):
    def finish(update, first):
        h_out[0] = h_ref[0] + update

    ff_steps(layer, a_ref, (b0_ref, b1_ref), ((own1, own2), (sib1, sib2)), w1, w2, m_scr, sems, finish)


def ff_kernel(layer, h_ref, a_ref, b1_ref, w_ref, h_out, w1, w2, m_scr, sems):
    def finish(update, first):
        h_out[0] = h_ref[0] + update

    ff_steps(layer, a_ref, (b1_ref,), ((w_ref,),), w1, w2, m_scr, sems, finish)


def ff_last_kernel(layer, h_ref, a_ref, b1_ref, vec_ref, w_ref, h_out, a_out, w1, w2, m_scr, sems):
    def finish(update, first):
        h = h_ref[0] + update + vec_ref[0:1]
        h_out[0] = h
        a_out[0] = layer_norm(h, vec_ref[1:2], vec_ref[2:3])

    ff_steps(layer, a_ref, (b1_ref,), ((w_ref,),), w1, w2, m_scr, sems, finish)


def ff_end_kernel(layer, h_ref, a_ref, b1_ref, vec_ref, io_ref, x0, x1, x2, x3, wp_ref, w_ref, y_ref,
                  w1, w2, m_scr, wp, wp_sem, sems):
    tok = x0.shape[1]
    last = pltpu.make_async_copy(wp_ref.at[1], wp, wp_sem.at[0])

    @pl.when(pl.program_id(0) == 0)
    def _():
        last.start()

    def finish(update, first):
        h = h_ref[0] + update + vec_ref[0:1]
        if first:
            last.wait()
        y = jnp.dot(h.astype(BF16), wp[...], preferred_element_type=F32) + io_ref[3:4]
        for i, ref in enumerate((x0, x1) if first else (x2, x3)):
            y_ref[i, 0] = (y[i * tok:(i + 1) * tok] + ref[0].astype(F32)).astype(BF16)

    ff_steps(layer, a_ref, (b1_ref,), ((w_ref,),), w1, w2, m_scr, sems, finish)


def rows_spec(shape):
    return pl.BlockSpec((1,) + shape, lambda i: (i, 0, 0))


def fixed_spec(shape, layer):
    return pl.BlockSpec((1,) + shape, lambda i: (layer,) + (0,) * len(shape))


def vec_spec(rows, cols):
    return pl.BlockSpec((rows, cols), lambda i: (0, 0))


def call(kernel, grid, in_specs, out_specs, out_shape, flops, scratch=(), aliases=None):
    return pl.pallas_call(
        kernel, grid=grid, in_specs=in_specs, out_specs=out_specs, out_shape=out_shape,
        scratch_shapes=scratch, input_output_aliases=aliases or {},
        cost_estimate=pl.CostEstimate(flops=flops, bytes_accessed=16 << 20, transcendentals=0),
        compiler_params=pltpu.CompilerParams(vmem_limit_bytes=VMEM_LIMIT))


def tie(*values):
    return lax.optimization_barrier(values)


def solution(mesh):
    tp_size = mesh.shape["tp"]
    dp_size = mesh.shape["dp"]

    def swap(value, mask):
        return lax.ppermute(value, "tp", [(i, i ^ mask) for i in range(tp_size)])

    def body(latents, context, io_vecs, w_proj, block_vecs, w_qkv, w_o1, w_q2, w_kv2, w_o2, w_ff1, b_ff1, w_ff2):
        batch, rows_loc, side, channels = latents.shape
        tok = rows_loc * side
        layers = w_qkv.shape[0]
        width = w_o1.shape[1] * HEAD
        ff = w_ff2.shape[1]
        ctx_len = context.shape[1]
        ctx_pad = -(-ctx_len // 16) * 16
        mine = batch // tp_size
        n_tok = tp_size * tok
        me = lax.axis_index("tp")
        dp_me = lax.axis_index("dp")

        def piece_of(value, layer, axis):
            rows = value.shape[axis] // dp_size
            start = [0] * value.ndim
            start[0], start[axis] = layer, dp_me * rows
            size = list(value.shape)
            size[0], size[axis] = 1, rows
            return lax.dynamic_slice(value, start, size)

        def gather(piece):
            return lax.all_gather(piece, "dp", axis=0, tiled=True)

        qkv_t = w_qkv.transpose(0, 2, 3, 4, 1).reshape(layers, 3 * width, channels)
        q2_t = w_q2.transpose(0, 2, 3, 1).reshape(layers, width, channels)
        o1_t = w_o1.reshape(layers, width, channels)
        o2_t = w_o2.reshape(layers, width, channels)
        ff1_t = w_ff1.transpose(0, 2, 1, 3)

        def ff_piece(ff1, ff2, layer):
            return jnp.concatenate([piece_of(ff1, layer, 2)[0], piece_of(ff2, layer, 1)])

        x_rows = latents.reshape(tp_size, mine, tok, channels)

        def group_of(array, index):
            return lax.dynamic_index_in_dim(array, index, 0, keepdims=False)

        x_parts = [group_of(x_rows, me)] + [swap(group_of(x_rows, me ^ m), m) for m in (1, 2, 3)]
        far_qkv = swap(piece_of(qkv_t, 0, 1)[0], 2)
        far_rest = swap(jnp.concatenate([piece_of(w, 0, 1)[0] for w in (o1_t, q2_t, o2_t)]), 2)
        sib_qkv, sib_o1, sib_q2, sib_o2 = (
            swap(w, 1) for w in (qkv_t, o1_t, q2_t, o2_t))
        bias = [b_ff1] + [swap(b_ff1, m) for m in (1, 2, 3)]

        kv = jnp.einsum("blc,rcjhd->rbljhd", context, w_kv2, preferred_element_type=F32).astype(BF16)
        kv = kv.reshape(layers, batch, ctx_len, 2 * width)
        kv = jnp.pad(kv, ((0, 0), (0, 0), (0, ctx_pad - ctx_len), (0, 0)))
        kv_out = [lax.dynamic_slice_in_dim(kv, (me ^ m) * mine, mine, 1) for m in range(tp_size)]
        kv_out[0], piece = tie(kv_out[0], far_qkv)
        full_qkv = gather(piece)
        kv_parts = [kv_out[0]] + [swap(kv_out[m], m) for m in (1, 2, 3)]
        ff_src = ff_piece(ff1_t, w_ff2, 0)
        far_ff = swap(ff_src, 2)
        sib_ff1, sib_ff2 = swap(ff1_t, 1), swap(w_ff2, 1)
        x_parts = list(tie(*x_parts, ff_src, *kv_out))[:tp_size]

        grid = (mine,)
        total = mine * n_tok
        a_shape = jax.ShapeDtypeStruct((mine, n_tok, channels), BF16)
        h_shape = jax.ShapeDtypeStruct((mine, n_tok, channels), F32)
        o_shape = jax.ShapeDtypeStruct((mine, n_tok, width), BF16)
        a_spec, o_spec = rows_spec((n_tok, channels)), rows_spec((n_tok, width))
        x_spec = rows_spec((tok, channels))

        hidden, act = call(
            in_kernel, grid,
            [x_spec] * 4 + [fixed_spec((channels, channels), 0), vec_spec(4, channels), vec_spec(2, channels)],
            [a_spec, a_spec], [h_shape, a_shape], 2 * total * channels * channels,
        )(*x_parts, w_proj, io_vecs, block_vecs[0, 0:2])

        def self_attn(act, weight, spec):
            return call(self_kernel, grid, [a_spec, spec], o_spec, o_shape,
                        2 * total * channels * 3 * width + 16 * total * n_tok * width)(act, weight)

        tile = n_tok // 2
        tiles = (2 * mine,)
        t_spec = pl.BlockSpec((1, tile, channels), lambda i: (i // 2, i % 2, 0))
        any_spec = pl.BlockSpec(memory_space=pl.ANY)
        group = 4
        cross_groups = SHARDS * width // (group * HEAD)

        def middle(hidden, mixed, vecs, layer, slot, rest, rest_sib):
            ot_spec = pl.BlockSpec((1, tile, width), lambda i: (i // 2, i % 2, 0))
            kv_spec = pl.BlockSpec((1, 1, ctx_pad, 2 * width), lambda i: (layer, i // 2, 0, 0))
            square = pltpu.VMEM((channels, channels), BF16)
            return call(
                functools.partial(mid_kernel, ctx_len, layer, slot), tiles,
                [t_spec] + [ot_spec] * 4 + [kv_spec] * 4 + [vec_spec(6, channels)] + [any_spec] * 8,
                [t_spec, t_spec], [h_shape, a_shape], 8 * total * channels * channels,
                [pltpu.VMEM((tile, channels), BF16), square, square, square,
                 pltpu.VMEM((cross_groups, group * 128, group * HEAD), BF16),
                 pltpu.VMEM((cross_groups, group * 128, 2 * group * HEAD), BF16),
                 pltpu.VMEM((cross_groups, tile, group * 128), BF16),
                 pltpu.SemaphoreType.DMA((3,))], {0: 0},
            )(hidden, *mixed, *kv_parts, vecs, o1_t, sib_o1, q2_t, sib_q2, o2_t, sib_o2, rest, rest_sib)

        chunks = ff // FF_COLS
        ff_flops = 6 * total * channels * ff

        def ff_scratch(n, *more):
            return [pltpu.VMEM((n, 2, channels, ff), BF16), pltpu.VMEM((n * ff, channels), BF16),
                    pltpu.VMEM((tile, n * ff), BF16), *more, pltpu.SemaphoreType.DMA((n * (chunks + 1),))]

        b_spec = [fixed_spec((2, ff), layer) for layer in range(layers)]

        def feed_forward_pair(hidden, act, layer):
            return call(functools.partial(ff_pair_kernel, layer), tiles,
                        [t_spec, t_spec] + [b_spec[layer]] * 2 + [any_spec] * 4, t_spec, h_shape,
                        2 * ff_flops, ff_scratch(2), {0: 0})(
                        hidden, act, bias[0], bias[1], ff1_t, w_ff2, sib_ff1, sib_ff2)

        def feed_forward(hidden, act, layer, shard, weight):
            return call(functools.partial(ff_kernel, layer), tiles,
                        [t_spec, t_spec, b_spec[layer], any_spec], t_spec, h_shape,
                        ff_flops, ff_scratch(1), {0: 0})(hidden, act, bias[shard], weight)

        def far_spec(rows, slot):
            return pl.BlockSpec((dp_size, rows // dp_size, channels), lambda i: (0, slot, 0))

        act, piece = tie(act, far_rest)
        full_rest = gather(piece)
        for layer in range(layers):
            vecs = block_vecs[layer]
            specs = [fixed_spec((3 * width, channels), layer)] * 2 + [far_spec(3 * width, 0)] * 2
            m0 = self_attn(act, qkv_t, specs[0])
            act, m0 = tie(act, m0)
            m1 = self_attn(act, sib_qkv, specs[1])
            act, m1, full = tie(act, m1, full_qkv)
            rem = full.reshape(dp_size, -1, channels)
            rem_sib = swap(rem, 1)
            if layer == 0:
                act, src_a, src_b, src_c = tie(act, qkv_t, ff1_t, w_ff2)
                far_qkv = swap(piece_of(src_a, 1, 1)[0], 2)
                far_ff1 = swap(ff_piece(src_b, src_c, 1), 2)
            m2 = self_attn(act, rem, specs[2])
            if layer == 0:
                act, m2, rest = tie(act, m2, full_rest)
                rest = rest.reshape(dp_size, -1, channels)
            rest_sib = swap(rest, 1)
            if layer == 0:
                act, *src = tie(act, o1_t, q2_t, o2_t)
                next_rest = swap(jnp.concatenate([w[1].reshape(dp_size, -1, channels) for w in src], axis=1), 2)
            m3 = self_attn(act, rem_sib, specs[3])
            if layer == 0:
                act, m3, piece = tie(act, m3, far_ff)
                full_ff = gather(piece)
            hidden, act = middle(hidden, [m0, m1, m2, m3], jnp.stack([vecs[i] for i in (6, 2, 3, 7, 4, 5)]),
                                 layer, 0, rest, rest_sib)
            if layer == 0:
                act, piece = tie(act, far_qkv)
                full_qkv = gather(piece)
            hidden = feed_forward_pair(hidden, act, layer)
            hidden, act, full = tie(hidden, act, full_ff)
            rem = full.reshape(dp_size, 3, ff // dp_size, channels)
            rem_sib = swap(rem, 1)
            hidden = feed_forward(hidden, act, layer, 2, rem)
            if layer == 0:
                hidden, piece, rest = tie(hidden, far_ff1, next_rest)
                next_ff = gather(piece)
            if layer < layers - 1:
                full_ff = next_ff
                after = block_vecs[layer + 1]
                hidden, act = call(
                    functools.partial(ff_last_kernel, layer), tiles,
                    [t_spec, t_spec, b_spec[layer], vec_spec(3, channels), any_spec],
                    [t_spec, t_spec], [h_shape, a_shape], ff_flops,
                    ff_scratch(1), {0: 0},
                )(hidden, act, bias[3], jnp.stack([vecs[8], after[0], after[1]]), rem_sib)

        y = []
        for sample in range(mine):
            row_spec = pl.BlockSpec((1, tile, channels), lambda i, sample=sample: (sample, i, 0))
            x_spec = pl.BlockSpec((1, tok, channels), lambda i, sample=sample: (sample, 0, 0))
            parts = call(
                functools.partial(ff_end_kernel, layers - 1), (2,),
                [row_spec, row_spec, b_spec[layers - 1], vec_spec(1, channels), vec_spec(4, channels)]
                + [x_spec] * 4 + [any_spec] * 2,
                pl.BlockSpec((tp_size // 2, 1, tok, channels), lambda i: (i, 0, 0, 0)),
                jax.ShapeDtypeStruct((tp_size, 1, tok, channels), BF16), ff_flops // mine,
                ff_scratch(1, pltpu.VMEM((channels, channels), BF16), pltpu.SemaphoreType.DMA((1,))),
                None,
            )(hidden, act, bias[3], vecs[8:9], io_vecs, *x_parts, w_proj, rem_sib)
            y.append([parts[0]] + [swap(parts[m], m) for m in (1, 2, 3)])
            if sample < mine - 1:
                hidden, parts = tie(hidden, parts)
        out = jnp.zeros((tp_size, mine, tok, channels), BF16)
        for m in range(tp_size):
            for sample in range(mine):
                out = lax.dynamic_update_slice(out, y[sample][m][None], (me ^ m, sample, 0, 0))
        return out.reshape(batch, rows_loc, side, channels)

    act_spec = P("dp", "tp", None, None)
    in_specs = (act_spec, P("dp", None, None), P(), P(), P(),
                P(None, None, None, "tp", None), P(None, "tp", None, None),
                P(None, None, "tp", None), P(None, None, None, "tp", None),
                P(None, "tp", None, None), P(None, None, None, "tp"),
                P(None, None, "tp"), P(None, "tp", None))
    return jax.shard_map(body, mesh=mesh, in_specs=in_specs, out_specs=act_spec, check_vma=False)
```

```python
import functools

import jax
import jax.numpy as jnp
from jax import lax
from jax.experimental import pallas as pl
from jax.experimental.pallas import tpu as pltpu
from jax.sharding import PartitionSpec as P


GROUPS = 32
GN_EPS = 1e-6
LN_EPS = 1e-5
SHARDS = 4
HEAD = 64
LOG2E = 1.4426950408889634
F32 = jnp.float32
BF16 = jnp.bfloat16
NT = (((1,), (1,)), ((), ()))
VMEM_LIMIT = 67043328


def layer_norm(hidden, ln_gain, ln_shift):
    average = jnp.mean(hidden, axis=-1, keepdims=True)
    centered = hidden - average
    variance = jnp.mean(centered * centered, axis=-1, keepdims=True)
    return (centered * lax.rsqrt(variance + LN_EPS) * ln_gain + ln_shift).astype(BF16)


def attend(q, k, v):
    scores = lax.dot_general(q, k, NT, preferred_element_type=F32)
    top = jnp.max(scores, axis=-1, keepdims=True)
    probs = jnp.exp2((scores - top) * (HEAD ** -0.5 * LOG2E)).astype(BF16)
    values = jnp.concatenate([v, jnp.ones_like(v)], axis=1)
    mixed = jnp.dot(probs, values, preferred_element_type=F32)
    return (mixed[:, :HEAD] / mixed[:, HEAD:]).astype(BF16)


def in_kernel(x0, x1, x2, x3, w_ref, io_ref, ln_ref, h_out, a_out, g_scr):
    tok, channels = x0.shape[1:]
    parts = [ref[0].astype(F32) for ref in (x0, x1, x2, x3)]
    size = channels // GROUPS
    count = len(parts) * tok * size
    lanes = 128
    row = lax.broadcasted_iota(jnp.int32, (channels, lanes), 0)
    first = lax.broadcasted_iota(jnp.int32, (channels, lanes), 1) * size
    member = ((row >= first) & (row < first + size)).astype(F32)

    def group_average(columns):
        per_group = jnp.dot(jnp.broadcast_to(columns, (8, channels)), member,
                            precision=lax.Precision.HIGHEST, preferred_element_type=F32) / count
        return lax.dot_general(per_group, member, NT, precision=lax.Precision.HIGHEST,
                               preferred_element_type=F32)[0:1]

    mean = group_average(sum(jnp.sum(p, axis=0, keepdims=True) for p in parts))
    var = group_average(sum(jnp.sum((p - mean) * (p - mean), axis=0, keepdims=True) for p in parts))
    inverse = lax.rsqrt(var + GN_EPS)
    for i, p in enumerate(parts):
        g_scr[i * tok:(i + 1) * tok, :] = ((p - mean) * inverse * io_ref[0:1] + io_ref[1:2]).astype(BF16)
    h = jnp.dot(g_scr[...], w_ref[0], preferred_element_type=F32) + io_ref[2:3]
    h_out[0] = h
    a_out[0] = layer_norm(h, ln_ref[0:1], ln_ref[1:2])


def self_kernel(layer, a_ref, own_ref, sib_ref, o0, o1, w, sems):
    width = o0.shape[-1]
    copies = []
    for n, ref in enumerate((own_ref, sib_ref)):
        if ref.shape[1] == w.shape[1]:
            pairs = [(ref.at[layer], w.at[n])]
        else:
            rows = ref.shape[1]
            pairs = [(ref.at[d], w.at[n, pl.ds(d * rows, rows)]) for d in range(ref.shape[0])]
        copies.append([pltpu.make_async_copy(src, to, sems.at[n]) for src, to in pairs])

    @pl.when(pl.program_id(0) == 0)
    def _():
        for some in copies:
            for copy in some:
                copy.start()

    for n, o_ref in enumerate((o0, o1)):
        @pl.when(pl.program_id(0) == 0)
        def _():
            for copy in copies[n]:
                copy.wait()

        qkv = lax.dot_general(a_ref[0], w[n], NT, preferred_element_type=F32).astype(BF16)
        for head in range(width // HEAD):
            lo = head * HEAD
            o_ref[0, :, lo:lo + HEAD] = attend(
                qkv[:, lo:lo + HEAD], qkv[:, width + lo:width + lo + HEAD],
                qkv[:, 2 * width + lo:2 * width + lo + HEAD])


def row_copies(own, sib, rest, rest_sib, layer, slot, dst, sem):
    width = own.shape[1]
    pieces = rest.shape[0]
    rows = width // pieces
    pairs = [(ref.at[layer], dst.at[pl.ds(i * width, width)]) for i, ref in enumerate((own, sib))]
    for i, ref in ((2, rest), (3, rest_sib)):
        pairs += [(ref.at[d, pl.ds(slot * rows, rows)], dst.at[pl.ds(i * width + d * rows, rows)]) for d in range(pieces)]
    return [pltpu.make_async_copy(src, to, sem) for src, to in pairs]


def mid_kernel(valid, layer, slot, h_ref, o0, o1, o2, o3, kv0, kv1, kv2, kv3, vec_ref,
               o1_own, o1_sib, q2_own, q2_sib, o2_own, o2_sib, rest, rest_sib,
               h_out, a_out, o_all, w_out1, w_q, w_out2, k_scr, v_scr, p_scr, sems):
    step = pl.program_id(0)
    width = o0.shape[-1]
    heads = width // HEAD
    keys = kv0.shape[2]
    lanes = 128
    group = k_scr.shape[2] // HEAD
    cols = group * HEAD
    copies = [row_copies(own, sib, rest, rest_sib, layer, slot + i, dst, sems.at[i]) for i, (own, sib, dst) in enumerate(
        ((o1_own, o1_sib, w_out1), (q2_own, q2_sib, w_q), (o2_own, o2_sib, w_out2)))]

    def wait(i):
        @pl.when(step == 0)
        def _():
            for copy in copies[i]:
                copy.wait()

    @pl.when(step == 0)
    def _():
        for some in copies:
            for copy in some:
                copy.start()
        k_scr[...] = jnp.zeros_like(k_scr)
        v_scr[...] = jnp.zeros_like(v_scr)

    @pl.when(step % 2 == 0)
    def _():
        live = lax.broadcasted_iota(jnp.int32, (keys, HEAD), 0) < valid
        for shard, ref in enumerate((kv0, kv1, kv2, kv3)):
            kv = ref[0, 0]
            for head in range(heads):
                place = shard * heads + head
                g, r = place // group, place % group
                rows = slice(r * lanes, r * lanes + keys)
                at = slice(r * HEAD, (r + 1) * HEAD)
                k_scr[g, rows, at] = kv[:, head * HEAD:(head + 1) * HEAD]
                v_scr[g, rows, at] = kv[:, width + head * HEAD:width + (head + 1) * HEAD]
                v_scr[g, rows, cols + r * HEAD:cols + (r + 1) * HEAD] = live.astype(BF16)

    for i, o_ref in enumerate((o0, o1, o2, o3)):
        o_all[:, i * width:(i + 1) * width] = o_ref[0]
    wait(0)
    h = h_ref[0] + jnp.dot(o_all[...], w_out1[...], preferred_element_type=F32) + vec_ref[0:1]
    act = layer_norm(h, vec_ref[1:2], vec_ref[2:3])
    wait(1)
    q = lax.dot_general(act, w_q[...], NT, preferred_element_type=F32).astype(BF16)
    live = lax.broadcasted_iota(jnp.int32, (q.shape[0], lanes), 1) < valid
    for g in range(k_scr.shape[0]):
        at = slice(g * cols, (g + 1) * cols)
        scores = lax.dot_general(q[:, at], k_scr[g], NT, preferred_element_type=F32)
        for r in range(group):
            sl = slice(r * lanes, (r + 1) * lanes)
            s = jnp.where(live, scores[:, sl], -jnp.inf)
            top = jnp.max(s, axis=-1, keepdims=True)
            p_scr[g, :, sl] = jnp.exp2((s - top) * (HEAD ** -0.5 * LOG2E)).astype(BF16)
        mixed = jnp.dot(p_scr[g], v_scr[g], preferred_element_type=F32)
        o_all[:, at] = (mixed[:, :cols] / mixed[:, cols:]).astype(BF16)
    wait(2)
    h = h + jnp.dot(o_all[...], w_out2[...], preferred_element_type=F32) + vec_ref[3:4]
    h_out[0] = h
    a_out[0] = layer_norm(h, vec_ref[4:5], vec_ref[5:6])


FF_COLS = 256


def ff_copies(layer, shards, w1, w2, sems):
    ff = w1.shape[3]
    chunks = ff // FF_COLS
    first, second = [], []
    for n, refs in enumerate(shards):
        for j in range(chunks):
            at = pl.ds(j * FF_COLS, FF_COLS)
            if len(refs) == 2:
                first.append([(refs[0].at[layer, :, :, at], w1.at[n, :, :, at])])
            else:
                rows = refs[0].shape[2]
                first.append([(refs[0].at[d, pl.ds(0, 2), :, at], w1.at[n, :, pl.ds(d * rows, rows), at])
                              for d in range(refs[0].shape[0])])
        if len(refs) == 2:
            second.append([(refs[1].at[layer], w2.at[pl.ds(n * ff, ff)])])
        else:
            rows = refs[0].shape[2]
            second.append([(refs[0].at[d, 2], w2.at[pl.ds(n * ff + d * rows, rows)]) for d in range(refs[0].shape[0])])
    return [[pltpu.make_async_copy(src, to, sems.at[i]) for src, to in pairs] for i, pairs in enumerate(first + second)]


def ff_steps(layer, a_ref, biases, shards, w1, w2, m_scr, sems, finish):
    step = pl.program_id(0)
    groups = ff_copies(layer, shards, w1, w2, sems)
    ff = w1.shape[3]
    chunks = ff // FF_COLS
    ahead = 2 * chunks

    def start(i):
        for copy in groups[i] if i < len(groups) else ():
            copy.start()

    def run(first):
        if first:
            for i in range(ahead):
                start(i)
        a = a_ref[0]
        for n, b1_ref in enumerate(biases):
            for j in range(chunks):
                if first:
                    start(n * chunks + j + ahead)
                    for copy in groups[n * chunks + j]:
                        copy.wait()
                sl = slice(j * FF_COLS, (j + 1) * FF_COLS)
                u0 = jnp.dot(a, w1[n, 0, :, sl], preferred_element_type=F32) + b1_ref[0, 0:1, sl]
                u1 = jnp.dot(a, w1[n, 1, :, sl], preferred_element_type=F32) + b1_ref[0, 1:2, sl]
                gate = 0.5 * u1 * (1.0 + lax.erf(u1 * (0.5 ** 0.5)))
                m_scr[:, n * ff + j * FF_COLS:n * ff + (j + 1) * FF_COLS] = (u0 * gate).astype(BF16)
        if first:
            for some in groups[len(biases) * chunks:]:
                for copy in some:
                    copy.wait()
        finish(jnp.dot(m_scr[...], w2[...], preferred_element_type=F32), first)

    pl.when(step == 0)(functools.partial(run, True))
    pl.when(step > 0)(functools.partial(run, False))


def ff_kernel(layer, kinds, h_ref, a_ref, *rest):
    biases, refs = rest[:len(kinds)], list(rest[len(kinds):-5])
    h_out, w1, w2, m_scr, sems = rest[-5:]
    shards = [[refs.pop(0) for _ in range(kind)] for kind in kinds]

    def finish(update, first):
        h_out[0] = h_ref[0] + update

    ff_steps(layer, a_ref, biases, shards, w1, w2, m_scr, sems, finish)


def ff_last_kernel(layer, h_ref, a_ref, b1_ref, vec_ref, w_ref, h_out, a_out, w1, w2, m_scr, sems):
    def finish(update, first):
        h = h_ref[0] + update + vec_ref[0:1]
        h_out[0] = h
        a_out[0] = layer_norm(h, vec_ref[1:2], vec_ref[2:3])

    ff_steps(layer, a_ref, (b1_ref,), ((w_ref,),), w1, w2, m_scr, sems, finish)


def ff_end_kernel(layer, h_ref, a_ref, b0_ref, b1_ref, vec_ref, io_ref, x0, x1, x2, x3, wp_ref, w0_ref, w1_ref, y_ref,
                  w1, w2, m_scr, wp, wp_sem, sems):
    tok = x0.shape[1]
    last = pltpu.make_async_copy(wp_ref.at[1], wp, wp_sem.at[0])

    @pl.when(pl.program_id(0) == 0)
    def _():
        last.start()

    def finish(update, first):
        h = h_ref[0] + update + vec_ref[0:1]
        if first:
            last.wait()
        y = jnp.dot(h.astype(BF16), wp[...], preferred_element_type=F32) + io_ref[3:4]
        for i, ref in enumerate((x0, x1) if first else (x2, x3)):
            y_ref[i, 0] = (y[i * tok:(i + 1) * tok] + ref[0].astype(F32)).astype(BF16)

    ff_steps(layer, a_ref, (b0_ref, b1_ref), ((w0_ref,), (w1_ref,)), w1, w2, m_scr, sems, finish)


def rows_spec(shape):
    return pl.BlockSpec((1,) + shape, lambda i: (i, 0, 0))


def fixed_spec(shape, layer):
    return pl.BlockSpec((1,) + shape, lambda i: (layer,) + (0,) * len(shape))


def vec_spec(rows, cols):
    return pl.BlockSpec((rows, cols), lambda i: (0, 0))


def call(kernel, grid, in_specs, out_specs, out_shape, flops, scratch=(), aliases=None):
    return pl.pallas_call(
        kernel, grid=grid, in_specs=in_specs, out_specs=out_specs, out_shape=out_shape,
        scratch_shapes=scratch, input_output_aliases=aliases or {},
        cost_estimate=pl.CostEstimate(flops=flops, bytes_accessed=16 << 20, transcendentals=0),
        compiler_params=pltpu.CompilerParams(vmem_limit_bytes=VMEM_LIMIT))


def tie(*values):
    return lax.optimization_barrier(values)


def solution(mesh):
    tp_size = mesh.shape["tp"]
    dp_size = mesh.shape["dp"]

    def swap(value, mask):
        return lax.ppermute(value, "tp", [(i, i ^ mask) for i in range(tp_size)])

    def body(latents, context, io_vecs, w_proj, block_vecs, w_qkv, w_o1, w_q2, w_kv2, w_o2, w_ff1, b_ff1, w_ff2):
        batch, rows_loc, side, channels = latents.shape
        tok = rows_loc * side
        layers = w_qkv.shape[0]
        width = w_o1.shape[1] * HEAD
        ff = w_ff2.shape[1]
        ctx_len = context.shape[1]
        ctx_pad = -(-ctx_len // 16) * 16
        mine = batch // tp_size
        n_tok = tp_size * tok
        me = lax.axis_index("tp")
        dp_me = lax.axis_index("dp")

        def piece_of(value, layer, axis):
            rows = value.shape[axis] // dp_size
            start = [0] * value.ndim
            start[0], start[axis] = layer, dp_me * rows
            size = list(value.shape)
            size[0], size[axis] = 1, rows
            return lax.dynamic_slice(value, start, size)

        def gather(piece):
            return lax.all_gather(piece, "dp", axis=0, tiled=True)

        qkv_t = w_qkv.transpose(0, 2, 3, 4, 1).reshape(layers, 3 * width, channels)
        q2_t = w_q2.transpose(0, 2, 3, 1).reshape(layers, width, channels)
        o1_t = w_o1.reshape(layers, width, channels)
        o2_t = w_o2.reshape(layers, width, channels)
        ff1_t = w_ff1.transpose(0, 2, 1, 3)

        def ff_piece(ff1, ff2, layer):
            return jnp.concatenate([piece_of(ff1, layer, 2)[0], piece_of(ff2, layer, 1)])

        x_rows = latents.reshape(tp_size, mine, tok, channels)

        def group_of(array, index):
            return lax.dynamic_index_in_dim(array, index, 0, keepdims=False)

        x_parts = [group_of(x_rows, me)] + [swap(group_of(x_rows, me ^ m), m) for m in (1, 2, 3)]
        far_qkv = swap(piece_of(qkv_t, 0, 1)[0], 2)
        far_rest = swap(jnp.concatenate([piece_of(w, 0, 1)[0] for w in (o1_t, q2_t, o2_t)]), 2)
        sib_qkv, sib_o1, sib_q2, sib_o2 = (
            swap(w, 1) for w in (qkv_t, o1_t, q2_t, o2_t))
        bias = [b_ff1] + [swap(b_ff1, m) for m in (1, 2, 3)]

        kv = jnp.einsum("blc,rcjhd->rbljhd", context, w_kv2, preferred_element_type=F32).astype(BF16)
        kv = kv.reshape(layers, batch, ctx_len, 2 * width)
        kv = jnp.pad(kv, ((0, 0), (0, 0), (0, ctx_pad - ctx_len), (0, 0)))
        kv_out = [lax.dynamic_slice_in_dim(kv, (me ^ m) * mine, mine, 1) for m in range(tp_size)]
        kv_out[0], piece = tie(kv_out[0], far_qkv)
        full_qkv = gather(piece)
        kv_parts = [kv_out[0]] + [swap(kv_out[m], m) for m in (1, 2, 3)]
        ff_src = ff_piece(ff1_t, w_ff2, 0)
        far_ff = swap(ff_src, 2)
        sib_ff1, sib_ff2 = swap(ff1_t, 1), swap(w_ff2, 1)
        x_parts = list(tie(*x_parts, ff_src, *kv_out))[:tp_size]

        grid = (mine,)
        total = mine * n_tok
        a_shape = jax.ShapeDtypeStruct((mine, n_tok, channels), BF16)
        h_shape = jax.ShapeDtypeStruct((mine, n_tok, channels), F32)
        o_shape = jax.ShapeDtypeStruct((mine, n_tok, width), BF16)
        a_spec, o_spec = rows_spec((n_tok, channels)), rows_spec((n_tok, width))
        x_spec = rows_spec((tok, channels))

        hidden, act = call(
            in_kernel, grid,
            [x_spec] * 4 + [fixed_spec((channels, channels), 0), vec_spec(4, channels), vec_spec(2, channels)],
            [a_spec, a_spec], [h_shape, a_shape], 2 * total * channels * channels,
            [pltpu.VMEM((n_tok, channels), BF16)],
        )(*x_parts, w_proj, io_vecs, block_vecs[0, 0:2])

        def self_attn(act, first, second, layer):
            return call(functools.partial(self_kernel, layer), grid,
                        [a_spec] + [pl.BlockSpec(memory_space=pl.ANY)] * 2, [o_spec, o_spec], [o_shape, o_shape],
                        4 * total * channels * 3 * width + 32 * total * n_tok * width,
                        [pltpu.VMEM((2, 3 * width, channels), BF16), pltpu.SemaphoreType.DMA((2,))])(act, first, second)

        tile = n_tok // 2
        tiles = (2 * mine,)
        t_spec = pl.BlockSpec((1, tile, channels), lambda i: (i // 2, i % 2, 0))
        any_spec = pl.BlockSpec(memory_space=pl.ANY)
        group = 4
        cross_groups = SHARDS * width // (group * HEAD)

        def middle(hidden, mixed, vecs, layer, slot, rest, rest_sib):
            ot_spec = pl.BlockSpec((1, tile, width), lambda i: (i // 2, i % 2, 0))
            kv_spec = pl.BlockSpec((1, 1, ctx_pad, 2 * width), lambda i: (layer, i // 2, 0, 0))
            square = pltpu.VMEM((channels, channels), BF16)
            return call(
                functools.partial(mid_kernel, ctx_len, layer, slot), tiles,
                [t_spec] + [ot_spec] * 4 + [kv_spec] * 4 + [vec_spec(6, channels)] + [any_spec] * 8,
                [t_spec, t_spec], [h_shape, a_shape], 8 * total * channels * channels,
                [pltpu.VMEM((tile, channels), BF16), square, square, square,
                 pltpu.VMEM((cross_groups, group * 128, group * HEAD), BF16),
                 pltpu.VMEM((cross_groups, group * 128, 2 * group * HEAD), BF16),
                 pltpu.VMEM((cross_groups, tile, group * 128), BF16),
                 pltpu.SemaphoreType.DMA((3,))], {0: 0},
            )(hidden, *mixed, *kv_parts, vecs, o1_t, sib_o1, q2_t, sib_q2, o2_t, sib_o2, rest, rest_sib)

        chunks = ff // FF_COLS
        ff_flops = 6 * total * channels * ff

        def ff_scratch(n, *more):
            return [pltpu.VMEM((n, 2, channels, ff), BF16), pltpu.VMEM((n * ff, channels), BF16),
                    pltpu.VMEM((tile, n * ff), BF16), *more, pltpu.SemaphoreType.DMA((n * (chunks + 1),))]

        b_spec = [fixed_spec((2, ff), layer) for layer in range(layers)]

        def feed_forward(hidden, act, layer, *shards):
            n = len(shards)
            kinds = tuple(len(weights) for _, weights in shards)
            return call(functools.partial(ff_kernel, layer, kinds), tiles,
                        [t_spec, t_spec] + [b_spec[layer]] * n + [any_spec] * sum(kinds), t_spec, h_shape,
                        n * ff_flops, ff_scratch(n), {0: 0})(
                        hidden, act, *[bias[i] for i, _ in shards], *[w for _, weights in shards for w in weights])

        act, piece = tie(act, far_rest)
        full_rest = gather(piece)
        for layer in range(layers):
            vecs = block_vecs[layer]
            act, full = tie(act, full_qkv)
            rem = full.reshape(dp_size, -1, channels)
            rem_sib = swap(rem, 1)
            m0, m1 = self_attn(act, qkv_t, sib_qkv, layer)
            if layer == 0:
                act, m0, rest, src_a, src_b, src_c = tie(act, m0, full_rest, qkv_t, ff1_t, w_ff2)
                far_qkv = swap(piece_of(src_a, 1, 1)[0], 2)
                far_ff1 = swap(ff_piece(src_b, src_c, 1), 2)
                rest = rest.reshape(dp_size, -1, channels)
                act, *src = tie(act, o1_t, q2_t, o2_t)
                next_rest = swap(jnp.concatenate([w[1].reshape(dp_size, -1, channels) for w in src], axis=1), 2)
            else:
                act, m0 = tie(act, m0)
            rest_sib = swap(rest, 1)
            m2, m3 = self_attn(act, rem, rem_sib, layer)
            if layer == 0:
                act, m3, piece = tie(act, m3, far_ff)
                full_ff = gather(piece)
            hidden, act = middle(hidden, [m0, m1, m2, m3], jnp.stack([vecs[i] for i in (6, 2, 3, 7, 4, 5)]),
                                 layer, 0, rest, rest_sib)
            if layer == 0:
                act, piece = tie(act, far_qkv)
                full_qkv = gather(piece)
            own, sib = (0, (ff1_t, w_ff2)), (1, (sib_ff1, sib_ff2))
            if layer == 0:
                hidden = feed_forward(hidden, act, layer, own, sib)
            else:
                hidden = feed_forward(hidden, act, layer, own)
            hidden, act, full = tie(hidden, act, full_ff)
            rem = full.reshape(dp_size, 3, ff // dp_size, channels)
            rem_sib = swap(rem, 1)
            if layer == 0:
                hidden = feed_forward(hidden, act, layer, (2, (rem,)))
                hidden, piece, rest = tie(hidden, far_ff1, next_rest)
                next_ff = gather(piece)
            else:
                hidden = feed_forward(hidden, act, layer, sib)
            if layer < layers - 1:
                full_ff = next_ff
                after = block_vecs[layer + 1]
                hidden, act = call(
                    functools.partial(ff_last_kernel, layer), tiles,
                    [t_spec, t_spec, b_spec[layer], vec_spec(3, channels), any_spec],
                    [t_spec, t_spec], [h_shape, a_shape], ff_flops,
                    ff_scratch(1), {0: 0},
                )(hidden, act, bias[3], jnp.stack([vecs[8], after[0], after[1]]), rem_sib)

        y = []
        for sample in range(mine):
            row_spec = pl.BlockSpec((1, tile, channels), lambda i, sample=sample: (sample, i, 0))
            x_spec = pl.BlockSpec((1, tok, channels), lambda i, sample=sample: (sample, 0, 0))
            parts = call(
                functools.partial(ff_end_kernel, layers - 1), (2,),
                [row_spec, row_spec] + [b_spec[layers - 1]] * 2 + [vec_spec(1, channels), vec_spec(4, channels)]
                + [x_spec] * 4 + [any_spec] * 3,
                pl.BlockSpec((tp_size // 2, 1, tok, channels), lambda i: (i, 0, 0, 0)),
                jax.ShapeDtypeStruct((tp_size, 1, tok, channels), BF16), 2 * ff_flops // mine,
                ff_scratch(2, pltpu.VMEM((channels, channels), BF16), pltpu.SemaphoreType.DMA((1,))),
                None,
            )(hidden, act, bias[2], bias[3], vecs[8:9], io_vecs, *x_parts, w_proj, rem, rem_sib)
            y.append([parts[0]] + [swap(parts[m], m) for m in (1, 2, 3)])
            if sample < mine - 1:
                hidden, parts = tie(hidden, parts)
        out = jnp.zeros((tp_size, mine, tok, channels), BF16)
        for m in range(tp_size):
            for sample in range(mine):
                out = lax.dynamic_update_slice(out, y[sample][m][None], (me ^ m, sample, 0, 0))
        return out.reshape(batch, rows_loc, side, channels)

    act_spec = P("dp", "tp", None, None)
    in_specs = (act_spec, P("dp", None, None), P(), P(), P(),
                P(None, None, None, "tp", None), P(None, "tp", None, None),
                P(None, None, "tp", None), P(None, None, None, "tp", None),
                P(None, "tp", None, None), P(None, None, None, "tp"),
                P(None, None, "tp"), P(None, "tp", None))
    return jax.shard_map(body, mesh=mesh, in_specs=in_specs, out_specs=act_spec, check_vma=False)
```

```python
import functools

import jax
import jax.numpy as jnp
from jax import lax
from jax.experimental import pallas as pl
from jax.experimental.pallas import tpu as pltpu
from jax.sharding import PartitionSpec as P


GROUPS = 32
GN_EPS = 1e-6
LN_EPS = 1e-5
SHARDS = 4
HEAD = 64
LOG2E = 1.4426950408889634
F32 = jnp.float32
BF16 = jnp.bfloat16
NT = (((1,), (1,)), ((), ()))
VMEM_LIMIT = 67043328


def layer_norm(hidden, ln_gain, ln_shift):
    average = jnp.mean(hidden, axis=-1, keepdims=True)
    centered = hidden - average
    variance = jnp.mean(centered * centered, axis=-1, keepdims=True)
    return (centered * lax.rsqrt(variance + LN_EPS) * ln_gain + ln_shift).astype(BF16)


def attend(q, k, v):
    scores = lax.dot_general(q, k, NT, preferred_element_type=F32)
    top = jnp.max(scores, axis=-1, keepdims=True)
    probs = jnp.exp2((scores - top) * (HEAD ** -0.5 * LOG2E)).astype(BF16)
    values = jnp.concatenate([v, jnp.ones_like(v)], axis=1)
    mixed = jnp.dot(probs, values, preferred_element_type=F32)
    return (mixed[:, :HEAD] / mixed[:, HEAD:]).astype(BF16)


def in_kernel(x0, x1, x2, x3, w_ref, io_ref, ln_ref, h_out, a_out, g_scr):
    tok, channels = x0.shape[1:]
    parts = [ref[0].astype(F32) for ref in (x0, x1, x2, x3)]
    size = channels // GROUPS
    count = len(parts) * tok * size
    lanes = 128
    row = lax.broadcasted_iota(jnp.int32, (channels, lanes), 0)
    first = lax.broadcasted_iota(jnp.int32, (channels, lanes), 1) * size
    member = ((row >= first) & (row < first + size)).astype(F32)

    def group_average(columns):
        per_group = jnp.dot(jnp.broadcast_to(columns, (8, channels)), member,
                            precision=lax.Precision.HIGHEST, preferred_element_type=F32) / count
        return lax.dot_general(per_group, member, NT, precision=lax.Precision.HIGHEST,
                               preferred_element_type=F32)[0:1]

    mean = group_average(sum(jnp.sum(p, axis=0, keepdims=True) for p in parts))
    var = group_average(sum(jnp.sum((p - mean) * (p - mean), axis=0, keepdims=True) for p in parts))
    inverse = lax.rsqrt(var + GN_EPS)
    for i, p in enumerate(parts):
        g_scr[i * tok:(i + 1) * tok, :] = ((p - mean) * inverse * io_ref[0:1] + io_ref[1:2]).astype(BF16)
    h = jnp.dot(g_scr[...], w_ref[0], preferred_element_type=F32) + io_ref[2:3]
    h_out[0] = h
    a_out[0] = layer_norm(h, ln_ref[0:1], ln_ref[1:2])


def self_kernel(layer, a_ref, own_ref, sib_ref, o0, o1, w, sems):
    width = o0.shape[-1]
    copies = []
    for n, ref in enumerate((own_ref, sib_ref)):
        if ref.shape[1] == w.shape[1]:
            pairs = [(ref.at[layer], w.at[n])]
        else:
            rows = ref.shape[1]
            pairs = [(ref.at[d], w.at[n, pl.ds(d * rows, rows)]) for d in range(ref.shape[0])]
        copies.append([pltpu.make_async_copy(src, to, sems.at[n]) for src, to in pairs])

    @pl.when(pl.program_id(0) == 0)
    def _():
        for some in copies:
            for copy in some:
                copy.start()

    for n, o_ref in enumerate((o0, o1)):
        @pl.when(pl.program_id(0) == 0)
        def _():
            for copy in copies[n]:
                copy.wait()

        qkv = lax.dot_general(a_ref[0], w[n], NT, preferred_element_type=F32).astype(BF16)
        for head in range(width // HEAD):
            lo = head * HEAD
            o_ref[0, :, lo:lo + HEAD] = attend(
                qkv[:, lo:lo + HEAD], qkv[:, width + lo:width + lo + HEAD],
                qkv[:, 2 * width + lo:2 * width + lo + HEAD])


def row_copies(own, sib, rest, rest_sib, layer, slot, dst, sem):
    width = own.shape[1]
    pieces = rest.shape[0]
    rows = width // pieces
    pairs = [(ref.at[layer], dst.at[pl.ds(i * width, width)]) for i, ref in enumerate((own, sib))]
    for i, ref in ((2, rest), (3, rest_sib)):
        pairs += [(ref.at[d, pl.ds(slot * rows, rows)], dst.at[pl.ds(i * width + d * rows, rows)]) for d in range(pieces)]
    return [pltpu.make_async_copy(src, to, sem) for src, to in pairs]


def mid_kernel(valid, layer, slot, h_ref, o0, o1, o2, o3, kv0, kv1, kv2, kv3, vec_ref,
               o1_own, o1_sib, q2_own, q2_sib, o2_own, o2_sib, rest, rest_sib,
               h_out, a_out, o_all, w_out1, w_q, w_out2, k_scr, v_scr, p_scr, sems):
    step = pl.program_id(0)
    width = o0.shape[-1]
    heads = width // HEAD
    keys = kv0.shape[2]
    lanes = 128
    group = k_scr.shape[2] // HEAD
    cols = group * HEAD
    copies = [row_copies(own, sib, rest, rest_sib, layer, slot + i, dst, sems.at[i]) for i, (own, sib, dst) in enumerate(
        ((o1_own, o1_sib, w_out1), (q2_own, q2_sib, w_q), (o2_own, o2_sib, w_out2)))]

    @pl.when(step == 0)
    def _():
        for some in copies:
            for copy in some:
                copy.start()
        k_scr[...] = jnp.zeros_like(k_scr)
        v_scr[...] = jnp.zeros_like(v_scr)

    one = (lax.broadcasted_iota(jnp.int32, (keys, HEAD), 0) < valid).astype(BF16)
    for shard, ref in enumerate((kv0, kv1, kv2, kv3)):
        kv = ref[0, 0]
        for head in range(heads):
            place = shard * heads + head
            g, r = place // group, place % group
            rows = slice(r * lanes, r * lanes + keys)
            at = slice(r * HEAD, (r + 1) * HEAD)
            k_scr[g, rows, at] = kv[:, head * HEAD:(head + 1) * HEAD]
            v_scr[g, rows, at] = kv[:, width + head * HEAD:width + (head + 1) * HEAD]
            v_scr[g, rows, cols + r * HEAD:cols + (r + 1) * HEAD] = one
    for i, o_ref in enumerate((o0, o1, o2, o3)):
        o_all[:, i * width:(i + 1) * width] = o_ref[0]

    half = h_ref.shape[1] // 2
    halves = [slice(0, half), slice(half, 2 * half)]

    def run(first):
        def wait(i):
            if first:
                for copy in copies[i]:
                    copy.wait()

        wait(0)
        h = [h_ref[0, at, :] + jnp.dot(o_all[at, :], w_out1[...], preferred_element_type=F32) + vec_ref[0:1] for at in halves]
        for at, value in zip(halves, h):
            h_out[0, at, :] = value
        act = [layer_norm(value, vec_ref[1:2], vec_ref[2:3]) for value in h]
        wait(1)
        q = [lax.dot_general(value, w_q[...], NT, preferred_element_type=F32).astype(BF16) for value in act]
        live = lax.broadcasted_iota(jnp.int32, (half, lanes), 1) < valid
        for g in range(k_scr.shape[0]):
            at = slice(g * cols, (g + 1) * cols)
            scores = [lax.dot_general(value[:, at], k_scr[g], NT, preferred_element_type=F32) for value in q]
            for rows, part in zip(halves, scores):
                for r in range(group):
                    sl = slice(r * lanes, (r + 1) * lanes)
                    s = jnp.where(live, part[:, sl], -jnp.inf)
                    top = jnp.max(s, axis=-1, keepdims=True)
                    p_scr[g, rows, sl] = jnp.exp2((s - top) * (HEAD ** -0.5 * LOG2E)).astype(BF16)
            for rows in halves:
                mixed = jnp.dot(p_scr[g, rows, :], v_scr[g], preferred_element_type=F32)
                o_all[rows, at] = (mixed[:, :cols] / mixed[:, cols:]).astype(BF16)
        wait(2)
        h = [h_out[0, at, :] + jnp.dot(o_all[at, :], w_out2[...], preferred_element_type=F32) + vec_ref[3:4] for at in halves]
        for at, value in zip(halves, h):
            h_out[0, at, :] = value
            a_out[0, at, :] = layer_norm(value, vec_ref[4:5], vec_ref[5:6])

    pl.when(step == 0)(functools.partial(run, True))
    pl.when(step > 0)(functools.partial(run, False))


FF_COLS = 256


def ff_copies(layer, shards, w1, w2, sems):
    channels, ff = w1.shape[2:]
    chunks = ff // FF_COLS
    first, second = [], []
    for n, refs in enumerate(shards):
        packed = refs[0].shape[2] != channels
        rows = refs[0].shape[2]
        pieces = range(refs[0].shape[0])
        for j in range(chunks):
            at = pl.ds(j * FF_COLS, FF_COLS)
            if packed:
                first.append([(refs[0].at[d, pl.ds(0, 2), :, at], w1.at[n, :, pl.ds(d * rows, rows), at]) for d in pieces])
            else:
                first.append([(refs[0].at[layer, :, :, at], w1.at[n, :, :, at])])
        if len(refs) == 2:
            second.append([(refs[1].at[layer if refs[1].shape[0] > 1 else 0], w2.at[pl.ds(n * ff, ff)])])
        else:
            second.append([(refs[0].at[d, 2], w2.at[pl.ds(n * ff + d * rows, rows)]) for d in pieces])
    return [[pltpu.make_async_copy(src, to, sems.at[i]) for src, to in pairs] for i, pairs in enumerate(first + second)]


def ff_steps(layer, a_ref, biases, shards, w1, w2, m_scr, sems, finish):
    step = pl.program_id(0)
    groups = ff_copies(layer, shards, w1, w2, sems)
    ff = w1.shape[3]
    chunks = ff // FF_COLS
    ahead = len(groups)

    def start(i):
        for copy in groups[i] if i < len(groups) else ():
            copy.start()

    def run(first):
        if first:
            for i in range(ahead):
                start(i)
        a = a_ref[0]
        for n, b1_ref in enumerate(biases):
            for j in range(chunks):
                if first:
                    start(n * chunks + j + ahead)
                    for copy in groups[n * chunks + j]:
                        copy.wait()
                sl = slice(j * FF_COLS, (j + 1) * FF_COLS)
                u0 = jnp.dot(a, w1[n, 0, :, sl], preferred_element_type=F32) + b1_ref[0, 0:1, sl]
                u1 = jnp.dot(a, w1[n, 1, :, sl], preferred_element_type=F32) + b1_ref[0, 1:2, sl]
                gate = 0.5 * u1 * (1.0 + lax.erf(u1 * (0.5 ** 0.5)))
                m_scr[:, n * ff + j * FF_COLS:n * ff + (j + 1) * FF_COLS] = (u0 * gate).astype(BF16)
        if first:
            for some in groups[len(biases) * chunks:]:
                for copy in some:
                    copy.wait()
        finish(jnp.dot(m_scr[...], w2[...], preferred_element_type=F32), first)

    pl.when(step == 0)(functools.partial(run, True))
    pl.when(step > 0)(functools.partial(run, False))


def ff_kernel(layer, kinds, h_ref, a_ref, *rest):
    biases, refs = rest[:len(kinds)], list(rest[len(kinds):-5])
    h_out, w1, w2, m_scr, sems = rest[-5:]
    shards = [[refs.pop(0) for _ in range(kind)] for kind in kinds]

    def finish(update, first):
        h_out[0] = h_ref[0] + update

    ff_steps(layer, a_ref, biases, shards, w1, w2, m_scr, sems, finish)


def ff_last_kernel(layer, h_ref, a_ref, b1_ref, vec_ref, w_ref, h_out, a_out, w1, w2, m_scr, sems):
    def finish(update, first):
        h = h_ref[0] + update + vec_ref[0:1]
        h_out[0] = h
        a_out[0] = layer_norm(h, vec_ref[1:2], vec_ref[2:3])

    ff_steps(layer, a_ref, (b1_ref,), ((w_ref,),), w1, w2, m_scr, sems, finish)


def ff_end_kernel(layer, h_ref, a_ref, b1, b2, b3, vec_ref, io_ref, x0, x1, x2, x3, wp_ref, *rest):
    refs, (y_ref, w1, w2, m_scr, wp, wp_sem, sems) = rest[:-7], rest[-7:]
    shards = [refs[i:i + 2] for i in range(0, len(refs), 2)]
    tok = x0.shape[1]
    last = pltpu.make_async_copy(wp_ref.at[1], wp, wp_sem.at[0])

    def finish(update, first):
        if first:
            last.start()
        h = h_ref[0] + update + vec_ref[0:1]
        if first:
            last.wait()
        y = jnp.dot(h.astype(BF16), wp[...], preferred_element_type=F32) + io_ref[3:4]
        for i, ref in enumerate((x0, x1) if first else (x2, x3)):
            y_ref[i, 0] = (y[i * tok:(i + 1) * tok] + ref[0].astype(F32)).astype(BF16)

    ff_steps(layer, a_ref, (b1, b2, b3), shards, w1, w2, m_scr, sems, finish)


def rows_spec(shape):
    return pl.BlockSpec((1,) + shape, lambda i: (i, 0, 0))


def fixed_spec(shape, layer):
    return pl.BlockSpec((1,) + shape, lambda i: (layer,) + (0,) * len(shape))


def vec_spec(rows, cols):
    return pl.BlockSpec((rows, cols), lambda i: (0, 0))


def call(kernel, grid, in_specs, out_specs, out_shape, flops, scratch=(), aliases=None):
    return pl.pallas_call(
        kernel, grid=grid, in_specs=in_specs, out_specs=out_specs, out_shape=out_shape,
        scratch_shapes=scratch, input_output_aliases=aliases or {},
        cost_estimate=pl.CostEstimate(flops=flops, bytes_accessed=16 << 20, transcendentals=0),
        compiler_params=pltpu.CompilerParams(vmem_limit_bytes=VMEM_LIMIT))


def tie(*values):
    return lax.optimization_barrier(values)


def solution(mesh):
    tp_size = mesh.shape["tp"]
    dp_size = mesh.shape["dp"]

    def swap(value, mask):
        return lax.ppermute(value, "tp", [(i, i ^ mask) for i in range(tp_size)])

    def body(latents, context, io_vecs, w_proj, block_vecs, w_qkv, w_o1, w_q2, w_kv2, w_o2, w_ff1, b_ff1, w_ff2):
        batch, rows_loc, side, channels = latents.shape
        tok = rows_loc * side
        layers = w_qkv.shape[0]
        width = w_o1.shape[1] * HEAD
        ff = w_ff2.shape[1]
        ctx_len = context.shape[1]
        ctx_pad = -(-ctx_len // 16) * 16
        mine = batch // tp_size
        n_tok = tp_size * tok
        me = lax.axis_index("tp")
        dp_me = lax.axis_index("dp")

        def piece_of(value, layer, axis):
            rows = value.shape[axis] // dp_size
            start = [0] * value.ndim
            start[0], start[axis] = layer, dp_me * rows
            size = list(value.shape)
            size[0], size[axis] = 1, rows
            return lax.dynamic_slice(value, start, size)

        def gather(piece):
            return lax.all_gather(piece, "dp", axis=0, tiled=True)

        qkv_t = w_qkv.transpose(0, 2, 3, 4, 1).reshape(layers, 3 * width, channels)
        q2_t = w_q2.transpose(0, 2, 3, 1).reshape(layers, width, channels)
        o1_t = w_o1.reshape(layers, width, channels)
        o2_t = w_o2.reshape(layers, width, channels)
        ff1_t = w_ff1.transpose(0, 2, 1, 3)

        def ff_piece(ff1, ff2, layer):
            return jnp.concatenate([piece_of(ff1, layer, 2)[0], piece_of(ff2, layer, 1)])

        x_rows = latents.reshape(tp_size, mine, tok, channels)

        def group_of(array, index):
            return lax.dynamic_index_in_dim(array, index, 0, keepdims=False)

        x_parts = [group_of(x_rows, me)] + [swap(group_of(x_rows, me ^ m), m) for m in (1, 2, 3)]
        far_qkv = swap(piece_of(qkv_t, 0, 1)[0], 2)
        far_rest = swap(jnp.concatenate([piece_of(w, 0, 1)[0] for w in (o1_t, q2_t, o2_t)]), 2)
        sib_qkv, sib_o1, sib_q2, sib_o2 = (
            swap(w, 1) for w in (qkv_t, o1_t, q2_t, o2_t))
        bias = [b_ff1] + [swap(b_ff1, m) for m in (1, 2, 3)]

        kv = jnp.einsum("blc,rcjhd->rbljhd", context, w_kv2, preferred_element_type=F32).astype(BF16)
        kv = kv.reshape(layers, batch, ctx_len, 2 * width)
        kv = jnp.pad(kv, ((0, 0), (0, 0), (0, ctx_pad - ctx_len), (0, 0)))
        kv_out = [lax.dynamic_slice_in_dim(kv, (me ^ m) * mine, mine, 1) for m in range(tp_size)]
        kv_out[0], piece = tie(kv_out[0], far_qkv)
        full_qkv = gather(piece)
        kv_parts = [kv_out[0]] + [swap(kv_out[m], m) for m in (1, 2, 3)]
        ff_src = ff_piece(ff1_t, w_ff2, 0)
        far_ff = swap(ff_src, 2)
        sib_ff1, sib_ff2 = swap(ff1_t, 1), swap(w_ff2, 1)
        x_parts = list(tie(*x_parts, ff_src, *kv_out))[:tp_size]

        grid = (mine,)
        total = mine * n_tok
        a_shape = jax.ShapeDtypeStruct((mine, n_tok, channels), BF16)
        h_shape = jax.ShapeDtypeStruct((mine, n_tok, channels), F32)
        o_shape = jax.ShapeDtypeStruct((mine, n_tok, width), BF16)
        a_spec, o_spec = rows_spec((n_tok, channels)), rows_spec((n_tok, width))
        x_spec = rows_spec((tok, channels))

        hidden, act = call(
            in_kernel, grid,
            [x_spec] * 4 + [fixed_spec((channels, channels), 0), vec_spec(4, channels), vec_spec(2, channels)],
            [a_spec, a_spec], [h_shape, a_shape], 2 * total * channels * channels,
            [pltpu.VMEM((n_tok, channels), BF16)],
        )(*x_parts, w_proj, io_vecs, block_vecs[0, 0:2])

        def self_attn(act, first, second, layer):
            return call(functools.partial(self_kernel, layer), grid,
                        [a_spec] + [pl.BlockSpec(memory_space=pl.ANY)] * 2, [o_spec, o_spec], [o_shape, o_shape],
                        4 * total * channels * 3 * width + 32 * total * n_tok * width,
                        [pltpu.VMEM((2, 3 * width, channels), BF16), pltpu.SemaphoreType.DMA((2,))])(act, first, second)

        tile = n_tok // 2
        tiles = (2 * mine,)
        t_spec = pl.BlockSpec((1, tile, channels), lambda i: (i // 2, i % 2, 0))
        any_spec = pl.BlockSpec(memory_space=pl.ANY)
        group = 4
        cross_groups = SHARDS * width // (group * HEAD)

        def middle(hidden, mixed, vecs, layer, slot, rest, rest_sib):
            kv_spec = pl.BlockSpec((1, 1, ctx_pad, 2 * width), lambda i: (layer, i, 0, 0))
            square = pltpu.VMEM((channels, channels), BF16)
            return call(
                functools.partial(mid_kernel, ctx_len, layer, slot), grid,
                [a_spec] + [o_spec] * 4 + [kv_spec] * 4 + [vec_spec(6, channels)] + [any_spec] * 8,
                [a_spec, a_spec], [h_shape, a_shape], 8 * total * channels * channels,
                [pltpu.VMEM((n_tok, channels), BF16), square, square, square,
                 pltpu.VMEM((cross_groups, group * 128, group * HEAD), BF16),
                 pltpu.VMEM((cross_groups, group * 128, 2 * group * HEAD), BF16),
                 pltpu.VMEM((cross_groups, n_tok, group * 128), BF16),
                 pltpu.SemaphoreType.DMA((3,))], {0: 0},
            )(hidden, *mixed, *kv_parts, vecs, o1_t, sib_o1, q2_t, sib_q2, o2_t, sib_o2, rest, rest_sib)

        chunks = ff // FF_COLS
        ff_flops = 6 * total * channels * ff

        def ff_scratch(n, *more):
            return [pltpu.VMEM((n, 2, channels, ff), BF16), pltpu.VMEM((n * ff, channels), BF16),
                    pltpu.VMEM((tile, n * ff), BF16), *more, pltpu.SemaphoreType.DMA((n * (chunks + 1),))]

        b_spec = [fixed_spec((2, ff), layer) for layer in range(layers)]

        def feed_forward(hidden, act, layer, *shards):
            n = len(shards)
            kinds = tuple(len(weights) for _, weights in shards)
            return call(functools.partial(ff_kernel, layer, kinds), tiles,
                        [t_spec, t_spec] + [b_spec[layer]] * n + [any_spec] * sum(kinds), t_spec, h_shape,
                        n * ff_flops, ff_scratch(n), {0: 0})(
                        hidden, act, *[bias[i] for i, _ in shards], *[w for _, weights in shards for w in weights])

        act, piece = tie(act, far_rest)
        full_rest = gather(piece)
        for layer in range(layers):
            vecs = block_vecs[layer]
            act, full = tie(act, full_qkv)
            rem = full.reshape(dp_size, -1, channels)
            rem_sib = swap(rem, 1)
            m0, m1 = self_attn(act, qkv_t, sib_qkv, layer)
            act, m0 = tie(act, m0)
            if layer == 1:
                rest_sib = swap(rest, 1)
            m2, m3 = self_attn(act, rem, rem_sib, layer)
            if layer == 0:
                act, m3, piece, rest = tie(act, m3, far_ff, full_rest)
                full_ff = gather(piece)
                rest = rest.reshape(dp_size, -1, channels)
                rest_sib = swap(rest, 1)
                act, src_a, src_b, src_c, *src = tie(act, qkv_t, ff1_t, w_ff2, o1_t, q2_t, o2_t)
                far_qkv = swap(piece_of(src_a, 1, 1)[0], 2)
                far_ff1 = swap(piece_of(src_b, 1, 2)[0], 2)
                next_rest = swap(jnp.concatenate([w[1].reshape(dp_size, -1, channels) for w in src], axis=1), 2)
                next_ff2 = swap(src_c[1:], 2)
            else:
                m3, next_ff2 = tie(m3, next_ff2)
                next_ff2_sib = swap(next_ff2, 1)
            hidden, act = middle(hidden, [m0, m1, m2, m3], jnp.stack([vecs[i] for i in (6, 2, 3, 7, 4, 5)]),
                                 layer, 0, rest, rest_sib)
            if layer == 0:
                act, piece = tie(act, far_qkv)
                full_qkv = gather(piece)
                hidden = feed_forward(hidden, act, layer, (0, (ff1_t, w_ff2)), (1, (sib_ff1, sib_ff2)))
                hidden, act, full, piece = tie(hidden, act, full_ff, far_ff1)
                next_ff = gather(piece)
                rem = full.reshape(dp_size, 3, ff // dp_size, channels)
                rem_sib = swap(rem, 1)
                hidden = feed_forward(hidden, act, layer, (2, (rem,)))
                hidden, rest = tie(hidden, next_rest)
                after = block_vecs[layer + 1]
                hidden, act = call(
                    functools.partial(ff_last_kernel, layer), tiles,
                    [t_spec, t_spec, b_spec[layer], vec_spec(3, channels), any_spec],
                    [t_spec, t_spec], [h_shape, a_shape], ff_flops,
                    ff_scratch(1), {0: 0},
                )(hidden, act, bias[3], jnp.stack([vecs[8], after[0], after[1]]), rem_sib)

        hidden, act, full = tie(hidden, act, next_ff)
        rem = full.reshape(dp_size, 2, ff // dp_size, channels)
        ff_weights = [sib_ff1, sib_ff2, rem, next_ff2, swap(rem, 1), next_ff2_sib]
        hidden = feed_forward(hidden, act, layers - 1, (0, (ff1_t, w_ff2)))
        y = []
        for sample in range(mine):
            row_spec = pl.BlockSpec((1, tile, channels), lambda i, sample=sample: (sample, i, 0))
            x_spec = pl.BlockSpec((1, tok, channels), lambda i, sample=sample: (sample, 0, 0))
            parts = call(
                functools.partial(ff_end_kernel, layers - 1), (2,),
                [row_spec, row_spec] + [b_spec[layers - 1]] * 3 + [vec_spec(1, channels), vec_spec(4, channels)]
                + [x_spec] * 4 + [any_spec] * 7,
                pl.BlockSpec((tp_size // 2, 1, tok, channels), lambda i: (i, 0, 0, 0)),
                jax.ShapeDtypeStruct((tp_size, 1, tok, channels), BF16), 3 * ff_flops // mine,
                ff_scratch(3, pltpu.VMEM((channels, channels), BF16), pltpu.SemaphoreType.DMA((1,))),
                None,
            )(hidden, act, *bias[1:], vecs[8:9], io_vecs, *x_parts, w_proj, *ff_weights)
            y.append([parts[0]] + [swap(parts[m], m) for m in (1, 2, 3)])
            if sample < mine - 1:
                hidden, parts = tie(hidden, parts)
        out = jnp.zeros((tp_size, mine, tok, channels), BF16)
        for m in range(tp_size):
            for sample in range(mine):
                out = lax.dynamic_update_slice(out, y[sample][m][None], (me ^ m, sample, 0, 0))
        return out.reshape(batch, rows_loc, side, channels)

    act_spec = P("dp", "tp", None, None)
    in_specs = (act_spec, P("dp", None, None), P(), P(), P(),
                P(None, None, None, "tp", None), P(None, "tp", None, None),
                P(None, None, "tp", None), P(None, None, None, "tp", None),
                P(None, "tp", None, None), P(None, None, None, "tp"),
                P(None, None, "tp"), P(None, "tp", None))
    return jax.shard_map(body, mesh=mesh, in_specs=in_specs, out_specs=act_spec, check_vma=False)
```

```python
import functools

import jax
import jax.numpy as jnp
from jax import lax
from jax.experimental import pallas as pl
from jax.experimental.pallas import tpu as pltpu
from jax.sharding import PartitionSpec as P


GROUPS = 32
GN_EPS = 1e-6
LN_EPS = 1e-5
SHARDS = 4
HEAD = 64
LOG2E = 1.4426950408889634
F32 = jnp.float32
BF16 = jnp.bfloat16
NT = (((1,), (1,)), ((), ()))
VMEM_LIMIT = 67043328


def layer_norm(hidden, ln_gain, ln_shift):
    average = jnp.mean(hidden, axis=-1, keepdims=True)
    centered = hidden - average
    variance = jnp.mean(centered * centered, axis=-1, keepdims=True)
    return (centered * lax.rsqrt(variance + LN_EPS) * ln_gain + ln_shift).astype(BF16)


def attend(q, k, v):
    scores = lax.dot_general(q, k, NT, preferred_element_type=F32)
    top = jnp.max(scores, axis=-1, keepdims=True)
    probs = jnp.exp2((scores - top) * (HEAD ** -0.5 * LOG2E)).astype(BF16)
    values = jnp.concatenate([v, jnp.ones_like(v)], axis=1)
    mixed = jnp.dot(probs, values, preferred_element_type=F32)
    return (mixed[:, :HEAD] / mixed[:, HEAD:]).astype(BF16)


def in_kernel(x0, x1, x2, x3, w_ref, io_ref, ln_ref, h_out, a_out, g_scr):
    tok, channels = x0.shape[1:]
    parts = [ref[0].astype(F32) for ref in (x0, x1, x2, x3)]
    size = channels // GROUPS
    count = len(parts) * tok * size
    lanes = 128
    row = lax.broadcasted_iota(jnp.int32, (channels, lanes), 0)
    first = lax.broadcasted_iota(jnp.int32, (channels, lanes), 1) * size
    member = ((row >= first) & (row < first + size)).astype(F32)

    def group_average(columns):
        per_group = jnp.dot(jnp.broadcast_to(columns, (8, channels)), member,
                            precision=lax.Precision.HIGHEST, preferred_element_type=F32) / count
        return lax.dot_general(per_group, member, NT, precision=lax.Precision.HIGHEST,
                               preferred_element_type=F32)[0:1]

    mean = group_average(sum(jnp.sum(p, axis=0, keepdims=True) for p in parts))
    var = group_average(sum(jnp.sum((p - mean) * (p - mean), axis=0, keepdims=True) for p in parts))
    inverse = lax.rsqrt(var + GN_EPS)
    for i, p in enumerate(parts):
        g_scr[i * tok:(i + 1) * tok, :] = ((p - mean) * inverse * io_ref[0:1] + io_ref[1:2]).astype(BF16)
    h = jnp.dot(g_scr[...], w_ref[0], preferred_element_type=F32) + io_ref[2:3]
    h_out[0] = h
    a_out[0] = layer_norm(h, ln_ref[0:1], ln_ref[1:2])


def self_kernel(layer, a_ref, own_ref, sib_ref, o0, o1, w, sems):
    width = o0.shape[-1]
    copies = []
    for n, ref in enumerate((own_ref, sib_ref)):
        if ref.shape[1] == w.shape[1]:
            pairs = [(ref.at[layer], w.at[n])]
        else:
            rows = ref.shape[1]
            pairs = [(ref.at[d], w.at[n, pl.ds(d * rows, rows)]) for d in range(ref.shape[0])]
        copies.append([pltpu.make_async_copy(src, to, sems.at[n]) for src, to in pairs])

    @pl.when(pl.program_id(0) == 0)
    def _():
        for some in copies:
            for copy in some:
                copy.start()

    for n, o_ref in enumerate((o0, o1)):
        @pl.when(pl.program_id(0) == 0)
        def _():
            for copy in copies[n]:
                copy.wait()

        qkv = lax.dot_general(a_ref[0], w[n], NT, preferred_element_type=F32).astype(BF16)
        for head in range(width // HEAD):
            lo = head * HEAD
            o_ref[0, :, lo:lo + HEAD] = attend(
                qkv[:, lo:lo + HEAD], qkv[:, width + lo:width + lo + HEAD],
                qkv[:, 2 * width + lo:2 * width + lo + HEAD])


def row_copies(own, sib, rest, rest_sib, layer, slot, dst, sem):
    width = own.shape[1]
    pieces = rest.shape[0]
    rows = width // pieces
    pairs = [(ref.at[layer], dst.at[pl.ds(i * width, width)]) for i, ref in enumerate((own, sib))]
    for i, ref in ((2, rest), (3, rest_sib)):
        pairs += [(ref.at[d, pl.ds(slot * rows, rows)], dst.at[pl.ds(i * width + d * rows, rows)]) for d in range(pieces)]
    return [pltpu.make_async_copy(src, to, sem) for src, to in pairs]


def mid_kernel(valid, layer, slot, h_ref, o0, o1, o2, o3, kv0, kv1, kv2, kv3, vec_ref,
               o1_own, o1_sib, q2_own, q2_sib, o2_own, o2_sib, rest, rest_sib,
               h_out, a_out, o_all, w_out1, w_q, w_out2, k_scr, v_scr, p_scr, sems):
    step = pl.program_id(0)
    width = o0.shape[-1]
    heads = width // HEAD
    keys = kv0.shape[2]
    lanes = 128
    group = k_scr.shape[2] // HEAD
    cols = group * HEAD
    copies = [row_copies(own, sib, rest, rest_sib, layer, slot + i, dst, sems.at[i]) for i, (own, sib, dst) in enumerate(
        ((o1_own, o1_sib, w_out1), (q2_own, q2_sib, w_q), (o2_own, o2_sib, w_out2)))]

    @pl.when(step == 0)
    def _():
        for some in copies:
            for copy in some:
                copy.start()
        k_scr[...] = jnp.zeros_like(k_scr)
        v_scr[...] = jnp.zeros_like(v_scr)

    one = (lax.broadcasted_iota(jnp.int32, (keys, HEAD), 0) < valid).astype(BF16)
    for shard, ref in enumerate((kv0, kv1, kv2, kv3)):
        kv = ref[0, 0]
        for head in range(heads):
            place = shard * heads + head
            g, r = place // group, place % group
            rows = slice(r * lanes, r * lanes + keys)
            at = slice(r * HEAD, (r + 1) * HEAD)
            k_scr[g, rows, at] = kv[:, head * HEAD:(head + 1) * HEAD]
            v_scr[g, rows, at] = kv[:, width + head * HEAD:width + (head + 1) * HEAD]
            v_scr[g, rows, cols + r * HEAD:cols + (r + 1) * HEAD] = one
    for i, o_ref in enumerate((o0, o1, o2, o3)):
        o_all[:, i * width:(i + 1) * width] = o_ref[0]

    half = h_ref.shape[1] // 2
    halves = [slice(0, half), slice(half, 2 * half)]

    def run(first):
        def wait(i):
            if first:
                for copy in copies[i]:
                    copy.wait()

        wait(0)
        h = [h_ref[0, at, :] + jnp.dot(o_all[at, :], w_out1[...], preferred_element_type=F32) + vec_ref[0:1] for at in halves]
        for at, value in zip(halves, h):
            h_out[0, at, :] = value
        act = [layer_norm(value, vec_ref[1:2], vec_ref[2:3]) for value in h]
        wait(1)
        q = [lax.dot_general(value, w_q[...], NT, preferred_element_type=F32).astype(BF16) for value in act]
        live = lax.broadcasted_iota(jnp.int32, (half, lanes), 1) < valid
        for g in range(k_scr.shape[0]):
            at = slice(g * cols, (g + 1) * cols)
            scores = [lax.dot_general(value[:, at], k_scr[g], NT, preferred_element_type=F32) for value in q]
            for rows, part in zip(halves, scores):
                for r in range(group):
                    sl = slice(r * lanes, (r + 1) * lanes)
                    s = jnp.where(live, part[:, sl], -jnp.inf)
                    top = jnp.max(s, axis=-1, keepdims=True)
                    p_scr[g, rows, sl] = jnp.exp2((s - top) * (HEAD ** -0.5 * LOG2E)).astype(BF16)
            for rows in halves:
                mixed = jnp.dot(p_scr[g, rows, :], v_scr[g], preferred_element_type=F32)
                o_all[rows, at] = (mixed[:, :cols] / mixed[:, cols:]).astype(BF16)
        wait(2)
        h = [h_out[0, at, :] + jnp.dot(o_all[at, :], w_out2[...], preferred_element_type=F32) + vec_ref[3:4] for at in halves]
        for at, value in zip(halves, h):
            h_out[0, at, :] = value
            a_out[0, at, :] = layer_norm(value, vec_ref[4:5], vec_ref[5:6])

    pl.when(step == 0)(functools.partial(run, True))
    pl.when(step > 0)(functools.partial(run, False))


FF_COLS = 256


def ff_copies(layer, shards, w1, w2, sems):
    channels, ff = w1.shape[2:]
    chunks = ff // FF_COLS
    first, second = [], []
    for n, refs in enumerate(shards):
        packed = refs[0].shape[2] != channels
        rows = refs[0].shape[2]
        pieces = range(refs[0].shape[0])
        for j in range(chunks):
            at = pl.ds(j * FF_COLS, FF_COLS)
            if packed:
                first.append([(refs[0].at[d, pl.ds(0, 2), :, at], w1.at[n, :, pl.ds(d * rows, rows), at]) for d in pieces])
            else:
                first.append([(refs[0].at[layer, :, :, at], w1.at[n, :, :, at])])
        if len(refs) == 2:
            second.append([(refs[1].at[layer if refs[1].shape[0] > 1 else 0], w2.at[pl.ds(n * ff, ff)])])
        else:
            second.append([(refs[0].at[d, 2], w2.at[pl.ds(n * ff + d * rows, rows)]) for d in pieces])
    return [[pltpu.make_async_copy(src, to, sems.at[i]) for src, to in pairs] for i, pairs in enumerate(first + second)]


def ff_steps(layer, a_ref, biases, shards, w1, w2, m_scr, sems, finish):
    step = pl.program_id(0)
    groups = ff_copies(layer, shards, w1, w2, sems)
    ff = w1.shape[3]
    chunks = ff // FF_COLS
    ahead = len(groups)

    def start(i):
        for copy in groups[i] if i < len(groups) else ():
            copy.start()

    def run(first):
        if first:
            for i in range(ahead):
                start(i)
        a = a_ref[0]
        for n, b1_ref in enumerate(biases):
            for j in range(chunks):
                if first:
                    start(n * chunks + j + ahead)
                    for copy in groups[n * chunks + j]:
                        copy.wait()
                sl = slice(j * FF_COLS, (j + 1) * FF_COLS)
                u0 = jnp.dot(a, w1[n, 0, :, sl], preferred_element_type=F32) + b1_ref[0, 0:1, sl]
                u1 = jnp.dot(a, w1[n, 1, :, sl], preferred_element_type=F32) + b1_ref[0, 1:2, sl]
                gate = 0.5 * u1 * (1.0 + lax.erf(u1 * (0.5 ** 0.5)))
                m_scr[:, n * ff + j * FF_COLS:n * ff + (j + 1) * FF_COLS] = (u0 * gate).astype(BF16)
        if first:
            for some in groups[len(biases) * chunks:]:
                for copy in some:
                    copy.wait()
        finish(jnp.dot(m_scr[...], w2[...], preferred_element_type=F32), first)

    pl.when(step == 0)(functools.partial(run, True))
    pl.when(step > 0)(functools.partial(run, False))


def ff_kernel(layer, kinds, h_ref, a_ref, *rest):
    biases, refs = rest[:len(kinds)], list(rest[len(kinds):-5])
    h_out, w1, w2, m_scr, sems = rest[-5:]
    shards = [[refs.pop(0) for _ in range(kind)] for kind in kinds]

    def finish(update, first):
        h_out[0] = h_ref[0] + update

    ff_steps(layer, a_ref, biases, shards, w1, w2, m_scr, sems, finish)


def ff_last_kernel(layer, h_ref, a_ref, b1_ref, vec_ref, w1_ref, w2_ref, h_out, a_out, w1, w2, m_scr, sems):
    def finish(update, first):
        h = h_ref[0] + update + vec_ref[0:1]
        h_out[0] = h
        a_out[0] = layer_norm(h, vec_ref[1:2], vec_ref[2:3])

    ff_steps(layer, a_ref, (b1_ref,), ((w1_ref, w2_ref),), w1, w2, m_scr, sems, finish)


def ff_end_kernel(layer, h_ref, a_ref, b1, b2, b3, vec_ref, io_ref, x0, x1, wp_ref, *rest):
    refs, (y_ref, w1, w2, m_scr, wp, wp_sem, sems) = rest[:-7], rest[-7:]
    shards = [refs[i:i + 2] for i in range(0, len(refs), 2)]
    tok = x0.shape[1]
    last = pltpu.make_async_copy(wp_ref.at[1], wp, wp_sem.at[0])

    def finish(update, first):
        if first:
            last.start()
        h = h_ref[0] + update + vec_ref[0:1]
        if first:
            last.wait()
        y = jnp.dot(h.astype(BF16), wp[...], preferred_element_type=F32) + io_ref[3:4]
        for i, ref in enumerate((x0, x1)):
            y_ref[i, 0] = (y[i * tok:(i + 1) * tok] + ref[0].astype(F32)).astype(BF16)

    ff_steps(layer, a_ref, (b1, b2, b3), shards, w1, w2, m_scr, sems, finish)


def rows_spec(shape):
    return pl.BlockSpec((1,) + shape, lambda i: (i, 0, 0))


def fixed_spec(shape, layer):
    return pl.BlockSpec((1,) + shape, lambda i: (layer,) + (0,) * len(shape))


def vec_spec(rows, cols):
    return pl.BlockSpec((rows, cols), lambda i: (0, 0))


def call(kernel, grid, in_specs, out_specs, out_shape, flops, scratch=(), aliases=None):
    return pl.pallas_call(
        kernel, grid=grid, in_specs=in_specs, out_specs=out_specs, out_shape=out_shape,
        scratch_shapes=scratch, input_output_aliases=aliases or {},
        cost_estimate=pl.CostEstimate(flops=flops, bytes_accessed=16 << 20, transcendentals=0),
        compiler_params=pltpu.CompilerParams(vmem_limit_bytes=VMEM_LIMIT))


def tie(*values):
    return lax.optimization_barrier(values)


def solution(mesh):
    tp_size = mesh.shape["tp"]
    dp_size = mesh.shape["dp"]

    def swap(value, mask):
        return lax.ppermute(value, "tp", [(i, i ^ mask) for i in range(tp_size)])

    def body(latents, context, io_vecs, w_proj, block_vecs, w_qkv, w_o1, w_q2, w_kv2, w_o2, w_ff1, b_ff1, w_ff2):
        batch, rows_loc, side, channels = latents.shape
        tok = rows_loc * side
        layers = w_qkv.shape[0]
        width = w_o1.shape[1] * HEAD
        ff = w_ff2.shape[1]
        ctx_len = context.shape[1]
        ctx_pad = -(-ctx_len // 16) * 16
        mine = batch // tp_size
        n_tok = tp_size * tok
        me = lax.axis_index("tp")
        dp_me = lax.axis_index("dp")

        def piece_of(value, layer, axis):
            rows = value.shape[axis] // dp_size
            start = [0] * value.ndim
            start[0], start[axis] = layer, dp_me * rows
            size = list(value.shape)
            size[0], size[axis] = 1, rows
            return lax.dynamic_slice(value, start, size)

        def gather(piece):
            return lax.all_gather(piece, "dp", axis=0, tiled=True)

        qkv_t = w_qkv.transpose(0, 2, 3, 4, 1).reshape(layers, 3 * width, channels)
        q2_t = w_q2.transpose(0, 2, 3, 1).reshape(layers, width, channels)
        o1_t = w_o1.reshape(layers, width, channels)
        o2_t = w_o2.reshape(layers, width, channels)
        ff1_t = w_ff1.transpose(0, 2, 1, 3)

        x_rows = latents.reshape(tp_size, mine, tok, channels)

        def group_of(array, index):
            return lax.dynamic_index_in_dim(array, index, 0, keepdims=False)

        x_parts = [group_of(x_rows, me)] + [swap(group_of(x_rows, me ^ m), m) for m in (1, 2, 3)]
        far_qkv = swap(piece_of(qkv_t, 0, 1)[0], 2)
        far_rest = swap(jnp.concatenate([piece_of(w, 0, 1)[0] for w in (o1_t, q2_t, o2_t)]), 2)
        sib_qkv, sib_o1, sib_q2, sib_o2 = (
            swap(w, 1) for w in (qkv_t, o1_t, q2_t, o2_t))
        bias = [b_ff1] + [swap(b_ff1, m) for m in (1, 2, 3)]

        kv = jnp.einsum("blc,rcjhd->rbljhd", context, w_kv2, preferred_element_type=F32).astype(BF16)
        kv = kv.reshape(layers, batch, ctx_len, 2 * width)
        kv = jnp.pad(kv, ((0, 0), (0, 0), (0, ctx_pad - ctx_len), (0, 0)))
        kv_out = [lax.dynamic_slice_in_dim(kv, (me ^ m) * mine, mine, 1) for m in range(tp_size)]
        kv_out[0], piece = tie(kv_out[0], far_qkv)
        full_qkv = gather(piece)
        kv_parts = [kv_out[0]] + [swap(kv_out[m], m) for m in (1, 2, 3)]
        ff_src = [piece_of(ff1_t, 0, 2)[0], piece_of(w_ff2, 0, 1)[0]]
        far_ff, far_second = swap(ff_src[0], 2), swap(ff_src[1], 2)
        sib_ff1, sib_ff2 = swap(ff1_t, 1), swap(w_ff2, 1)
        x_parts = list(tie(*x_parts, *ff_src, *kv_out))[:tp_size]

        grid = (mine,)
        total = mine * n_tok
        a_shape = jax.ShapeDtypeStruct((mine, n_tok, channels), BF16)
        h_shape = jax.ShapeDtypeStruct((mine, n_tok, channels), F32)
        o_shape = jax.ShapeDtypeStruct((mine, n_tok, width), BF16)
        a_spec, o_spec = rows_spec((n_tok, channels)), rows_spec((n_tok, width))
        x_spec = rows_spec((tok, channels))

        hidden, act = call(
            in_kernel, grid,
            [x_spec] * 4 + [fixed_spec((channels, channels), 0), vec_spec(4, channels), vec_spec(2, channels)],
            [a_spec, a_spec], [h_shape, a_shape], 2 * total * channels * channels,
            [pltpu.VMEM((n_tok, channels), BF16)],
        )(*x_parts, w_proj, io_vecs, block_vecs[0, 0:2])

        def self_attn(act, first, second, layer):
            return call(functools.partial(self_kernel, layer), grid,
                        [a_spec] + [pl.BlockSpec(memory_space=pl.ANY)] * 2, [o_spec, o_spec], [o_shape, o_shape],
                        4 * total * channels * 3 * width + 32 * total * n_tok * width,
                        [pltpu.VMEM((2, 3 * width, channels), BF16), pltpu.SemaphoreType.DMA((2,))])(act, first, second)

        tile = n_tok // 2
        tiles = (2 * mine,)
        t_spec = pl.BlockSpec((1, tile, channels), lambda i: (i // 2, i % 2, 0))
        any_spec = pl.BlockSpec(memory_space=pl.ANY)
        group = 4
        cross_groups = SHARDS * width // (group * HEAD)

        def middle(hidden, mixed, vecs, layer, slot, rest, rest_sib):
            kv_spec = pl.BlockSpec((1, 1, ctx_pad, 2 * width), lambda i: (layer, i, 0, 0))
            square = pltpu.VMEM((channels, channels), BF16)
            return call(
                functools.partial(mid_kernel, ctx_len, layer, slot), grid,
                [a_spec] + [o_spec] * 4 + [kv_spec] * 4 + [vec_spec(6, channels)] + [any_spec] * 8,
                [a_spec, a_spec], [h_shape, a_shape], 8 * total * channels * channels,
                [pltpu.VMEM((n_tok, channels), BF16), square, square, square,
                 pltpu.VMEM((cross_groups, group * 128, group * HEAD), BF16),
                 pltpu.VMEM((cross_groups, group * 128, 2 * group * HEAD), BF16),
                 pltpu.VMEM((cross_groups, n_tok, group * 128), BF16),
                 pltpu.SemaphoreType.DMA((3,))], {0: 0},
            )(hidden, *mixed, *kv_parts, vecs, o1_t, sib_o1, q2_t, sib_q2, o2_t, sib_o2, rest, rest_sib)

        chunks = ff // FF_COLS
        ff_flops = 6 * total * channels * ff

        def ff_scratch(n, *more):
            return [pltpu.VMEM((n, 2, channels, ff), BF16), pltpu.VMEM((n * ff, channels), BF16),
                    pltpu.VMEM((tile, n * ff), BF16), *more, pltpu.SemaphoreType.DMA((n * (chunks + 1),))]

        b_spec = [fixed_spec((2, ff), layer) for layer in range(layers)]

        def feed_forward(hidden, act, layer, *shards):
            n = len(shards)
            kinds = tuple(len(weights) for _, weights in shards)
            return call(functools.partial(ff_kernel, layer, kinds), tiles,
                        [t_spec, t_spec] + [b_spec[layer]] * n + [any_spec] * sum(kinds), t_spec, h_shape,
                        n * ff_flops, ff_scratch(n), {0: 0})(
                        hidden, act, *[bias[i] for i, _ in shards], *[w for _, weights in shards for w in weights])

        act, piece = tie(act, far_rest)
        full_rest = gather(piece)
        for layer in range(layers):
            vecs = block_vecs[layer]
            act, full = tie(act, full_qkv)
            rem = full.reshape(dp_size, -1, channels)
            rem_sib = swap(rem, 1)
            m0, m1 = self_attn(act, qkv_t, sib_qkv, layer)
            act, m0 = tie(act, m0)
            if layer == 0:
                act, piece = tie(act, far_ff)
                full_ff = gather(piece)
            else:
                m0, rest = tie(m0, next_rest)
                rest_sib = swap(rest, 1)
            m2, m3 = self_attn(act, rem, rem_sib, layer)
            if layer == 0:
                act, m3, piece, rest = tie(act, m3, far_second, full_rest)
                full_second = gather(piece)
                rest = rest.reshape(dp_size, -1, channels)
                rest_sib = swap(rest, 1)
                act, src_a, src_b, src_c, *src = tie(act, qkv_t, ff1_t, w_ff2, o1_t, q2_t, o2_t)
                far_qkv = swap(piece_of(src_a, 1, 1)[0], 2)
                far_ff1 = swap(piece_of(src_b, 1, 2)[0], 2)
                next_rest = swap(jnp.concatenate([w[1].reshape(dp_size, -1, channels) for w in src], axis=1), 2)
                next_ff2 = swap(src_c[1:], 2)
            hidden, act = middle(hidden, [m0, m1, m2, m3], jnp.stack([vecs[i] for i in (6, 2, 3, 7, 4, 5)]),
                                 layer, 0, rest, rest_sib)
            if layer == 0:
                act, piece = tie(act, far_qkv)
                full_qkv = gather(piece)
                hidden = feed_forward(hidden, act, layer, (0, (ff1_t, w_ff2)), (1, (sib_ff1, sib_ff2)))
                hidden, act, full, piece = tie(hidden, act, full_ff, far_ff1)
                next_ff = gather(piece)
                rem = full.reshape(dp_size, 2, ff // dp_size, channels)
                rem_sib = swap(rem, 1)
                hidden, second = tie(hidden, full_second[None])
                second_sib = swap(second, 1)
                hidden = feed_forward(hidden, act, layer, (2, (rem, second)))
                after = block_vecs[layer + 1]
                hidden, act = call(
                    functools.partial(ff_last_kernel, layer), tiles,
                    [t_spec, t_spec, b_spec[layer], vec_spec(3, channels), any_spec, any_spec],
                    [t_spec, t_spec], [h_shape, a_shape], ff_flops,
                    ff_scratch(1), {0: 0},
                )(hidden, act, bias[3], jnp.stack([vecs[8], after[0], after[1]]), rem_sib, second_sib)

        hidden, act, full, next_ff2 = tie(hidden, act, next_ff, next_ff2)
        next_ff2_sib = swap(next_ff2, 1)
        rem = full.reshape(dp_size, 2, ff // dp_size, channels)
        ff_weights = [sib_ff1, sib_ff2, rem, next_ff2, swap(rem, 1), next_ff2_sib]
        hidden = feed_forward(hidden, act, layers - 1, (0, (ff1_t, w_ff2)))
        parts = [None] * tp_size
        split = tp_size // 2
        for half in (1, 0):
            row_spec = pl.BlockSpec((1, tile, channels), lambda i, half=half: (i, half, 0))
            pair = call(
                functools.partial(ff_end_kernel, layers - 1), grid,
                [row_spec, row_spec] + [b_spec[layers - 1]] * 3 + [vec_spec(1, channels), vec_spec(4, channels)]
                + [x_spec] * 2 + [any_spec] * 7,
                pl.BlockSpec((split, 1, tok, channels), lambda i: (0, i, 0, 0)),
                jax.ShapeDtypeStruct((split, mine, tok, channels), BF16), 3 * ff_flops // 2,
                ff_scratch(3, pltpu.VMEM((channels, channels), BF16), pltpu.SemaphoreType.DMA((1,))),
                None,
            )(hidden, act, *bias[1:], vecs[8:9], io_vecs, *x_parts[half * split:(half + 1) * split], w_proj, *ff_weights)
            for i in range(split):
                m = half * split + i
                parts[m] = swap(pair[i], m) if m else pair[i]
            if half:
                hidden, pair = tie(hidden, pair)
        out = jnp.zeros((tp_size, mine, tok, channels), BF16)
        for m in (0, 2, 3, 1):
            out = lax.dynamic_update_index_in_dim(out, parts[m], me ^ m, 0)
        return out.reshape(batch, rows_loc, side, channels)

    act_spec = P("dp", "tp", None, None)
    in_specs = (act_spec, P("dp", None, None), P(), P(), P(),
                P(None, None, None, "tp", None), P(None, "tp", None, None),
                P(None, None, "tp", None), P(None, None, None, "tp", None),
                P(None, "tp", None, None), P(None, None, None, "tp"),
                P(None, None, "tp"), P(None, "tp", None))
    return jax.shard_map(body, mesh=mesh, in_specs=in_specs, out_specs=act_spec, check_vma=False)
```

```python
import functools

import jax
import jax.numpy as jnp
from jax import lax
from jax.experimental import pallas as pl
from jax.experimental.pallas import tpu as pltpu
from jax.sharding import PartitionSpec as P


GROUPS = 32
GN_EPS = 1e-6
LN_EPS = 1e-5
SHARDS = 4
HEAD = 64
LOG2E = 1.4426950408889634
F32 = jnp.float32
BF16 = jnp.bfloat16
NT = (((1,), (1,)), ((), ()))
VMEM_LIMIT = 67043328


def layer_norm(hidden, ln_gain, ln_shift):
    average = jnp.mean(hidden, axis=-1, keepdims=True)
    centered = hidden - average
    variance = jnp.mean(centered * centered, axis=-1, keepdims=True)
    return (centered * lax.rsqrt(variance + LN_EPS) * ln_gain + ln_shift).astype(BF16)


def attend(q, k, v):
    scores = lax.dot_general(q, k, NT, preferred_element_type=F32)
    top = jnp.max(scores, axis=-1, keepdims=True)
    probs = jnp.exp2((scores - top) * (HEAD ** -0.5 * LOG2E)).astype(BF16)
    values = jnp.concatenate([v, jnp.ones_like(v)], axis=1)
    mixed = jnp.dot(probs, values, preferred_element_type=F32)
    return (mixed[:, :HEAD] / mixed[:, HEAD:]).astype(BF16)


def in_kernel(x0, x1, x2, x3, w_ref, io_ref, ln_ref, h_out, a_out, g_scr):
    tok, channels = x0.shape[1:]
    parts = [ref[0].astype(F32) for ref in (x0, x1, x2, x3)]
    size = channels // GROUPS
    count = len(parts) * tok * size
    lanes = 128
    row = lax.broadcasted_iota(jnp.int32, (channels, lanes), 0)
    first = lax.broadcasted_iota(jnp.int32, (channels, lanes), 1) * size
    member = ((row >= first) & (row < first + size)).astype(F32)

    def group_average(columns):
        per_group = jnp.dot(jnp.broadcast_to(columns, (8, channels)), member,
                            precision=lax.Precision.HIGHEST, preferred_element_type=F32) / count
        return lax.dot_general(per_group, member, NT, precision=lax.Precision.HIGHEST,
                               preferred_element_type=F32)[0:1]

    mean = group_average(sum(jnp.sum(p, axis=0, keepdims=True) for p in parts))
    var = group_average(sum(jnp.sum((p - mean) * (p - mean), axis=0, keepdims=True) for p in parts))
    inverse = lax.rsqrt(var + GN_EPS)
    for i, p in enumerate(parts):
        g_scr[i * tok:(i + 1) * tok, :] = ((p - mean) * inverse * io_ref[0:1] + io_ref[1:2]).astype(BF16)
    h = jnp.dot(g_scr[...], w_ref[0], preferred_element_type=F32) + io_ref[2:3]
    h_out[0] = h
    a_out[0] = layer_norm(h, ln_ref[0:1], ln_ref[1:2])


def self_kernel(layer, a_ref, own_ref, sib_ref, o0, o1, w, sems):
    width = o0.shape[-1]
    copies = []
    for n, ref in enumerate((own_ref, sib_ref)):
        if ref.shape[1] == w.shape[1]:
            pairs = [(ref.at[layer], w.at[n])]
        else:
            rows = ref.shape[1]
            pairs = [(ref.at[d], w.at[n, pl.ds(d * rows, rows)]) for d in range(ref.shape[0])]
        copies.append([pltpu.make_async_copy(src, to, sems.at[n]) for src, to in pairs])

    @pl.when(pl.program_id(0) == 0)
    def _():
        for some in copies:
            for copy in some:
                copy.start()

    for n, o_ref in enumerate((o0, o1)):
        @pl.when(pl.program_id(0) == 0)
        def _():
            for copy in copies[n]:
                copy.wait()

        qkv = lax.dot_general(a_ref[0], w[n], NT, preferred_element_type=F32).astype(BF16)
        for head in range(width // HEAD):
            lo = head * HEAD
            o_ref[0, :, lo:lo + HEAD] = attend(
                qkv[:, lo:lo + HEAD], qkv[:, width + lo:width + lo + HEAD],
                qkv[:, 2 * width + lo:2 * width + lo + HEAD])


def row_copies(own, sib, rest, rest_sib, layer, slot, dst, sem):
    width = own.shape[1]
    pieces = rest.shape[0]
    rows = width // pieces
    pairs = [(ref.at[layer], dst.at[pl.ds(i * width, width)]) for i, ref in enumerate((own, sib))]
    for i, ref in ((2, rest), (3, rest_sib)):
        pairs += [(ref.at[d, pl.ds(slot * rows, rows)], dst.at[pl.ds(i * width + d * rows, rows)]) for d in range(pieces)]
    return [pltpu.make_async_copy(src, to, sem) for src, to in pairs]


def mid_kernel(valid, layer, slot, h_ref, o0, o1, o2, o3, kv0, kv1, kv2, kv3, vec_ref,
               o1_own, o1_sib, q2_own, q2_sib, o2_own, o2_sib, rest, rest_sib,
               h_out, a_out, o_all, w_out1, w_q, w_out2, k_scr, v_scr, p_scr, sems):
    step = pl.program_id(0)
    width = o0.shape[-1]
    heads = width // HEAD
    keys = kv0.shape[2]
    lanes = 128
    group = k_scr.shape[2] // HEAD
    cols = group * HEAD
    copies = [row_copies(own, sib, rest, rest_sib, layer, slot + i, dst, sems.at[i]) for i, (own, sib, dst) in enumerate(
        ((o1_own, o1_sib, w_out1), (q2_own, q2_sib, w_q), (o2_own, o2_sib, w_out2)))]

    @pl.when(step == 0)
    def _():
        for some in copies:
            for copy in some:
                copy.start()
        k_scr[...] = jnp.zeros_like(k_scr)
        v_scr[...] = jnp.zeros_like(v_scr)

    one = (lax.broadcasted_iota(jnp.int32, (keys, HEAD), 0) < valid).astype(BF16)
    for shard, ref in enumerate((kv0, kv1, kv2, kv3)):
        kv = ref[0, 0]
        for head in range(heads):
            place = shard * heads + head
            g, r = place // group, place % group
            rows = slice(r * lanes, r * lanes + keys)
            at = slice(r * HEAD, (r + 1) * HEAD)
            k_scr[g, rows, at] = kv[:, head * HEAD:(head + 1) * HEAD]
            v_scr[g, rows, at] = kv[:, width + head * HEAD:width + (head + 1) * HEAD]
            v_scr[g, rows, cols + r * HEAD:cols + (r + 1) * HEAD] = one
    for i, o_ref in enumerate((o0, o1, o2, o3)):
        o_all[:, i * width:(i + 1) * width] = o_ref[0]

    half = h_ref.shape[1] // 2
    halves = [slice(0, half), slice(half, 2 * half)]

    def run(first):
        def wait(i):
            if first:
                for copy in copies[i]:
                    copy.wait()

        wait(0)
        h = [h_ref[0, at, :] + jnp.dot(o_all[at, :], w_out1[...], preferred_element_type=F32) + vec_ref[0:1] for at in halves]
        for at, value in zip(halves, h):
            h_out[0, at, :] = value
        act = [layer_norm(value, vec_ref[1:2], vec_ref[2:3]) for value in h]
        wait(1)
        q = [lax.dot_general(value, w_q[...], NT, preferred_element_type=F32).astype(BF16) for value in act]
        live = lax.broadcasted_iota(jnp.int32, (half, lanes), 1) < valid
        for g in range(k_scr.shape[0]):
            at = slice(g * cols, (g + 1) * cols)
            scores = [lax.dot_general(value[:, at], k_scr[g], NT, preferred_element_type=F32) for value in q]
            for rows, part in zip(halves, scores):
                for r in range(group):
                    sl = slice(r * lanes, (r + 1) * lanes)
                    s = jnp.where(live, part[:, sl], -jnp.inf)
                    top = jnp.max(s, axis=-1, keepdims=True)
                    p_scr[g, rows, sl] = jnp.exp2((s - top) * (HEAD ** -0.5 * LOG2E)).astype(BF16)
            for rows in halves:
                mixed = jnp.dot(p_scr[g, rows, :], v_scr[g], preferred_element_type=F32)
                o_all[rows, at] = (mixed[:, :cols] / mixed[:, cols:]).astype(BF16)
        wait(2)
        h = [h_out[0, at, :] + jnp.dot(o_all[at, :], w_out2[...], preferred_element_type=F32) + vec_ref[3:4] for at in halves]
        for at, value in zip(halves, h):
            h_out[0, at, :] = value
            a_out[0, at, :] = layer_norm(value, vec_ref[4:5], vec_ref[5:6])

    pl.when(step == 0)(functools.partial(run, True))
    pl.when(step > 0)(functools.partial(run, False))


FF_COLS = 256


def ff_copies(layer, shards, w1, w2, sems):
    channels, ff = w1.shape[2:]
    chunks = ff // FF_COLS
    first, second = [], []
    for n, refs in enumerate(shards):
        packed = refs[0].shape[2] != channels
        rows = refs[0].shape[2]
        pieces = range(refs[0].shape[0])
        for j in range(chunks):
            at = pl.ds(j * FF_COLS, FF_COLS)
            if packed:
                first.append([(refs[0].at[d, pl.ds(0, 2), :, at], w1.at[n, :, pl.ds(d * rows, rows), at]) for d in pieces])
            else:
                first.append([(refs[0].at[layer, :, :, at], w1.at[n, :, :, at])])
        if len(refs) == 2:
            second.append([(refs[1].at[layer if refs[1].shape[0] > 1 else 0], w2.at[pl.ds(n * ff, ff)])])
        else:
            second.append([(refs[0].at[d, 2], w2.at[pl.ds(n * ff + d * rows, rows)]) for d in pieces])
    return [[pltpu.make_async_copy(src, to, sems.at[i]) for src, to in pairs] for i, pairs in enumerate(first + second)]


def ff_steps(layer, a_ref, biases, shards, w1, w2, m_scr, sems, finish):
    step = pl.program_id(0)
    groups = ff_copies(layer, shards, w1, w2, sems)
    ff = w1.shape[3]
    chunks = ff // FF_COLS
    ahead = len(groups)

    def start(i):
        for copy in groups[i] if i < len(groups) else ():
            copy.start()

    def run(first):
        if first:
            for i in range(ahead):
                start(i)
        a = a_ref[0]
        for n, b1_ref in enumerate(biases):
            for j in range(chunks):
                if first:
                    start(n * chunks + j + ahead)
                    for copy in groups[n * chunks + j]:
                        copy.wait()
                sl = slice(j * FF_COLS, (j + 1) * FF_COLS)
                u0 = jnp.dot(a, w1[n, 0, :, sl], preferred_element_type=F32) + b1_ref[0, 0:1, sl]
                u1 = jnp.dot(a, w1[n, 1, :, sl], preferred_element_type=F32) + b1_ref[0, 1:2, sl]
                gate = 0.5 * u1 * (1.0 + lax.erf(u1 * (0.5 ** 0.5)))
                m_scr[:, n * ff + j * FF_COLS:n * ff + (j + 1) * FF_COLS] = (u0 * gate).astype(BF16)
        if first:
            for some in groups[len(biases) * chunks:]:
                for copy in some:
                    copy.wait()
        finish(jnp.dot(m_scr[...], w2[...], preferred_element_type=F32), first)

    pl.when(step == 0)(functools.partial(run, True))
    pl.when(step > 0)(functools.partial(run, False))


def ff_kernel(layer, kinds, h_ref, a_ref, *rest):
    biases, refs = rest[:len(kinds)], list(rest[len(kinds):-5])
    h_out, w1, w2, m_scr, sems = rest[-5:]
    shards = [[refs.pop(0) for _ in range(kind)] for kind in kinds]

    def finish(update, first):
        h_out[0] = h_ref[0] + update

    ff_steps(layer, a_ref, biases, shards, w1, w2, m_scr, sems, finish)


def ff_last_kernel(layer, h_ref, a_ref, b1_ref, vec_ref, w1_ref, w2_ref, h_out, a_out, w1, w2, m_scr, sems):
    def finish(update, first):
        h = h_ref[0] + update + vec_ref[0:1]
        h_out[0] = h
        a_out[0] = layer_norm(h, vec_ref[1:2], vec_ref[2:3])

    ff_steps(layer, a_ref, (b1_ref,), ((w1_ref, w2_ref),), w1, w2, m_scr, sems, finish)


def ff_end_kernel(layer, h_ref, a_ref, b2, b3, vec_ref, io_ref, x0, x1, wp_ref, *rest):
    refs, (y_ref, w1, w2, m_scr, wp, wp_sem, sems) = rest[:-7], rest[-7:]
    shards = [refs[i:i + 2] for i in range(0, len(refs), 2)]
    tok = x0.shape[1]
    last = pltpu.make_async_copy(wp_ref.at[1], wp, wp_sem.at[0])

    def finish(update, first):
        if first:
            last.start()
        h = h_ref[0] + update + vec_ref[0:1]
        if first:
            last.wait()
        y = jnp.dot(h.astype(BF16), wp[...], preferred_element_type=F32) + io_ref[3:4]
        for i, ref in enumerate((x0, x1)):
            y_ref[i, 0] = (y[i * tok:(i + 1) * tok] + ref[0].astype(F32)).astype(BF16)

    ff_steps(layer, a_ref, (b2, b3), shards, w1, w2, m_scr, sems, finish)


def rows_spec(shape):
    return pl.BlockSpec((1,) + shape, lambda i: (i, 0, 0))


def fixed_spec(shape, layer):
    return pl.BlockSpec((1,) + shape, lambda i: (layer,) + (0,) * len(shape))


def vec_spec(rows, cols):
    return pl.BlockSpec((rows, cols), lambda i: (0, 0))


def call(kernel, grid, in_specs, out_specs, out_shape, flops, scratch=(), aliases=None):
    return pl.pallas_call(
        kernel, grid=grid, in_specs=in_specs, out_specs=out_specs, out_shape=out_shape,
        scratch_shapes=scratch, input_output_aliases=aliases or {},
        cost_estimate=pl.CostEstimate(flops=flops, bytes_accessed=16 << 20, transcendentals=0),
        compiler_params=pltpu.CompilerParams(vmem_limit_bytes=VMEM_LIMIT))


def tie(*values):
    return lax.optimization_barrier(values)


def solution(mesh):
    tp_size = mesh.shape["tp"]
    dp_size = mesh.shape["dp"]

    def swap(value, mask):
        return lax.ppermute(value, "tp", [(i, i ^ mask) for i in range(tp_size)])

    def body(latents, context, io_vecs, w_proj, block_vecs, w_qkv, w_o1, w_q2, w_kv2, w_o2, w_ff1, b_ff1, w_ff2):
        batch, rows_loc, side, channels = latents.shape
        tok = rows_loc * side
        layers = w_qkv.shape[0]
        width = w_o1.shape[1] * HEAD
        ff = w_ff2.shape[1]
        ctx_len = context.shape[1]
        ctx_pad = -(-ctx_len // 16) * 16
        mine = batch // tp_size
        n_tok = tp_size * tok
        me = lax.axis_index("tp")
        dp_me = lax.axis_index("dp")

        def piece_of(value, layer, axis):
            rows = value.shape[axis] // dp_size
            start = [0] * value.ndim
            start[0], start[axis] = layer, dp_me * rows
            size = list(value.shape)
            size[0], size[axis] = 1, rows
            return lax.dynamic_slice(value, start, size)

        def gather(piece):
            return lax.all_gather(piece, "dp", axis=0, tiled=True)

        qkv_t = w_qkv.transpose(0, 2, 3, 4, 1).reshape(layers, 3 * width, channels)
        q2_t = w_q2.transpose(0, 2, 3, 1).reshape(layers, width, channels)
        o1_t = w_o1.reshape(layers, width, channels)
        o2_t = w_o2.reshape(layers, width, channels)
        ff1_t = w_ff1.transpose(0, 2, 1, 3)

        x_rows = latents.reshape(tp_size, mine, tok, channels)

        def group_of(array, index):
            return lax.dynamic_index_in_dim(array, index, 0, keepdims=False)

        x_parts = [group_of(x_rows, me)] + [swap(group_of(x_rows, me ^ m), m) for m in (1, 2, 3)]
        far_qkv = swap(piece_of(qkv_t, 0, 1)[0], 2)
        far_rest = swap(jnp.concatenate([piece_of(w, 0, 1)[0] for w in (o1_t, q2_t, o2_t)]), 2)
        sib_qkv, sib_o1, sib_q2, sib_o2 = (
            swap(w, 1) for w in (qkv_t, o1_t, q2_t, o2_t))
        bias = [b_ff1] + [swap(b_ff1, m) for m in (1, 2, 3)]

        kv = jnp.einsum("blc,rcjhd->rbljhd", context, w_kv2, preferred_element_type=F32).astype(BF16)
        kv = kv.reshape(layers, batch, ctx_len, 2 * width)
        kv = jnp.pad(kv, ((0, 0), (0, 0), (0, ctx_pad - ctx_len), (0, 0)))
        kv_out = [lax.dynamic_slice_in_dim(kv, (me ^ m) * mine, mine, 1) for m in range(tp_size)]
        kv_out[0], piece = tie(kv_out[0], far_qkv)
        full_qkv = gather(piece)
        kv_parts = [kv_out[0]] + [swap(kv_out[m], m) for m in (1, 2, 3)]
        ff_src = [piece_of(ff1_t, 0, 2)[0], w_ff2[:1]]
        qkv_src = piece_of(qkv_t, 1, 1)[0]
        next_qkv = swap(qkv_src, 2)
        far_ff, far_second = swap(ff_src[0], 2), swap(ff_src[1], 2)
        sib_ff1, sib_ff2 = swap(ff1_t, 1), swap(w_ff2, 1)
        x_parts = list(tie(*x_parts, *ff_src, qkv_src, *kv_out))[:tp_size]

        grid = (mine,)
        total = mine * n_tok
        a_shape = jax.ShapeDtypeStruct((mine, n_tok, channels), BF16)
        h_shape = jax.ShapeDtypeStruct((mine, n_tok, channels), F32)
        o_shape = jax.ShapeDtypeStruct((mine, n_tok, width), BF16)
        a_spec, o_spec = rows_spec((n_tok, channels)), rows_spec((n_tok, width))
        x_spec = rows_spec((tok, channels))

        hidden, act = call(
            in_kernel, grid,
            [x_spec] * 4 + [fixed_spec((channels, channels), 0), vec_spec(4, channels), vec_spec(2, channels)],
            [a_spec, a_spec], [h_shape, a_shape], 2 * total * channels * channels,
            [pltpu.VMEM((n_tok, channels), BF16)],
        )(*x_parts, w_proj, io_vecs, block_vecs[0, 0:2])

        def self_attn(act, first, second, layer):
            return call(functools.partial(self_kernel, layer), grid,
                        [a_spec] + [pl.BlockSpec(memory_space=pl.ANY)] * 2, [o_spec, o_spec], [o_shape, o_shape],
                        4 * total * channels * 3 * width + 32 * total * n_tok * width,
                        [pltpu.VMEM((2, 3 * width, channels), BF16), pltpu.SemaphoreType.DMA((2,))])(act, first, second)

        tile = n_tok // 2
        tiles = (2 * mine,)
        t_spec = pl.BlockSpec((1, tile, channels), lambda i: (i // 2, i % 2, 0))
        any_spec = pl.BlockSpec(memory_space=pl.ANY)
        group = 4
        cross_groups = SHARDS * width // (group * HEAD)

        def middle(hidden, mixed, vecs, layer, slot, rest, rest_sib):
            kv_spec = pl.BlockSpec((1, 1, ctx_pad, 2 * width), lambda i: (layer, i, 0, 0))
            square = pltpu.VMEM((channels, channels), BF16)
            return call(
                functools.partial(mid_kernel, ctx_len, layer, slot), grid,
                [a_spec] + [o_spec] * 4 + [kv_spec] * 4 + [vec_spec(6, channels)] + [any_spec] * 8,
                [a_spec, a_spec], [h_shape, a_shape], 8 * total * channels * channels,
                [pltpu.VMEM((n_tok, channels), BF16), square, square, square,
                 pltpu.VMEM((cross_groups, group * 128, group * HEAD), BF16),
                 pltpu.VMEM((cross_groups, group * 128, 2 * group * HEAD), BF16),
                 pltpu.VMEM((cross_groups, n_tok, group * 128), BF16),
                 pltpu.SemaphoreType.DMA((3,))], {0: 0},
            )(hidden, *mixed, *kv_parts, vecs, o1_t, sib_o1, q2_t, sib_q2, o2_t, sib_o2, rest, rest_sib)

        chunks = ff // FF_COLS
        ff_flops = 6 * total * channels * ff

        def ff_scratch(n, *more):
            return [pltpu.VMEM((n, 2, channels, ff), BF16), pltpu.VMEM((n * ff, channels), BF16),
                    pltpu.VMEM((tile, n * ff), BF16), *more, pltpu.SemaphoreType.DMA((n * (chunks + 1),))]

        b_spec = [fixed_spec((2, ff), layer) for layer in range(layers)]

        def feed_forward(hidden, act, layer, *shards):
            n = len(shards)
            kinds = tuple(len(weights) for _, weights in shards)
            return call(functools.partial(ff_kernel, layer, kinds), tiles,
                        [t_spec, t_spec] + [b_spec[layer]] * n + [any_spec] * sum(kinds), t_spec, h_shape,
                        n * ff_flops, ff_scratch(n), {0: 0})(
                        hidden, act, *[bias[i] for i, _ in shards], *[w for _, weights in shards for w in weights])

        act, piece = tie(act, far_rest)
        full_rest = gather(piece)
        for layer in range(layers):
            vecs = block_vecs[layer]
            act, full = tie(act, full_qkv)
            rem = full.reshape(dp_size, -1, channels)
            rem_sib = swap(rem, 1)
            m0, m1 = self_attn(act, qkv_t, sib_qkv, layer)
            act, m0 = tie(act, m0)
            if layer == 0:
                act, piece = tie(act, far_ff)
                full_ff = gather(piece)
            else:
                act, m0, rest, piece = tie(act, m0, full_rest, far_ff1)
                next_ff = gather(piece)
                rest = rest.reshape(dp_size, -1, channels)
                rest_sib = swap(rest, 1)
            m2, m3 = self_attn(act, rem, rem_sib, layer)
            if layer == 0:
                act, m3, rest = tie(act, m3, full_rest)
                rest = rest.reshape(dp_size, -1, channels)
                rest_sib = swap(rest, 1)
                act, src_b, src_c, *src = tie(act, ff1_t, w_ff2, o1_t, q2_t, o2_t)
                next_rest = swap(jnp.concatenate([piece_of(w, 1, 1)[0] for w in src]), 2)
                far_ff1 = swap(piece_of(src_b, 1, 2)[0], 2)
                next_ff2 = swap(src_c[1:], 2)
            hidden, act = middle(hidden, [m0, m1, m2, m3], jnp.stack([vecs[i] for i in (6, 2, 3, 7, 4, 5)]),
                                 layer, 0, rest, rest_sib)
            if layer == 0:
                act, piece = tie(act, next_qkv)
                full_qkv = gather(piece)
                hidden = feed_forward(hidden, act, layer, (0, (ff1_t, w_ff2)), (1, (sib_ff1, sib_ff2)))
                hidden, act, full = tie(hidden, act, full_ff)
                rem = full.reshape(dp_size, 2, ff // dp_size, channels)
                rem_sib = swap(rem, 1)
                hidden, second = tie(hidden, far_second)
                second_sib = swap(second, 1)
                hidden = feed_forward(hidden, act, layer, (2, (rem, second)))
                hidden, piece = tie(hidden, next_rest)
                full_rest = gather(piece)
                after = block_vecs[layer + 1]
                hidden, act = call(
                    functools.partial(ff_last_kernel, layer), tiles,
                    [t_spec, t_spec, b_spec[layer], vec_spec(3, channels), any_spec, any_spec],
                    [t_spec, t_spec], [h_shape, a_shape], ff_flops,
                    ff_scratch(1), {0: 0},
                )(hidden, act, bias[3], jnp.stack([vecs[8], after[0], after[1]]), rem_sib, second_sib)

        hidden = feed_forward(hidden, act, layers - 1, (0, (ff1_t, w_ff2)))
        hidden, act, full, next_ff2 = tie(hidden, act, next_ff, next_ff2)
        rem = full.reshape(dp_size, 2, ff // dp_size, channels)
        ff_weights = [rem, next_ff2, swap(rem, 1), swap(next_ff2, 1)]
        hidden = feed_forward(hidden, act, layers - 1, (1, (sib_ff1, sib_ff2)))
        parts = [None] * tp_size
        split = tp_size // 2
        for half in (1, 0):
            row_spec = pl.BlockSpec((1, tile, channels), lambda i, half=half: (i, half, 0))
            pair = call(
                functools.partial(ff_end_kernel, layers - 1), grid,
                [row_spec, row_spec] + [b_spec[layers - 1]] * 2 + [vec_spec(1, channels), vec_spec(4, channels)]
                + [x_spec] * 2 + [any_spec] * 5,
                pl.BlockSpec((split, 1, tok, channels), lambda i: (0, i, 0, 0)),
                jax.ShapeDtypeStruct((split, mine, tok, channels), BF16), 2 * ff_flops // 2,
                ff_scratch(2, pltpu.VMEM((channels, channels), BF16), pltpu.SemaphoreType.DMA((1,))),
                None,
            )(hidden, act, *bias[2:], vecs[8:9], io_vecs, *x_parts[half * split:(half + 1) * split], w_proj, *ff_weights)
            for i in range(split):
                m = half * split + i
                parts[m] = swap(pair[i], m) if m else pair[i]
            if half:
                hidden, pair = tie(hidden, pair)
        out = jnp.zeros((tp_size, mine, tok, channels), BF16)
        for m in (0, 2, 3, 1):
            out = lax.dynamic_update_index_in_dim(out, parts[m], me ^ m, 0)
        return out.reshape(batch, rows_loc, side, channels)

    act_spec = P("dp", "tp", None, None)
    in_specs = (act_spec, P("dp", None, None), P(), P(), P(),
                P(None, None, None, "tp", None), P(None, "tp", None, None),
                P(None, None, "tp", None), P(None, None, None, "tp", None),
                P(None, "tp", None, None), P(None, None, None, "tp"),
                P(None, None, "tp"), P(None, "tp", None))
    return jax.shard_map(body, mesh=mesh, in_specs=in_specs, out_specs=act_spec, check_vma=False)
```
